32 devices in a mesh: fsdp: 16 (over z, x, core), dp: 2 (over y).
Axes of the slice: x: 2, y: 2, z: 4, core: 2. Of those that a mesh axis runs over, the one named last changes fastest.
Arguments:
- tokens: bfloat16 [64, 256, 1536], P(('fsdp', 'dp')), may hold values from -21 to 21
- segments: int32 [64, 256], P(('fsdp', 'dp')), may hold values from 0 to 2, never falling along the last dimension, each value on 1 to 192 neighbouring positions
- norm_gain: bfloat16 [1536], P('fsdp'), may hold values from 0.5 to 1.5
- w_in: bfloat16 [1536, 6448], P('fsdp'), may hold values from -1 to 1
- conv_weight: bfloat16 [4, 3328], P(None, 'fsdp'), may hold values from -3 to 3
- conv_bias: bfloat16 [3328], P('fsdp'), may hold values from -0.5 to 0.5
- dt_bias: float32 [48], replicated, may hold values from -1 to 2
- a_log: float32 [48], replicated, may hold values from 0 to 1.5
- d_skip: float32 [48], replicated, may hold values from 0.5 to 1.5
- gate_gain: bfloat16 [3072], P('fsdp'), may hold values from 0.5 to 1.5
- w_out: bfloat16 [3072, 1536], P('fsdp'), may hold values from -0.109375 to 0.109375
- cotangent: bfloat16 [64, 256, 1536], P(('fsdp', 'dp')), may hold values from -6 to 6
Outputs:
- block_out: bfloat16 [64, 256, 1536], P(('fsdp', 'dp'))
- grad_tokens: float32 [64, 256, 1536], P(('fsdp', 'dp'))
- grad_norm_gain: float32 [1536], P('fsdp')
- grad_w_in: float32 [1536, 6448], P('fsdp')
- grad_conv_weight: float32 [4, 3328], P(None, 'fsdp')
- grad_conv_bias: float32 [3328], P('fsdp')
- grad_dt_bias: float32 [48], replicated
- grad_a_log: float32 [48], replicated
- grad_d_skip: float32 [48], replicated
- grad_gate_gain: float32 [3072], P('fsdp')
- grad_w_out: float32 [3072, 1536], P('fsdp')
The draws below stay inside these ranges and needn't reach their ends.
Inputs may be any that keep to these rules, and one draw needn't show every extreme that they name: `segments`: along each sequence the segment numbers never fall; every document runs 1 to 192 tokens and one runs exactly 192.
All inputs are finite; a program needn't handle non-finite values.
Results may differ from the reference program's by a relative error of at most 0.0064.
Values may be sent and summed in bfloat16 or wider, within the bound.
A program may use at most 320 MiB of HBM per device.

```python
import math
import jax
import jax.numpy as jnp
import numpy as np
from jax import lax

D = 1536
DI = 3072
H = 48
P_SIZE = 64
N = 128
CONV = 4
LEN = 256
MICRO = 2
DOCS = 3
CONVDIM = 3328
PROJ = 6448
SEG_MOST = 192
SEQS = 64


def common_signs(key):
    picked = jax.random.randint(jax.random.fold_in(key, 7101), (D,), 0, 2)
    return (2 * picked - 1).astype(jnp.float32)


def draw_tokens(key, part):
    signs = common_signs(key)
    noise_key = jax.random.fold_in(key, 7102)
    noise = jnp.clip(jax.random.normal(noise_key, (SEQS, LEN, D), jnp.float32), -5.0, 5.0)
    groups = SEQS // MICRO
    width = D // groups
    order = jax.random.permutation(jax.random.fold_in(key, 7103), groups)
    seq_group = jnp.arange(SEQS) // MICRO
    feat_group = jnp.arange(D) // width
    paired = order[seq_group][:, None] == feat_group[None, :]
    factor = jnp.where(paired, 4.0, 1.0).astype(jnp.float32)
    values = noise * factor[:, None, :] + signs
    return values.astype(jnp.bfloat16)


def draw_w_in(key, part):
    signs = common_signs(key)
    noise_key = jax.random.fold_in(key, 7104)
    noise = jnp.clip(jax.random.normal(noise_key, (D, PROJ), jnp.float32), -4.0, 4.0)
    pull = 8.5
    values = noise * D ** (-0.5)
    step_columns = (jnp.arange(PROJ) >= PROJ - H).astype(jnp.float32)
    values = values - pull / D * signs[:, None] * step_columns[None, :]
    return values.astype(jnp.bfloat16)


def block_scale(key, dims, shards, least, top_value):
    loudness, own = 1.0, jax.random.fold_in(key, 6)
    for dim, blocks in shards:
        draws = jnp.exp(jax.random.uniform(jax.random.fold_in(own, dim), (blocks,), jnp.float32, least / len(shards), top_value / len(shards)))
        loudness = loudness * jnp.repeat(draws, dims[dim] // blocks).reshape([-1 if axis == dim else 1 for axis in range(len(dims))])
    return loudness


def length_profile(amount, total, reach, skew):
    portions = [(1 << 20) // math.isqrt(standing ** skew) + 1 for standing in range(2, amount + 1)]
    spare, counts = total - reach - (amount - 1), [1] * (amount - 1)
    while spare > 0:
        candidates = [i for i in range(amount - 1) if counts[i] < reach]
        mass, budget = sum([portions[i] for i in candidates]), spare
        for i in candidates:
            more = min(reach - counts[i], max(1, budget * portions[i] // mass), spare)
            counts[i] = counts[i] + more
            spare = spare - more
    return np.array([reach] + counts)


def uneven_parts(own_key, number_of, total, bound, lean):
    if number_of == 2:
        one = jax.random.randint(own_key, (), max(1, total - bound), min(bound, total - 1) + 1)
        return jnp.stack([one, total - one])
    sizes = jnp.asarray(length_profile(number_of, total, bound, lean), jnp.int32)
    pairs = (number_of - 1) // 2
    giver, receiver = sizes[1:1 + 2 * pairs:2], sizes[2:2 + 2 * pairs:2]
    margin = jnp.minimum(giver - 1, bound - receiver)
    shifted = jax.random.randint(jax.random.fold_in(own_key, 1), (pairs,), 0, 1 << 20) % (margin + 1)
    sizes = sizes.at[1:1 + 2 * pairs:2].set(giver - shifted).at[2:2 + 2 * pairs:2].set(receiver + shifted)
    return sizes[jax.random.permutation(jax.random.fold_in(own_key, 2), number_of)]


def bell_draw(stream_key, shape, spread, limit, pieces=(), kind=jnp.bfloat16):
    loudness = block_scale(stream_key, shape, pieces, -0.22, 0.18) if pieces else 1.0
    result = jax.random.normal(stream_key, shape, jnp.float32) * spread * loudness
    return jnp.minimum(jnp.maximum(result, -limit), limit).astype(kind)


def setup_inputs(seed: int = 0) -> dict:
    key_of = jax.random.split(jax.random.key(seed), 13)
    tokens = draw_tokens(jax.random.fold_in(key_of[12], 71), 0)
    segments = jax.vmap(lambda own: jnp.searchsorted(jnp.cumsum(uneven_parts(own, DOCS, LEN, SEG_MOST, 0)), jnp.arange(LEN), side="right"))(jax.random.split(key_of[1], SEQS)).reshape((SEQS, LEN)).astype(jnp.int32)
    norm_gain = jnp.clip(1.0 + 0.1 * jax.random.normal(key_of[2], (D,), jnp.float32), 0.5, 1.5).astype(jnp.bfloat16)
    w_in = draw_w_in(jax.random.fold_in(key_of[12], 71), 0)
    conv_weight = bell_draw(key_of[4], (CONV, CONVDIM), CONV ** -0.5, 3.0, ((1, 16),))
    conv_bias = jnp.clip(jax.random.uniform(key_of[5], (CONVDIM,), jnp.float32, -0.5, 0.5) * block_scale(key_of[5], (CONVDIM,), ((0, 16),), -0.4, 0.0), -0.5, 0.5).astype(jnp.bfloat16)
    dt_bias = jnp.clip(jax.random.uniform(key_of[6], (H,), jnp.float32, -1.0, 2.0), -1.0, 2.0)
    a_log = jnp.clip(jax.random.uniform(key_of[7], (H,), jnp.float32, 0.0, 1.5), 0.0, 1.5)
    d_skip = jnp.clip(jax.random.uniform(key_of[8], (H,), jnp.float32, 0.5, 1.5), 0.5, 1.5)
    gate_gain = jnp.clip(1.0 + 0.1 * jax.random.normal(key_of[9], (DI,), jnp.float32), 0.5, 1.5).astype(jnp.bfloat16)
    w_out = bell_draw(key_of[10], (DI, D), DI ** -0.5, 0.109375, ((0, 16),))
    cotangent = bell_draw(key_of[11], (SEQS, LEN, D), 1.0, 6.0, ((0, 32),))
    return {"tokens": tokens, "segments": segments, "norm_gain": norm_gain, "w_in": w_in, "conv_weight": conv_weight, "conv_bias": conv_bias, "dt_bias": dt_bias, "a_log": a_log, "d_skip": d_skip, "gate_gain": gate_gain, "w_out": w_out, "cotangent": cotangent}


epsilon = 1e-05
highest = lax.Precision.HIGHEST

def mixer_whole(projected, seg_row, conv_kernel, conv_shift, dt_offset, log_rate, skip_gain, out_gain):
    length = projected.shape[0]
    gate_part = projected[:, :DI]
    conv_part = projected[:, DI:DI + CONVDIM]
    step_raw = projected[:, DI + CONVDIM:]
    padded = jnp.pad(conv_part, ((CONV - 1, 0), (0, 0)))
    seg_padded = jnp.pad(seg_row, (CONV - 1, 0), constant_values=-1)
    summed = jnp.zeros_like(conv_part) + conv_shift
    for offset in range(CONV):
        window = padded[offset:offset + length]
        same_doc = (seg_padded[offset:offset + length] == seg_row).astype(jnp.float32)
        summed = summed + conv_kernel[offset] * window * same_doc[:, None]
    activated = jax.nn.silu(summed)
    head_inputs = activated[:, :DI].reshape(length, H, P_SIZE)
    b_rows = activated[:, DI:DI + N]
    c_rows = activated[:, DI + N:]
    step_size = jax.nn.softplus(step_raw + dt_offset)
    log_decay = -step_size * jnp.exp(log_rate)
    cumulative = jnp.cumsum(log_decay, axis=0).T
    position = jnp.arange(length)
    visible = (position[:, None] >= position[None, :]) & (seg_row[:, None] == seg_row[None, :])
    differences = cumulative[:, :, None] - cumulative[:, None, :]
    decay_mat = jnp.where(visible[None], jnp.exp(jnp.where(visible[None], differences, 0.0)), 0.0)
    scores = jnp.dot(c_rows, b_rows.T, precision=highest)
    weights = decay_mat * scores[None] * step_size.T[:, None, :]
    ssm_out = jnp.einsum('hts,shp->thp', weights, head_inputs, precision=highest) + skip_gain[:, None] * head_inputs
    gated_out = ssm_out.reshape(length, DI) * jax.nn.silu(gate_part)
    norm_scale = lax.rsqrt(lax.optimization_barrier(jnp.mean(gated_out * gated_out, axis=-1, keepdims=True)) + epsilon)
    return gated_out * norm_scale * out_gain

def reference(tokens, segments, norm_gain, w_in, conv_weight, conv_bias, dt_bias, a_log, d_skip, gate_gain, w_out, cotangent):
    gain_in = norm_gain.astype(jnp.float32)
    kernel_in = conv_weight.astype(jnp.float32)
    shift_in = conv_bias.astype(jnp.float32)
    gain_out = gate_gain.astype(jnp.float32)

    def one_sequence(totals, inputs_now):
        token_rows, seg_row, grad_rows = inputs_now
        residual = token_rows.astype(jnp.float32)
        rstd_rows = lax.rsqrt(lax.optimization_barrier(jnp.mean(residual * residual, axis=-1, keepdims=True)) + epsilon)
        unit_rows = residual * rstd_rows
        normed = (unit_rows * gain_in).astype(jnp.bfloat16)
        projected = jnp.dot(normed, w_in, preferred_element_type=jnp.float32)

        def mixer_row(proj_in, kernel_arg, shift_arg, offset_arg, rate_arg, skip_arg, gain_arg):
            return mixer_whole(proj_in, seg_row, kernel_arg, shift_arg, offset_arg, rate_arg, skip_arg, gain_arg)
        mixed_f, mixer_back = jax.vjp(mixer_row, projected, kernel_in, shift_in, dt_bias, a_log, d_skip, gain_out)
        mixed = mixed_f.astype(jnp.bfloat16)
        block_rows = (residual + jnp.dot(mixed, w_out, preferred_element_type=jnp.float32)).astype(jnp.bfloat16)
        grad_mixed = jnp.dot(grad_rows, w_out.T, preferred_element_type=jnp.float32)
        grad_proj, grad_kernel, grad_shift, grad_offset, grad_rate, grad_skip, grad_gate = mixer_back(grad_mixed)
        proj_back = grad_proj.astype(jnp.bfloat16)
        grad_normed = jnp.dot(proj_back, w_in.T, preferred_element_type=jnp.float32)
        grad_unit = grad_normed * gain_in
        grad_input = grad_rows.astype(jnp.float32) + rstd_rows * (grad_unit - unit_rows * lax.optimization_barrier(jnp.mean(grad_unit * unit_rows, axis=-1, keepdims=True)))
        updated = (totals[0] + lax.optimization_barrier(jnp.sum(grad_normed * unit_rows, axis=0)), totals[1] + jnp.dot(normed.T, proj_back, preferred_element_type=jnp.float32), totals[2] + grad_kernel, totals[3] + grad_shift, totals[4] + grad_offset, totals[5] + grad_rate, totals[6] + grad_skip, totals[7] + grad_gate, totals[8] + jnp.dot(mixed.T, grad_rows, preferred_element_type=jnp.float32))
        return (updated, (block_rows, grad_input))
    initial = (jnp.zeros((D,), jnp.float32), jnp.zeros((D, PROJ), jnp.float32), jnp.zeros((CONV, CONVDIM), jnp.float32), jnp.zeros((CONVDIM,), jnp.float32), jnp.zeros((H,), jnp.float32), jnp.zeros((H,), jnp.float32), jnp.zeros((H,), jnp.float32), jnp.zeros((DI,), jnp.float32), jnp.zeros((DI, D), jnp.float32))
    totals, stacked = lax.scan(one_sequence, initial, (tokens, segments, cotangent))
    return (stacked[0], stacked[1], totals[0], totals[1], totals[2], totals[3], totals[4], totals[5], totals[6], totals[7], totals[8])
```

```python
import functools

import jax
import jax.numpy as jnp
from jax import lax
from jax.experimental import pallas as pl
from jax.experimental.pallas import tpu as pltpu
from jax.sharding import PartitionSpec as P

f32, bf16 = jnp.float32, jnp.bfloat16
highest = lax.Precision.HIGHEST
epsilon = 1e-05
LANES = 128
BLOCK = 128
GROUP = 512
PAIRS = GROUP // LANES
NT = (((1,), (1,)), ((), ()))
NN = (((1,), (0,)), ((), ()))


def dot(a, b, dims=NN, precision=None):
    return lax.dot_general(a, b, dims, precision=precision, preferred_element_type=f32)


def sigmoid(v):
    return 0.5 + 0.5 * jnp.tanh(0.5 * v)


def conv_taps(xin, masks):
    taps = []
    for shift in (3, 2, 1):
        taps.append(pltpu.roll(xin, shift, 0) * masks[3 - shift])
    taps.append(xin)
    return taps


def conv_sum(taps, cw):
    total = cw[4:5, :] + cw[3:4, :] * taps[3]
    for k in range(3):
        total = total + cw[k : k + 1, :] * taps[k]
    return total


def conv_back(gsum, xin, cw, masks, length):
    grads = []
    gx = cw[3:4, :] * gsum
    for shift in (3, 2, 1):
        masked = gsum * masks[3 - shift]
        grads.append(jnp.sum(masked * pltpu.roll(xin, shift, 0), axis=0, keepdims=True))
        gx = gx + cw[3 - shift : 4 - shift, :] * pltpu.roll(masked, length - shift, 0)
    grads.append(jnp.sum(gsum * xin, axis=0, keepdims=True))
    grads.append(jnp.sum(gsum, axis=0, keepdims=True))
    return gx, grads


def prologue(heads, bc_ref, dtr_ref, segc_ref, segr_ref, cwbc_ref, hp_ref, mask_s, b_s, c_s, dt_s, cum_s, cumt_s, ef_s, la_s, sp_s):
    length = bc_ref.shape[0]
    segc = segc_ref[0]
    for j in range(3):
        mask_s[2 - j] = jnp.broadcast_to(segc[:, j + 1 : j + 2], (length, LANES))
    masks = [mask_s[k] for k in range(3)]
    for half, ref in ((0, b_s), (1, c_s)):
        sl = slice(half * LANES, (half + 1) * LANES)
        taps = conv_taps(bc_ref[:, sl], masks)
        summed = conv_sum(taps, cwbc_ref[:, sl])
        ref[...] = summed * sigmoid(summed)
    lane = lax.broadcasted_iota(jnp.int32, (length, LANES), 1)
    raw = jnp.where(lane < heads, dtr_ref[...] + hp_ref[0:1, :], 0.0)
    soft = jnp.maximum(raw, 0.0) + jnp.log1p(jnp.exp(-jnp.abs(raw)))
    dt = jnp.where(lane < heads, soft, 0.0)
    la = -dt * jnp.exp(hp_ref[1:2, :])
    row = lax.broadcasted_iota(jnp.int32, (length, length), 0)
    col = lax.broadcasted_iota(jnp.int32, (length, length), 1)
    tri = jnp.where(row >= col, 1.0, 0.0).astype(f32)
    cum = dot(tri, la, precision=highest)
    dt_s[...] = dt
    la_s[...] = la
    cum_s[...] = cum
    cumt_s[...] = cum.T
    sp_s[...] = sigmoid(raw)
    mid = cum[BLOCK - 1 : BLOCK, :]
    ef_s[:BLOCK] = jnp.exp(jnp.minimum(mid - cum[:BLOCK], 0.0))
    ef_s[BLOCK:] = jnp.exp(jnp.minimum(cum[BLOCK:] - mid, 0.0))
    same = (segc[:, 0:1] == segr_ref[0, 0:1, :]).astype(f32)
    return row, col, same


def headpick(first, shape):
    source = lax.broadcasted_iota(jnp.int32, shape, 0) // 64
    target = lax.broadcasted_iota(jnp.int32, shape, 1)
    source = source - 2 * (source // 2)
    return jnp.where(target == source + first, 1.0, 0.0).astype(bf16)


def headsum(value, pick):
    hi = value.astype(bf16)
    lo = (value - hi.astype(f32)).astype(bf16)
    return dot(jnp.concatenate([hi, lo], axis=1), pick)


def fwd_kernel(heads, z_ref, x_ref, bc_ref, dtr_ref, gm_ref, segc_ref, segr_ref, cwx_ref, cwbc_ref, hp_ref, cp_ref,
               mixed_ref, gz_ref, gy_ref, rs_ref, gg_ref,
               mask_s, b_s, c_s, dt_s, cum_s, cumt_s, ef_s, la_s, sp_s, sm_s, ssm_s, yd_s, u_s, st_s, rs_s):
    phase, group = pl.program_id(1), pl.program_id(2)
    length = z_ref.shape[0]
    lane = lax.broadcasted_iota(jnp.int32, (length, LANES), 1)
    first = lane < 64
    half = lax.broadcasted_iota(jnp.int32, (BLOCK, LANES), 1) < 64

    @pl.when((phase == 0) & (group == 0))
    def _():
        row, col, same = prologue(heads, bc_ref, dtr_ref, segc_ref, segr_ref, cwbc_ref, hp_ref, mask_s, b_s, c_s, dt_s, cum_s, cumt_s, ef_s, la_s, sp_s)
        scores = dot(c_s[...], b_s[...], NT, precision=highest)
        sm_s[...] = jnp.where(row >= col, scores * same, 0.0)
        st_s[...] = jnp.zeros_like(st_s)

    width = jnp.int32(8)
    shift = lax.rem(jnp.int32(LANES) - width * group, jnp.int32(LANES))

    @pl.when(phase == 0)
    def _():
        masks = [mask_s[k] for k in range(3)]
        dtg = pltpu.roll(dt_s[...], shift, 1)
        cumg = pltpu.roll(cum_s[...], shift, 1)
        efg = pltpu.roll(ef_s[...], shift, 1)
        cumt = cumt_s[pl.ds(pl.multiple_of(group * 8, 8), 8), :]
        square, across = st_s[0], st_s[1]
        for j in range(PAIRS):
            sl = slice(j * LANES, (j + 1) * LANES)
            place = pl.ds(pl.multiple_of(group * GROUP + j * LANES, LANES), LANES)
            xin = x_ref[:, sl]
            summed = conv_sum(conv_taps(xin, masks), cwx_ref[:, sl])
            xs = summed * sigmoid(summed)
            dtb = jnp.where(first, dtg[:, 2 * j : 2 * j + 1], dtg[:, 2 * j + 1 : 2 * j + 2])
            efb = jnp.where(first, efg[:, 2 * j : 2 * j + 1], efg[:, 2 * j + 1 : 2 * j + 2])
            xd = xs * dtb
            for i in range(2):
                rows = slice(i * BLOCK, (i + 1) * BLOCK)
                part = xd[rows]
                stack = jnp.concatenate([jnp.where(half, part, 0.0), jnp.where(half, 0.0, part)], axis=0).astype(bf16)
                decays = []
                for h in range(2):
                    arg = cumg[rows, 2 * j + h : 2 * j + h + 1] - cumt[2 * j + h : 2 * j + h + 1, rows]
                    decays.append((jnp.exp(jnp.minimum(arg, 0.0)) * sm_s[rows, rows]).astype(bf16))
                yd_s[rows, place] = dot(jnp.concatenate(decays, axis=1), stack)
            far = (xd[:BLOCK] * efb[:BLOCK]).astype(bf16)
            u = dot(sm_s[BLOCK:, :BLOCK].astype(bf16), far)
            u_s[:, place] = u
            base = yd_s[:, place] + cp_ref[0:1, sl] * xs
            ssm = jnp.concatenate([base[:BLOCK], base[BLOCK:] + efb[BLOCK:] * u], axis=0)
            ssm_s[:, place] = ssm
            zin = z_ref[:, sl]
            gated = ssm * (zin * sigmoid(zin))
            square = square + gated * gated
            across = across + gm_ref[:, sl] * cp_ref[1:2, sl] * gated
        st_s[0] = square
        st_s[1] = across

    @pl.when((phase == 1) & (group == 0))
    def _():
        inner = heads * 64
        mean = jnp.sum(st_s[0], axis=1, keepdims=True) / inner
        scale = lax.rsqrt(mean + epsilon)
        inward = jnp.sum(st_s[1], axis=1, keepdims=True) / inner
        st_s[0] = jnp.broadcast_to(scale, (length, LANES))
        st_s[1] = jnp.broadcast_to(scale * scale * scale * inward, (length, LANES))
        rs_s[...] = jnp.zeros_like(rs_s)

    @pl.when(phase == 1)
    def _():
        scale, lean = st_s[0], st_s[1]
        efg = pltpu.roll(ef_s[...], shift, 1)
        total = rs_s[...]
        for j in range(PAIRS):
            sl = slice(j * LANES, (j + 1) * LANES)
            place = pl.ds(pl.multiple_of(group * GROUP + j * LANES, LANES), LANES)
            zin = z_ref[:, sl]
            sg = sigmoid(zin)
            silu = zin * sg
            dsilu = sg + silu * (1.0 - sg)
            ssm = ssm_s[:, place]
            gated = ssm * silu
            unit = gated * scale
            gain = cp_ref[1:2, sl]
            gm = gm_ref[:, sl]
            mixed_ref[:, sl] = (unit * gain).astype(bf16)
            gg_ref[0, :, sl] = jnp.broadcast_to(jnp.sum(gm * unit, axis=0, keepdims=True), (8, LANES))
            ggated = scale * (gm * gain) - gated * lean
            gz_ref[:, sl] = (ggated * ssm * dsilu).astype(bf16)
            gy = ggated * silu
            gy_ref[:, sl] = gy
            efb = jnp.where(first, efg[:, 2 * j : 2 * j + 1], efg[:, 2 * j + 1 : 2 * j + 2])
            near = gy.astype(bf16).astype(f32) * yd_s[:, place]
            fare = (gy[BLOCK:] * efb[BLOCK:]).astype(bf16).astype(f32) * u_s[:, place]
            value = jnp.concatenate([near[:BLOCK], near[BLOCK:] + fare], axis=0)
            total = total + headsum(value, headpick(8 * group + 2 * j, (2 * LANES, LANES)))
        rs_s[...] = total
        rs_ref[0] = total


def bwd_kernel(heads, x_ref, bc_ref, dtr_ref, gy_ref, rs_ref, segc_ref, segr_ref, cwx_ref, cwbc_ref, hp_ref, cp_ref,
               px_ref, pr_ref, gp_ref, gbc_ref, gh_ref,
               mask_s, b_s, c_s, dt_s, cum_s, cumt_s, ef_s, la_s, sp_s, smt_s, gst_s, gc_s, gd_s):
    group = pl.program_id(1)
    length = x_ref.shape[0]
    lane = lax.broadcasted_iota(jnp.int32, (length, LANES), 1)
    first = lane < 64
    half = lax.broadcasted_iota(jnp.int32, (BLOCK, LANES), 1) < 64

    @pl.when(group == 0)
    def _():
        row, col, same = prologue(heads, bc_ref, dtr_ref, segc_ref, segr_ref, cwbc_ref, hp_ref, mask_s, b_s, c_s, dt_s, cum_s, cumt_s, ef_s, la_s, sp_s)
        scores = dot(b_s[...], c_s[...], NT, precision=highest)
        smt_s[...] = jnp.where(row <= col, scores * same, 0.0)
        gst_s[...] = jnp.zeros_like(gst_s)
        gc_s[...] = jnp.zeros_like(gc_s)
        gd_s[...] = jnp.zeros_like(gd_s)

    shift = lax.rem(jnp.int32(LANES) - jnp.int32(8) * group, jnp.int32(LANES))
    masks = [mask_s[k] for k in range(3)]
    dtg = pltpu.roll(dt_s[...], shift, 1)
    cumg = pltpu.roll(cum_s[...], shift, 1)
    efg = pltpu.roll(ef_s[...], shift, 1)
    cumt = cumt_s[pl.ds(pl.multiple_of(group * 8, 8), 8), :]
    gcum, gdir = gc_s[...], gd_s[...]
    for j in range(PAIRS):
        sl = slice(j * LANES, (j + 1) * LANES)
        xin = x_ref[:, sl]
        cw = cwx_ref[:, sl]
        summed = conv_sum(conv_taps(xin, masks), cw)
        sg = sigmoid(summed)
        xs = summed * sg
        dtb = jnp.where(first, dtg[:, 2 * j : 2 * j + 1], dtg[:, 2 * j + 1 : 2 * j + 2])
        efb = jnp.where(first, efg[:, 2 * j : 2 * j + 1], efg[:, 2 * j + 1 : 2 * j + 2])
        xd = xs * dtb
        gy = gy_ref[:, sl]
        gyb = gy.astype(bf16)
        inner = []
        for i in range(2):
            rows = slice(i * BLOCK, (i + 1) * BLOCK)
            part, gpart = xd[rows], gy[rows]
            stack = jnp.concatenate([jnp.where(half, part, 0.0), jnp.where(half, 0.0, part)], axis=0).astype(bf16)
            gstack = jnp.concatenate([jnp.where(half, gpart, 0.0), jnp.where(half, 0.0, gpart)], axis=0).astype(bf16)
            gw = dot(stack, gyb[rows], NT)
            weights = []
            gscore = gst_s[rows, rows]
            for h in range(2):
                arg = cumt[2 * j + h : 2 * j + h + 1, rows] - cumg[rows, 2 * j + h : 2 * j + h + 1]
                decay = jnp.exp(jnp.minimum(arg, 0.0))
                weights.append((decay * smt_s[rows, rows]).astype(bf16))
                gscore = gscore + gw[h * BLOCK : (h + 1) * BLOCK] * decay
            gst_s[rows, rows] = gscore
            inner.append(dot(jnp.concatenate(weights, axis=1), gstack))
        far = (xd[:BLOCK] * efb[:BLOCK]).astype(bf16)
        ge = (gy[BLOCK:] * efb[BLOCK:]).astype(bf16)
        gst_s[:BLOCK, BLOCK:] += dot(far, ge, NT)
        gfar = dot(smt_s[:BLOCK, BLOCK:].astype(bf16), ge)
        xdb = xd.astype(bf16).astype(f32)
        fall0 = xdb[:BLOCK] * inner[0] + far.astype(f32) * gfar
        fall = jnp.concatenate([fall0, xdb[BLOCK:] * inner[1]], axis=0)
        gxd = jnp.concatenate([inner[0] + efb[:BLOCK] * gfar, inner[1]], axis=0)
        sums = headsum(jnp.concatenate([fall, xs * gxd], axis=0), headpick(8 * group + 2 * j, (2 * LANES, LANES)))
        gcum = gcum - sums[:length]
        gdir = gdir + sums[length:]
        gxs = cp_ref[0:1, sl] * gy + dtb * gxd
        gsum = gxs * (sg + xs * (1.0 - sg))
        gx, grads = conv_back(gsum, xin, cw, masks, length)
        px_ref[:, sl] = gx.astype(bf16)
        grads.append(jnp.sum(gy * xs, axis=0, keepdims=True))
        for k, value in enumerate(grads):
            gp_ref[0, k : k + 1, sl] = value
        gp_ref[0, 6:8, sl] = jnp.zeros((2, LANES), f32)
    gc_s[...] = gcum
    gd_s[...] = gdir

    @pl.when(group == pl.num_programs(1) - 1)
    def _():
        row = lax.broadcasted_iota(jnp.int32, (length, length), 0)
        col = lax.broadcasted_iota(jnp.int32, (length, length), 1)
        same = segc_ref[0][:, 0:1] == segr_ref[0, 0:1, :]
        gscore = jnp.where((row <= col) & same, gst_s[...], 0.0)
        backs = (dot(gscore, c_s[...], precision=highest), dot(gscore.T, b_s[...], precision=highest))
        for part in range(2):
            sl = slice(part * LANES, (part + 1) * LANES)
            xin = bc_ref[:, sl]
            cw = cwbc_ref[:, sl]
            summed = conv_sum(conv_taps(xin, masks), cw)
            sg = sigmoid(summed)
            gsum = backs[part] * (sg + summed * sg * (1.0 - sg))
            gx, grads = conv_back(gsum, xin, cw, masks, length)
            pr_ref[:, sl] = gx.astype(bf16)
            for k, value in enumerate(grads):
                gbc_ref[0, k : k + 1, sl] = value
            gbc_ref[0, 5:8, sl] = jnp.zeros((3, LANES), f32)
        upper = jnp.where(row <= col, 1.0, 0.0).astype(f32)
        gla = dot(upper, gc_s[...] + rs_ref[0], precision=highest)
        graw = (gd_s[...] - gla * jnp.exp(hp_ref[1:2, :])) * sp_s[...]
        graw = jnp.where(lane < heads, graw, 0.0)
        pr_ref[:, 2 * LANES :] = graw.astype(bf16)
        gh_ref[0, 0:1] = jnp.sum(graw, axis=0, keepdims=True)
        gh_ref[0, 1:2] = jnp.sum(jnp.where(lane < heads, gla * la_s[...], 0.0), axis=0, keepdims=True)
        gh_ref[0, 2:8] = jnp.zeros((6, LANES), f32)


def small_scratch(length):
    return [
        pltpu.VMEM((3, length, LANES), f32),
        pltpu.VMEM((length, LANES), f32),
        pltpu.VMEM((length, LANES), f32),
        pltpu.VMEM((length, LANES), f32),
        pltpu.VMEM((length, LANES), f32),
        pltpu.VMEM((LANES, length), f32),
        pltpu.VMEM((length, LANES), f32),
        pltpu.VMEM((length, LANES), f32),
        pltpu.VMEM((length, LANES), f32),
    ]


def mixer_forward(projected, gm, segc, segr, cw, hp, cp, heads, state):
    seqs, length = segc.shape[:2]
    inner = gm.shape[1]
    groups = inner // GROUP
    rows = seqs * length
    kernel = functools.partial(fwd_kernel, heads)
    out_row = lambda b, p, g: (b, g * p)
    return pl.pallas_call(
        kernel,
        grid=(seqs, 2, groups),
        in_specs=[
            pl.BlockSpec((length, GROUP), lambda b, p, g: (b, g)),
            pl.BlockSpec((length, GROUP), lambda b, p, g: (b, groups + g * (1 - p) + (groups - 1) * p)),
            pl.BlockSpec((length, 2 * state), lambda b, p, g: (b, 2 * inner // (2 * state))),
            pl.BlockSpec((length, LANES), lambda b, p, g: (b, (2 * inner + 2 * state) // LANES)),
            pl.BlockSpec((length, GROUP), lambda b, p, g: (b, g)),
            pl.BlockSpec((1, length, LANES), lambda b, p, g: (b, 0, 0)),
            pl.BlockSpec((1, 8, length), lambda b, p, g: (b, 0, 0)),
            pl.BlockSpec((8, GROUP), lambda b, p, g: (0, g)),
            pl.BlockSpec((8, 2 * state), lambda b, p, g: (0, inner // (2 * state))),
            pl.BlockSpec((8, LANES), lambda b, p, g: (0, 0)),
            pl.BlockSpec((8, GROUP), lambda b, p, g: (0, g)),
        ],
        out_specs=[
            pl.BlockSpec((length, GROUP), out_row),
            pl.BlockSpec((length, GROUP), out_row),
            pl.BlockSpec((length, GROUP), out_row),
            pl.BlockSpec((1, length, LANES), lambda b, p, g: (b, 0, 0)),
            pl.BlockSpec((1, 8, GROUP), lambda b, p, g: (b, 0, g * p)),
        ],
        out_shape=[
            jax.ShapeDtypeStruct((rows, inner), bf16),
            jax.ShapeDtypeStruct((rows, inner), bf16),
            jax.ShapeDtypeStruct((rows, inner), f32),
            jax.ShapeDtypeStruct((seqs, length, LANES), f32),
            jax.ShapeDtypeStruct((seqs, 8, inner), f32),
        ],
        scratch_shapes=small_scratch(length) + [
            pltpu.VMEM((length, length), f32),
            pltpu.VMEM((length, inner), f32),
            pltpu.VMEM((length, inner), f32),
            pltpu.VMEM((length - BLOCK, inner), f32),
            pltpu.VMEM((2, length, LANES), f32),
            pltpu.VMEM((length, LANES), f32),
        ],
        compiler_params=pltpu.CompilerParams(vmem_limit_bytes=48 << 20),
        cost_estimate=pl.CostEstimate(flops=10**10, bytes_accessed=45 * 10**6, transcendentals=10**7),
        name="mixer_forward",
    )(projected, projected, projected, projected, gm, segc, segr, cw, cw, hp, cp)


def mixer_backward(projected, gy, rs, segc, segr, cw, hp, cp, heads, state):
    seqs, length = segc.shape[:2]
    inner = gy.shape[1]
    groups = inner // GROUP
    rows = seqs * length
    kernel = functools.partial(bwd_kernel, heads)
    return pl.pallas_call(
        kernel,
        grid=(seqs, groups),
        in_specs=[
            pl.BlockSpec((length, GROUP), lambda b, g: (b, groups + g)),
            pl.BlockSpec((length, 2 * state), lambda b, g: (b, 2 * inner // (2 * state))),
            pl.BlockSpec((length, LANES), lambda b, g: (b, (2 * inner + 2 * state) // LANES)),
            pl.BlockSpec((length, GROUP), lambda b, g: (b, g)),
            pl.BlockSpec((1, length, LANES), lambda b, g: (b, 0, 0)),
            pl.BlockSpec((1, length, LANES), lambda b, g: (b, 0, 0)),
            pl.BlockSpec((1, 8, length), lambda b, g: (b, 0, 0)),
            pl.BlockSpec((8, GROUP), lambda b, g: (0, g)),
            pl.BlockSpec((8, 2 * state), lambda b, g: (0, inner // (2 * state))),
            pl.BlockSpec((8, LANES), lambda b, g: (0, 0)),
            pl.BlockSpec((8, GROUP), lambda b, g: (0, g)),
        ],
        out_specs=[
            pl.BlockSpec((length, GROUP), lambda b, g: (b, g)),
            pl.BlockSpec((length, 3 * LANES), lambda b, g: (b, 0)),
            pl.BlockSpec((1, 8, GROUP), lambda b, g: (b, 0, g)),
            pl.BlockSpec((1, 8, 2 * state), lambda b, g: (b, 0, 0)),
            pl.BlockSpec((1, 8, LANES), lambda b, g: (b, 0, 0)),
        ],
        out_shape=[
            jax.ShapeDtypeStruct((rows, inner), bf16),
            jax.ShapeDtypeStruct((rows, 3 * LANES), bf16),
            jax.ShapeDtypeStruct((seqs, 8, inner), f32),
            jax.ShapeDtypeStruct((seqs, 8, 2 * state), f32),
            jax.ShapeDtypeStruct((seqs, 8, LANES), f32),
        ],
        scratch_shapes=small_scratch(length) + [
            pltpu.VMEM((length, length), f32),
            pltpu.VMEM((length, length), f32),
            pltpu.VMEM((length, LANES), f32),
            pltpu.VMEM((length, LANES), f32),
        ],
        compiler_params=pltpu.CompilerParams(vmem_limit_bytes=48 << 20),
        cost_estimate=pl.CostEstimate(flops=10**10, bytes_accessed=30 * 10**6, transcendentals=10**7),
        name="mixer_backward",
    )(projected, projected, projected, gy, rs, segc, segr, cw, cw, hp, cp)


def pad_lanes(v, width=LANES):
    return jnp.pad(v, ((0, 0), (0, width - v.shape[1])))


def mixer_tables(segments, kernel_full, shift_full, dt_bias, a_log, d_skip, gate_full):
    taps = kernel_full.shape[0]
    seqs, length = segments.shape
    columns = [segments.astype(f32)]
    where = jnp.arange(length)[None, :]
    for j in range(1, taps):
        before = jnp.pad(segments, ((0, 0), (j, 0)))[:, :length]
        columns.append(((before == segments) & (where >= j)).astype(f32))
    segc = jnp.pad(jnp.stack(columns, axis=-1), ((0, 0), (0, 0), (0, LANES - taps)))
    segr = jnp.broadcast_to(segments.astype(f32)[:, None, :], (seqs, 8, length))
    cw = jnp.concatenate([kernel_full.astype(f32), jnp.broadcast_to(shift_full.astype(f32)[None], (8 - taps, shift_full.shape[0]))])
    hp = pad_lanes(jnp.concatenate([dt_bias[None], jnp.broadcast_to(a_log[None], (7, a_log.shape[0]))]))
    heads = dt_bias.shape[0]
    size = gate_full.shape[0] // heads
    cp = jnp.concatenate([jnp.repeat(d_skip, size)[None], jnp.broadcast_to(gate_full.astype(f32)[None], (7, gate_full.shape[0]))])
    return segc, segr, cw, hp, cp


MESH = pl.DeviceIdType.MESH
PIECES = 3


def ring_place(chip, chips):
    wide = chips // 4
    z, q = chip // wide, chip % wide
    up = 1 + 3 * q + jnp.where(q % 2 == 0, z - 1, 3 - z)
    back = jnp.where(q == 0, 0, 4 * wide - q)
    return jnp.where(z == 0, back, up)


def ring_chip(place, chips):
    wide = chips // 4
    place = place % chips
    q = (place - 1 + chips) % chips // 3
    r = (place - 1 + chips) % chips % 3
    z = jnp.where(q % 2 == 0, 1 + r, 3 - r)
    inner = z * wide + q
    outer = (4 * wide - place) % (4 * wide)
    return jnp.where((place == 0) | (place > 3 * wide), outer, inner)


def gather_kernel(chips, count, *refs):
    ins, outs = refs[:count], refs[count : 2 * count]
    ring_send, ring_recv, far_send, far_recv, pair_send, pair_recv, own_sem = refs[2 * count :]
    me = lax.axis_index("fsdp")
    plane = lax.axis_index("dp")
    chip, core = me // 2, me % 2
    place = ring_place(chip, chips)
    right = 2 * ring_chip(place + 1, chips) + core
    left = 2 * ring_chip(place + chips - 1, chips) + core
    pair = {"fsdp": me + 1 - 2 * core}
    peer = {"dp": 1 - plane}
    ways = ({"fsdp": right}, {"fsdp": left})

    barrier = pltpu.get_barrier_semaphore()
    for other in (ways[0], ways[1], pair, peer):
        pl.semaphore_signal(barrier, inc=1, device_id=other, device_id_type=MESH)
    pl.semaphore_wait(barrier, 4)

    half = chips // 2
    whole = [k == count - 1 for k in range(count)]

    def steps(way, slot):
        return half if way == slot else half - 1

    def owner(way, step):
        move = -step if way == 0 else step
        return 2 * ring_chip(place + move + chips, chips) + core

    def part(refs, k, index, slot):
        if whole[k]:
            return refs[k].at[index]
        piece = 0 if slot == 0 else 1 + plane
        return refs[k].at[index, piece]

    def mine(k, slot):
        if whole[k]:
            return ins[k]
        piece = 0 if slot == 0 else 1 + plane
        return ins[k].at[piece]

    def slots(k):
        return (0,) if whole[k] else (0, 1)

    pending = []

    def send(source, target, send_sem, recv_sem, device):
        copy = pltpu.make_async_remote_copy(
            src_ref=source, dst_ref=target, send_sem=send_sem, recv_sem=recv_sem, device_id=device, device_id_type=MESH)
        copy.start()
        pending.append(copy)

    def arrived(target, send_sem, recv_sem):
        pltpu.make_async_remote_copy(
            src_ref=target, dst_ref=target, send_sem=send_sem, recv_sem=recv_sem, device_id=pair, device_id_type=MESH).wait_recv()

    def ring_sem(sem, way, step, k, slot):
        return sem.at[(way * half + step - 1) * 2 * count + 2 * k + slot]

    def far_sem(sem, way, step, k):
        return sem.at[(way * half + step - 1) * count + k]

    def pair_sem(sem, turn, k, slot):
        return sem.at[(turn * count + k) * 3 + slot]

    def turn(way, step):
        return 1 + (step - 1) * 2 + way

    local = []
    for k in range(count):
        for slot in slots(k):
            for way in range(2):
                send(mine(k, slot), part(outs, k, me, slot), ring_sem(ring_send, way, 1, k, slot), ring_sem(ring_recv, way, 1, k, slot), ways[way])
        send(ins[k], outs[k].at[me], pair_sem(pair_send, 0, k, 0), pair_sem(pair_recv, 0, k, 0), pair)
        copy = pltpu.make_async_copy(ins[k], outs[k].at[me], own_sem.at[k])
        copy.start()
        local.append(copy)

    def from_peer(way, step):
        index = owner(way, step)
        for k in range(count):
            if whole[k] or step > steps(way, 1):
                continue
            target = outs[k].at[index, 2 - plane]
            arrived(target, far_sem(far_send, way, step, k), far_sem(far_recv, way, step, k))
            send(target, target, pair_sem(pair_send, turn(way, step), k, 2), pair_sem(pair_recv, turn(way, step), k, 2), pair)

    for step in range(1, half + 1):
        for way in range(2):
            index = owner(way, step)
            for k in range(count):
                for slot in slots(k):
                    if step > steps(way, slot):
                        continue
                    target = part(outs, k, index, slot)
                    arrived(target, ring_sem(ring_send, way, step, k, slot), ring_sem(ring_recv, way, step, k, slot))
                    if step + 1 <= steps(way, slot):
                        send(target, target, ring_sem(ring_send, way, step + 1, k, slot), ring_sem(ring_recv, way, step + 1, k, slot), ways[way])
                    if slot == 1:
                        send(target, target, far_sem(far_send, way, step, k), far_sem(far_recv, way, step, k), peer)
                    send(target, target, pair_sem(pair_send, turn(way, step), k, slot), pair_sem(pair_recv, turn(way, step), k, slot), pair)
        if step > 1:
            for way in range(2):
                from_peer(way, step - 1)
    for way in range(2):
        from_peer(way, half)
    for k in range(count):
        other = outs[k].at[me + 1 - 2 * core]
        arrived(other, pair_sem(pair_send, 0, k, 0), pair_sem(pair_recv, 0, k, 0))
    for step in range(1, half + 1):
        for way in range(2):
            index = owner(way, step) + 1 - 2 * core
            for k in range(count):
                for slot in slots(k) + (() if whole[k] else (2,)):
                    if step > steps(way, min(slot, 1)):
                        continue
                    if slot == 2:
                        target = outs[k].at[index, 2 - plane]
                    else:
                        target = part(outs, k, index, slot)
                    sems = turn(way, step), k, slot
                    arrived(target, pair_sem(pair_send, *sems), pair_sem(pair_recv, *sems))
    for copy in local:
        copy.wait()
    for copy in pending:
        copy.wait_send()


def gather(arrays, devices):
    count = len(arrays)
    chips = devices // 2
    half = chips // 2
    dma = pltpu.SemaphoreType.DMA
    return pl.pallas_call(
        functools.partial(gather_kernel, chips, count),
        in_specs=[pl.BlockSpec(memory_space=pl.ANY)] * count,
        out_specs=[pl.BlockSpec(memory_space=pl.ANY)] * count,
        out_shape=[jax.ShapeDtypeStruct((devices,) + a.shape, a.dtype) for a in arrays],
        scratch_shapes=[
            dma((4 * half * count,)), dma((4 * half * count,)),
            dma((2 * half * count,)), dma((2 * half * count,)),
            dma(((2 * half + 1) * count * 3,)), dma(((2 * half + 1) * count * 3,)),
            dma((count,)),
        ],
        compiler_params=pltpu.CompilerParams(collective_id=0, has_side_effects=True),
        name="gather_weights",
    )(*arrays)


def small_rows(size):
    return 16 * (-(-size // (16 * LANES)))


def flat_pack(parts, rows):
    flat = jnp.concatenate([p.reshape(-1) for p in parts])
    return jnp.pad(flat, (0, rows * LANES - flat.shape[0])).reshape(rows, LANES)


def local(devices, tokens, segments, norm_gain, w_in, conv_weight, conv_bias, dt_bias, a_log, d_skip, gate_gain, w_out, cotangent):
    seqs, length, width = tokens.shape
    rows = seqs * length
    proj_width = w_in.shape[1]
    inner = devices * w_out.shape[0]
    taps = conv_weight.shape[0]
    heads = dt_bias.shape[0]
    share_n, share_c, share_g = norm_gain.shape[0], conv_bias.shape[0], gate_gain.shape[0]
    conv_width = devices * share_c
    state = (conv_width - inner) // 2

    size = share_n + share_g + (taps + 1) * share_c
    pack = flat_pack([norm_gain, gate_gain, conv_weight, conv_bias], small_rows(size))
    win_all, wout_all, pack_all = gather(
        [w_in.reshape(PIECES, -1, proj_width), w_out.reshape(PIECES, -1, width), pack], devices)
    w_in_full = win_all.reshape(width, proj_width)
    w_out_full = wout_all.reshape(inner, width)
    pack_all = pack_all.reshape(devices, -1)
    cuts = [share_n, share_n + share_g, share_n + share_g + taps * share_c, size]
    gain_full = pack_all[:, : cuts[0]].reshape(width)
    gate_full = pack_all[:, cuts[0] : cuts[1]].reshape(inner)
    kernel_full = pack_all[:, cuts[1] : cuts[2]].reshape(devices, taps, share_c).transpose(1, 0, 2).reshape(taps, conv_width)
    shift_full = pack_all[:, cuts[2] : cuts[3]].reshape(conv_width)

    residual = tokens.reshape(rows, width).astype(f32)
    rstd = lax.rsqrt(jnp.mean(residual * residual, axis=-1, keepdims=True) + epsilon)
    unit = residual * rstd
    gain_f = gain_full.astype(f32)
    normed = (unit * gain_f).astype(bf16)
    grad_rows = cotangent.reshape(rows, width)
    projected = dot(normed, w_in_full)
    gm = dot(grad_rows, w_out_full, NT)
    tables = mixer_tables(segments, kernel_full, shift_full, dt_bias, a_log, d_skip, gate_full)
    mixed, gz, gy, rs, gg = mixer_forward(projected, gm, *tables, heads, state)
    block_out = (residual + dot(mixed, w_out_full)).astype(bf16)
    grad_w_out = lax.dot_general(mixed, grad_rows, (((0,), (0,)), ((), ())), preferred_element_type=f32).astype(bf16)
    px, pr, gp, gbc, gh = mixer_backward(projected, gy, rs, *tables, heads, state)
    proj_back = jnp.concatenate([gz, px, pr[:, : 2 * state + heads]], axis=1)
    grad_normed = dot(proj_back, w_in_full, NT)
    grad_w_in = lax.dot_general(normed, proj_back, (((0,), (0,)), ((), ())), preferred_element_type=f32).astype(bf16)
    grad_norm = jnp.sum(grad_normed * unit, axis=0)
    grad_unit = grad_normed * gain_f
    grad_tokens = grad_rows.astype(f32) + rstd * (grad_unit - unit * jnp.mean(grad_unit * unit, axis=-1, keepdims=True))

    gp, gbc, gh = gp.sum(0), gbc.sum(0), gh.sum(0)
    grad_kernel = jnp.concatenate([gp[:taps], gbc[:taps]], axis=1)
    grad_shift = jnp.concatenate([gp[taps], gbc[taps]])
    grad_gate = gg[:, 0].sum(0)
    grad_skip = gp[taps + 1].reshape(heads, inner // heads).sum(1)

    small = jnp.concatenate([
        grad_norm.reshape(devices, share_n), grad_gate.reshape(devices, share_g),
        grad_kernel.reshape(taps, devices, share_c).transpose(1, 0, 2).reshape(devices, taps * share_c),
        grad_shift.reshape(devices, share_c)], axis=1)
    small = lax.psum_scatter(small, "fsdp", scatter_dimension=0, tiled=True)
    small = lax.psum(small, "dp")[0]
    head_grads = lax.psum(jnp.stack([gh[0, :heads], gh[1, :heads], grad_skip]), ("fsdp", "dp"))

    def owned(full):
        mine = lax.psum_scatter(full, "fsdp", scatter_dimension=0, tiled=True)
        other = lax.ppermute(mine, "dp", [(0, 1), (1, 0)])
        return mine.astype(f32) + other.astype(f32)

    return (
        block_out.reshape(seqs, length, width),
        grad_tokens.reshape(seqs, length, width),
        small[: cuts[0]],
        owned(grad_w_in),
        small[cuts[1] : cuts[2]].reshape(taps, share_c),
        small[cuts[2] : cuts[3]],
        head_grads[0],
        head_grads[1],
        head_grads[2],
        small[cuts[0] : cuts[1]],
        owned(grad_w_out),
    )


def solution(mesh):
    rows3, rows2 = P(("fsdp", "dp"), None, None), P(("fsdp", "dp"), None)
    return jax.shard_map(
        functools.partial(local, mesh.shape["fsdp"]),
        mesh=mesh,
        in_specs=(rows3, rows2, P("fsdp"), P("fsdp", None), P(None, "fsdp"), P("fsdp"), P(), P(), P(), P("fsdp"), P("fsdp", None), rows3),
        out_specs=(rows3, rows3, P("fsdp"), P("fsdp", None), P(None, "fsdp"), P("fsdp"), P(), P(), P(), P("fsdp"), P("fsdp", None)),
        check_vma=False,
    )
```

```python
import functools

import jax
import jax.numpy as jnp
from jax import lax
from jax.experimental import pallas as pl
from jax.experimental.pallas import tpu as pltpu
from jax.sharding import PartitionSpec as P

f32, bf16 = jnp.float32, jnp.bfloat16
highest = lax.Precision.HIGHEST
epsilon = 1e-05
LANES = 128
BLOCK = 128
GROUP = 512
PAIRS = GROUP // LANES
NT = (((1,), (1,)), ((), ()))
NN = (((1,), (0,)), ((), ()))


def dot(a, b, dims=NN, precision=None):
    return lax.dot_general(a, b, dims, precision=precision, preferred_element_type=f32)


def sigmoid(v):
    return 0.5 + 0.5 * jnp.tanh(0.5 * v)


def conv_taps(xin, masks):
    taps = []
    for shift in (3, 2, 1):
        taps.append(pltpu.roll(xin, shift, 0) * masks[3 - shift])
    taps.append(xin)
    return taps


def conv_sum(taps, cw):
    total = cw[4:5, :] + cw[3:4, :] * taps[3]
    for k in range(3):
        total = total + cw[k : k + 1, :] * taps[k]
    return total


def conv_back(gsum, xin, cw, masks, length):
    grads = []
    gx = cw[3:4, :] * gsum
    for shift in (3, 2, 1):
        masked = gsum * masks[3 - shift]
        grads.append(jnp.sum(masked * pltpu.roll(xin, shift, 0), axis=0, keepdims=True))
        gx = gx + cw[3 - shift : 4 - shift, :] * pltpu.roll(masked, length - shift, 0)
    grads.append(jnp.sum(gsum * xin, axis=0, keepdims=True))
    grads.append(jnp.sum(gsum, axis=0, keepdims=True))
    return gx, grads


def prologue(heads, bc_ref, dtr_ref, segc_ref, segr_ref, cwbc_ref, hp_ref, mask_s, b_s, c_s, dt_s, cum_s, cumt_s, ef_s, la_s, sp_s):
    length = bc_ref.shape[0]
    segc = segc_ref[0]
    for j in range(3):
        mask_s[2 - j] = jnp.broadcast_to(segc[:, j + 1 : j + 2], (length, LANES))
    masks = [mask_s[k] for k in range(3)]
    for half, ref in ((0, b_s), (1, c_s)):
        sl = slice(half * LANES, (half + 1) * LANES)
        taps = conv_taps(bc_ref[:, sl], masks)
        summed = conv_sum(taps, cwbc_ref[:, sl])
        ref[...] = summed * sigmoid(summed)
    lane = lax.broadcasted_iota(jnp.int32, (length, LANES), 1)
    raw = jnp.where(lane < heads, dtr_ref[...] + hp_ref[0:1, :], 0.0)
    soft = jnp.maximum(raw, 0.0) + jnp.log1p(jnp.exp(-jnp.abs(raw)))
    dt = jnp.where(lane < heads, soft, 0.0)
    la = -dt * jnp.exp(hp_ref[1:2, :])
    row = lax.broadcasted_iota(jnp.int32, (length, length), 0)
    col = lax.broadcasted_iota(jnp.int32, (length, length), 1)
    tri = jnp.where(row >= col, 1.0, 0.0).astype(f32)
    cum = dot(tri, la, precision=highest)
    dt_s[...] = dt
    la_s[...] = la
    cum_s[...] = cum
    cumt_s[...] = cum.T
    sp_s[...] = sigmoid(raw)
    mid = cum[BLOCK - 1 : BLOCK, :]
    ef_s[:BLOCK] = jnp.exp(jnp.minimum(mid - cum[:BLOCK], 0.0))
    ef_s[BLOCK:] = jnp.exp(jnp.minimum(cum[BLOCK:] - mid, 0.0))
    same = (segc[:, 0:1] == segr_ref[0, 0:1, :]).astype(f32)
    return row, col, same


def headpick(first, shape):
    source = lax.broadcasted_iota(jnp.int32, shape, 0) // 64
    target = lax.broadcasted_iota(jnp.int32, shape, 1)
    source = source - 2 * (source // 2)
    return jnp.where(target == source + first, 1.0, 0.0).astype(bf16)


def headsum(value, pick):
    hi = value.astype(bf16)
    lo = (value - hi.astype(f32)).astype(bf16)
    return dot(jnp.concatenate([hi, lo], axis=1), pick)


def fwd_kernel(heads, z_ref, x_ref, bc_ref, dtr_ref, gm_ref, segc_ref, segr_ref, cwx_ref, cwbc_ref, hp_ref, cp_ref,
               mixed_ref, gz_ref, gy_ref, rs_ref, gg_ref,
               mask_s, b_s, c_s, dt_s, cum_s, cumt_s, ef_s, la_s, sp_s, sm_s, ssm_s, yd_s, u_s, st_s, rs_s):
    phase, group = pl.program_id(1), pl.program_id(2)
    length = z_ref.shape[0]
    lane = lax.broadcasted_iota(jnp.int32, (length, LANES), 1)
    first = lane < 64
    half = lax.broadcasted_iota(jnp.int32, (BLOCK, LANES), 1) < 64

    @pl.when((phase == 0) & (group == 0))
    def _():
        row, col, same = prologue(heads, bc_ref, dtr_ref, segc_ref, segr_ref, cwbc_ref, hp_ref, mask_s, b_s, c_s, dt_s, cum_s, cumt_s, ef_s, la_s, sp_s)
        scores = dot(c_s[...], b_s[...], NT, precision=highest)
        sm_s[...] = jnp.where(row >= col, scores * same, 0.0)
        st_s[...] = jnp.zeros_like(st_s)

    width = jnp.int32(8)
    shift = lax.rem(jnp.int32(LANES) - width * group, jnp.int32(LANES))

    @pl.when(phase == 0)
    def _():
        masks = [mask_s[k] for k in range(3)]
        dtg = pltpu.roll(dt_s[...], shift, 1)
        cumg = pltpu.roll(cum_s[...], shift, 1)
        efg = pltpu.roll(ef_s[...], shift, 1)
        cumt = cumt_s[pl.ds(pl.multiple_of(group * 8, 8), 8), :]
        square, across = st_s[0], st_s[1]
        for j in range(PAIRS):
            sl = slice(j * LANES, (j + 1) * LANES)
            place = pl.ds(pl.multiple_of(group * GROUP + j * LANES, LANES), LANES)
            xin = x_ref[:, sl]
            summed = conv_sum(conv_taps(xin, masks), cwx_ref[:, sl])
            xs = summed * sigmoid(summed)
            dtb = jnp.where(first, dtg[:, 2 * j : 2 * j + 1], dtg[:, 2 * j + 1 : 2 * j + 2])
            efb = jnp.where(first, efg[:, 2 * j : 2 * j + 1], efg[:, 2 * j + 1 : 2 * j + 2])
            xd = xs * dtb
            for i in range(2):
                rows = slice(i * BLOCK, (i + 1) * BLOCK)
                part = xd[rows]
                stack = jnp.concatenate([jnp.where(half, part, 0.0), jnp.where(half, 0.0, part)], axis=0).astype(bf16)
                decays = []
                for h in range(2):
                    arg = cumg[rows, 2 * j + h : 2 * j + h + 1] - cumt[2 * j + h : 2 * j + h + 1, rows]
                    decays.append((jnp.exp(jnp.minimum(arg, 0.0)) * sm_s[rows, rows]).astype(bf16))
                yd_s[rows, place] = dot(jnp.concatenate(decays, axis=1), stack)
            far = (xd[:BLOCK] * efb[:BLOCK]).astype(bf16)
            u = dot(sm_s[BLOCK:, :BLOCK].astype(bf16), far)
            u_s[:, place] = u
            base = yd_s[:, place] + cp_ref[0:1, sl] * xs
            ssm = jnp.concatenate([base[:BLOCK], base[BLOCK:] + efb[BLOCK:] * u], axis=0)
            ssm_s[:, place] = ssm
            zin = z_ref[:, sl]
            gated = ssm * (zin * sigmoid(zin))
            square = square + gated * gated
            across = across + gm_ref[:, sl] * cp_ref[1:2, sl] * gated
        st_s[0] = square
        st_s[1] = across

    @pl.when((phase == 1) & (group == 0))
    def _():
        inner = heads * 64
        mean = jnp.sum(st_s[0], axis=1, keepdims=True) / inner
        scale = lax.rsqrt(mean + epsilon)
        inward = jnp.sum(st_s[1], axis=1, keepdims=True) / inner
        st_s[0] = jnp.broadcast_to(scale, (length, LANES))
        st_s[1] = jnp.broadcast_to(scale * scale * scale * inward, (length, LANES))
        rs_s[...] = jnp.zeros_like(rs_s)

    @pl.when(phase == 1)
    def _():
        scale, lean = st_s[0], st_s[1]
        efg = pltpu.roll(ef_s[...], shift, 1)
        total = rs_s[...]
        for j in range(PAIRS):
            sl = slice(j * LANES, (j + 1) * LANES)
            place = pl.ds(pl.multiple_of(group * GROUP + j * LANES, LANES), LANES)
            zin = z_ref[:, sl]
            sg = sigmoid(zin)
            silu = zin * sg
            dsilu = sg + silu * (1.0 - sg)
            ssm = ssm_s[:, place]
            gated = ssm * silu
            unit = gated * scale
            gain = cp_ref[1:2, sl]
            gm = gm_ref[:, sl]
            mixed_ref[:, sl] = (unit * gain).astype(bf16)
            gg_ref[0, :, sl] = jnp.broadcast_to(jnp.sum(gm * unit, axis=0, keepdims=True), (8, LANES))
            ggated = scale * (gm * gain) - gated * lean
            gz_ref[:, sl] = (ggated * ssm * dsilu).astype(bf16)
            gy = ggated * silu
            gy_ref[:, sl] = gy
            efb = jnp.where(first, efg[:, 2 * j : 2 * j + 1], efg[:, 2 * j + 1 : 2 * j + 2])
            near = gy.astype(bf16).astype(f32) * yd_s[:, place]
            fare = (gy[BLOCK:] * efb[BLOCK:]).astype(bf16).astype(f32) * u_s[:, place]
            value = jnp.concatenate([near[:BLOCK], near[BLOCK:] + fare], axis=0)
            total = total + headsum(value, headpick(8 * group + 2 * j, (2 * LANES, LANES)))
        rs_s[...] = total
        rs_ref[0] = total


def bwd_kernel(heads, x_ref, bc_ref, dtr_ref, gy_ref, rs_ref, segc_ref, segr_ref, cwx_ref, cwbc_ref, hp_ref, cp_ref,
               px_ref, pr_ref, gp_ref, gbc_ref, gh_ref,
               mask_s, b_s, c_s, dt_s, cum_s, cumt_s, ef_s, la_s, sp_s, smt_s, gst_s, gc_s, gd_s):
    group = pl.program_id(1)
    length = x_ref.shape[0]
    lane = lax.broadcasted_iota(jnp.int32, (length, LANES), 1)
    first = lane < 64
    half = lax.broadcasted_iota(jnp.int32, (BLOCK, LANES), 1) < 64

    @pl.when(group == 0)
    def _():
        row, col, same = prologue(heads, bc_ref, dtr_ref, segc_ref, segr_ref, cwbc_ref, hp_ref, mask_s, b_s, c_s, dt_s, cum_s, cumt_s, ef_s, la_s, sp_s)
        scores = dot(b_s[...], c_s[...], NT, precision=highest)
        smt_s[...] = jnp.where(row <= col, scores * same, 0.0)
        gst_s[...] = jnp.zeros_like(gst_s)
        gc_s[...] = jnp.zeros_like(gc_s)
        gd_s[...] = jnp.zeros_like(gd_s)

    shift = lax.rem(jnp.int32(LANES) - jnp.int32(8) * group, jnp.int32(LANES))
    masks = [mask_s[k] for k in range(3)]
    dtg = pltpu.roll(dt_s[...], shift, 1)
    cumg = pltpu.roll(cum_s[...], shift, 1)
    efg = pltpu.roll(ef_s[...], shift, 1)
    cumt = cumt_s[pl.ds(pl.multiple_of(group * 8, 8), 8), :]
    gcum, gdir = gc_s[...], gd_s[...]
    for j in range(PAIRS):
        sl = slice(j * LANES, (j + 1) * LANES)
        xin = x_ref[:, sl]
        cw = cwx_ref[:, sl]
        summed = conv_sum(conv_taps(xin, masks), cw)
        sg = sigmoid(summed)
        xs = summed * sg
        dtb = jnp.where(first, dtg[:, 2 * j : 2 * j + 1], dtg[:, 2 * j + 1 : 2 * j + 2])
        efb = jnp.where(first, efg[:, 2 * j : 2 * j + 1], efg[:, 2 * j + 1 : 2 * j + 2])
        xd = xs * dtb
        gy = gy_ref[:, sl]
        gyb = gy.astype(bf16)
        inner = []
        for i in range(2):
            rows = slice(i * BLOCK, (i + 1) * BLOCK)
            part, gpart = xd[rows], gy[rows]
            stack = jnp.concatenate([jnp.where(half, part, 0.0), jnp.where(half, 0.0, part)], axis=0).astype(bf16)
            gstack = jnp.concatenate([jnp.where(half, gpart, 0.0), jnp.where(half, 0.0, gpart)], axis=0).astype(bf16)
            gw = dot(stack, gyb[rows], NT)
            weights = []
            gscore = gst_s[rows, rows]
            for h in range(2):
                arg = cumt[2 * j + h : 2 * j + h + 1, rows] - cumg[rows, 2 * j + h : 2 * j + h + 1]
                decay = jnp.exp(jnp.minimum(arg, 0.0))
                weights.append((decay * smt_s[rows, rows]).astype(bf16))
                gscore = gscore + gw[h * BLOCK : (h + 1) * BLOCK] * decay
            gst_s[rows, rows] = gscore
            inner.append(dot(jnp.concatenate(weights, axis=1), gstack))
        far = (xd[:BLOCK] * efb[:BLOCK]).astype(bf16)
        ge = (gy[BLOCK:] * efb[BLOCK:]).astype(bf16)
        gst_s[:BLOCK, BLOCK:] += dot(far, ge, NT)
        gfar = dot(smt_s[:BLOCK, BLOCK:].astype(bf16), ge)
        xdb = xd.astype(bf16).astype(f32)
        fall0 = xdb[:BLOCK] * inner[0] + far.astype(f32) * gfar
        fall = jnp.concatenate([fall0, xdb[BLOCK:] * inner[1]], axis=0)
        gxd = jnp.concatenate([inner[0] + efb[:BLOCK] * gfar, inner[1]], axis=0)
        sums = headsum(jnp.concatenate([fall, xs * gxd], axis=0), headpick(8 * group + 2 * j, (2 * LANES, LANES)))
        gcum = gcum - sums[:length]
        gdir = gdir + sums[length:]
        gxs = cp_ref[0:1, sl] * gy + dtb * gxd
        gsum = gxs * (sg + xs * (1.0 - sg))
        gx, grads = conv_back(gsum, xin, cw, masks, length)
        px_ref[:, sl] = gx.astype(bf16)
        grads.append(jnp.sum(gy * xs, axis=0, keepdims=True))
        for k, value in enumerate(grads):
            gp_ref[0, k : k + 1, sl] = value
        gp_ref[0, 6:8, sl] = jnp.zeros((2, LANES), f32)
    gc_s[...] = gcum
    gd_s[...] = gdir

    @pl.when(group == pl.num_programs(1) - 1)
    def _():
        row = lax.broadcasted_iota(jnp.int32, (length, length), 0)
        col = lax.broadcasted_iota(jnp.int32, (length, length), 1)
        same = segc_ref[0][:, 0:1] == segr_ref[0, 0:1, :]
        gscore = jnp.where((row <= col) & same, gst_s[...], 0.0)
        backs = (dot(gscore, c_s[...], precision=highest), dot(gscore.T, b_s[...], precision=highest))
        for part in range(2):
            sl = slice(part * LANES, (part + 1) * LANES)
            xin = bc_ref[:, sl]
            cw = cwbc_ref[:, sl]
            summed = conv_sum(conv_taps(xin, masks), cw)
            sg = sigmoid(summed)
            gsum = backs[part] * (sg + summed * sg * (1.0 - sg))
            gx, grads = conv_back(gsum, xin, cw, masks, length)
            pr_ref[:, sl] = gx.astype(bf16)
            for k, value in enumerate(grads):
                gbc_ref[0, k : k + 1, sl] = value
            gbc_ref[0, 5:8, sl] = jnp.zeros((3, LANES), f32)
        upper = jnp.where(row <= col, 1.0, 0.0).astype(f32)
        gla = dot(upper, gc_s[...] + rs_ref[0], precision=highest)
        graw = (gd_s[...] - gla * jnp.exp(hp_ref[1:2, :])) * sp_s[...]
        graw = jnp.where(lane < heads, graw, 0.0)
        pr_ref[:, 2 * LANES :] = graw.astype(bf16)
        gh_ref[0, 0:1] = jnp.sum(graw, axis=0, keepdims=True)
        gh_ref[0, 1:2] = jnp.sum(jnp.where(lane < heads, gla * la_s[...], 0.0), axis=0, keepdims=True)
        gh_ref[0, 2:8] = jnp.zeros((6, LANES), f32)


def small_scratch(length):
    return [
        pltpu.VMEM((3, length, LANES), f32),
        pltpu.VMEM((length, LANES), f32),
        pltpu.VMEM((length, LANES), f32),
        pltpu.VMEM((length, LANES), f32),
        pltpu.VMEM((length, LANES), f32),
        pltpu.VMEM((LANES, length), f32),
        pltpu.VMEM((length, LANES), f32),
        pltpu.VMEM((length, LANES), f32),
        pltpu.VMEM((length, LANES), f32),
    ]


def mixer_forward(projected, gm, segc, segr, cw, hp, cp, heads, state):
    seqs, length = segc.shape[:2]
    inner = gm.shape[1]
    groups = inner // GROUP
    rows = seqs * length
    kernel = functools.partial(fwd_kernel, heads)
    out_row = lambda b, p, g: (b, g * p)
    return pl.pallas_call(
        kernel,
        grid=(seqs, 2, groups),
        in_specs=[
            pl.BlockSpec((length, GROUP), lambda b, p, g: (b, g)),
            pl.BlockSpec((length, GROUP), lambda b, p, g: (b, groups + g * (1 - p) + (groups - 1) * p)),
            pl.BlockSpec((length, 2 * state), lambda b, p, g: (b, 2 * inner // (2 * state))),
            pl.BlockSpec((length, LANES), lambda b, p, g: (b, (2 * inner + 2 * state) // LANES)),
            pl.BlockSpec((length, GROUP), lambda b, p, g: (b, g)),
            pl.BlockSpec((1, length, LANES), lambda b, p, g: (b, 0, 0)),
            pl.BlockSpec((1, 8, length), lambda b, p, g: (b, 0, 0)),
            pl.BlockSpec((8, GROUP), lambda b, p, g: (0, g)),
            pl.BlockSpec((8, 2 * state), lambda b, p, g: (0, inner // (2 * state))),
            pl.BlockSpec((8, LANES), lambda b, p, g: (0, 0)),
            pl.BlockSpec((8, GROUP), lambda b, p, g: (0, g)),
        ],
        out_specs=[
            pl.BlockSpec((length, GROUP), out_row),
            pl.BlockSpec((length, GROUP), out_row),
            pl.BlockSpec((length, GROUP), out_row),
            pl.BlockSpec((1, length, LANES), lambda b, p, g: (b, 0, 0)),
            pl.BlockSpec((1, 8, GROUP), lambda b, p, g: (b, 0, g * p)),
        ],
        out_shape=[
            jax.ShapeDtypeStruct((rows, inner), bf16),
            jax.ShapeDtypeStruct((rows, inner), bf16),
            jax.ShapeDtypeStruct((rows, inner), f32),
            jax.ShapeDtypeStruct((seqs, length, LANES), f32),
            jax.ShapeDtypeStruct((seqs, 8, inner), f32),
        ],
        scratch_shapes=small_scratch(length) + [
            pltpu.VMEM((length, length), f32),
            pltpu.VMEM((length, inner), f32),
            pltpu.VMEM((length, inner), f32),
            pltpu.VMEM((length - BLOCK, inner), f32),
            pltpu.VMEM((2, length, LANES), f32),
            pltpu.VMEM((length, LANES), f32),
        ],
        compiler_params=pltpu.CompilerParams(vmem_limit_bytes=48 << 20),
        cost_estimate=pl.CostEstimate(flops=10**10, bytes_accessed=45 * 10**6, transcendentals=10**7),
        name="mixer_forward",
    )(projected, projected, projected, projected, gm, segc, segr, cw, cw, hp, cp)


def mixer_backward(projected, gy, rs, segc, segr, cw, hp, cp, heads, state):
    seqs, length = segc.shape[:2]
    inner = gy.shape[1]
    groups = inner // GROUP
    rows = seqs * length
    kernel = functools.partial(bwd_kernel, heads)
    return pl.pallas_call(
        kernel,
        grid=(seqs, groups),
        in_specs=[
            pl.BlockSpec((length, GROUP), lambda b, g: (b, groups + g)),
            pl.BlockSpec((length, 2 * state), lambda b, g: (b, 2 * inner // (2 * state))),
            pl.BlockSpec((length, LANES), lambda b, g: (b, (2 * inner + 2 * state) // LANES)),
            pl.BlockSpec((length, GROUP), lambda b, g: (b, g)),
            pl.BlockSpec((1, length, LANES), lambda b, g: (b, 0, 0)),
            pl.BlockSpec((1, length, LANES), lambda b, g: (b, 0, 0)),
            pl.BlockSpec((1, 8, length), lambda b, g: (b, 0, 0)),
            pl.BlockSpec((8, GROUP), lambda b, g: (0, g)),
            pl.BlockSpec((8, 2 * state), lambda b, g: (0, inner // (2 * state))),
            pl.BlockSpec((8, LANES), lambda b, g: (0, 0)),
            pl.BlockSpec((8, GROUP), lambda b, g: (0, g)),
        ],
        out_specs=[
            pl.BlockSpec((length, GROUP), lambda b, g: (b, g)),
            pl.BlockSpec((length, 3 * LANES), lambda b, g: (b, 0)),
            pl.BlockSpec((1, 8, GROUP), lambda b, g: (b, 0, g)),
            pl.BlockSpec((1, 8, 2 * state), lambda b, g: (b, 0, 0)),
            pl.BlockSpec((1, 8, LANES), lambda b, g: (b, 0, 0)),
        ],
        out_shape=[
            jax.ShapeDtypeStruct((rows, inner), bf16),
            jax.ShapeDtypeStruct((rows, 3 * LANES), bf16),
            jax.ShapeDtypeStruct((seqs, 8, inner), f32),
            jax.ShapeDtypeStruct((seqs, 8, 2 * state), f32),
            jax.ShapeDtypeStruct((seqs, 8, LANES), f32),
        ],
        scratch_shapes=small_scratch(length) + [
            pltpu.VMEM((length, length), f32),
            pltpu.VMEM((length, length), f32),
            pltpu.VMEM((length, LANES), f32),
            pltpu.VMEM((length, LANES), f32),
        ],
        compiler_params=pltpu.CompilerParams(vmem_limit_bytes=48 << 20),
        cost_estimate=pl.CostEstimate(flops=10**10, bytes_accessed=30 * 10**6, transcendentals=10**7),
        name="mixer_backward",
    )(projected, projected, projected, gy, rs, segc, segr, cw, cw, hp, cp)


def pad_lanes(v, width=LANES):
    return jnp.pad(v, ((0, 0), (0, width - v.shape[1])))


def mixer_tables(segments, kernel_full, shift_full, dt_bias, a_log, d_skip, gate_full):
    taps = kernel_full.shape[0]
    seqs, length = segments.shape
    columns = [segments.astype(f32)]
    where = jnp.arange(length)[None, :]
    for j in range(1, taps):
        before = jnp.pad(segments, ((0, 0), (j, 0)))[:, :length]
        columns.append(((before == segments) & (where >= j)).astype(f32))
    segc = jnp.pad(jnp.stack(columns, axis=-1), ((0, 0), (0, 0), (0, LANES - taps)))
    segr = jnp.broadcast_to(segments.astype(f32)[:, None, :], (seqs, 8, length))
    cw = jnp.concatenate([kernel_full.astype(f32), jnp.broadcast_to(shift_full.astype(f32)[None], (8 - taps, shift_full.shape[0]))])
    hp = pad_lanes(jnp.concatenate([dt_bias[None], jnp.broadcast_to(a_log[None], (7, a_log.shape[0]))]))
    heads = dt_bias.shape[0]
    size = gate_full.shape[0] // heads
    cp = jnp.concatenate([jnp.repeat(d_skip, size)[None], jnp.broadcast_to(gate_full.astype(f32)[None], (7, gate_full.shape[0]))])
    return segc, segr, cw, hp, cp


MESH = pl.DeviceIdType.MESH
PIECES = 3


def ring_place(chip, chips):
    wide = chips // 4
    z, q = chip // wide, chip % wide
    up = 1 + 3 * q + jnp.where(q % 2 == 0, z - 1, 3 - z)
    back = jnp.where(q == 0, 0, 4 * wide - q)
    return jnp.where(z == 0, back, up)


def ring_chip(place, chips):
    wide = chips // 4
    place = place % chips
    q = (place - 1 + chips) % chips // 3
    r = (place - 1 + chips) % chips % 3
    z = jnp.where(q % 2 == 0, 1 + r, 3 - r)
    inner = z * wide + q
    outer = (4 * wide - place) % (4 * wide)
    return jnp.where((place == 0) | (place > 3 * wide), outer, inner)


def gather_kernel(chips, count, *refs):
    ins, outs = refs[:count], refs[count : 2 * count]
    ring_send, ring_recv, far_send, far_recv, pair_send, pair_recv, own_sem = refs[2 * count :]
    me = lax.axis_index("fsdp")
    plane = lax.axis_index("dp")
    chip, core = me // 2, me % 2
    place = ring_place(chip, chips)
    right = 2 * ring_chip(place + 1, chips) + core
    left = 2 * ring_chip(place + chips - 1, chips) + core
    pair = {"fsdp": me + 1 - 2 * core}
    peer = {"dp": 1 - plane}
    ways = ({"fsdp": right}, {"fsdp": left})

    barrier = pltpu.get_barrier_semaphore()
    for other in (ways[0], ways[1], pair, peer):
        pl.semaphore_signal(barrier, inc=1, device_id=other, device_id_type=MESH)
    pl.semaphore_wait(barrier, 4)

    half = chips // 2
    whole = [k == count - 1 for k in range(count)]

    def steps(way, slot):
        return half if way == slot else half - 1

    def owner(way, step):
        move = -step if way == 0 else step
        return 2 * ring_chip(place + move + chips, chips) + core

    def part(refs, k, index, slot):
        if whole[k]:
            return refs[k].at[index]
        piece = 0 if slot == 0 else 1 + plane
        return refs[k].at[index, piece]

    def mine(k, slot):
        if whole[k]:
            return ins[k]
        piece = 0 if slot == 0 else 1 + plane
        return ins[k].at[piece]

    def slots(k):
        return (0,) if whole[k] else (0, 1)

    pending = []

    def send(source, target, send_sem, recv_sem, device):
        copy = pltpu.make_async_remote_copy(
            src_ref=source, dst_ref=target, send_sem=send_sem, recv_sem=recv_sem, device_id=device, device_id_type=MESH)
        copy.start()
        pending.append(copy)

    def arrived(target, send_sem, recv_sem):
        pltpu.make_async_remote_copy(
            src_ref=target, dst_ref=target, send_sem=send_sem, recv_sem=recv_sem, device_id=pair, device_id_type=MESH).wait_recv()

    def ring_sem(sem, way, step, k, slot):
        return sem.at[(way * half + step - 1) * 2 * count + 2 * k + slot]

    def far_sem(sem, way, step, k):
        return sem.at[(way * half + step - 1) * count + k]

    def pair_sem(sem, turn, k, slot):
        return sem.at[(turn * count + k) * 3 + slot]

    def turn(way, step):
        return 1 + (step - 1) * 2 + way

    local = []
    for k in range(count):
        for slot in slots(k):
            for way in range(2):
                send(mine(k, slot), part(outs, k, me, slot), ring_sem(ring_send, way, 1, k, slot), ring_sem(ring_recv, way, 1, k, slot), ways[way])
        send(ins[k], outs[k].at[me], pair_sem(pair_send, 0, k, 0), pair_sem(pair_recv, 0, k, 0), pair)
        copy = pltpu.make_async_copy(ins[k], outs[k].at[me], own_sem.at[k])
        copy.start()
        local.append(copy)

    def from_peer(way, step):
        index = owner(way, step)
        for k in range(count):
            if whole[k] or step > steps(way, 1):
                continue
            target = outs[k].at[index, 2 - plane]
            arrived(target, far_sem(far_send, way, step, k), far_sem(far_recv, way, step, k))
            send(target, target, pair_sem(pair_send, turn(way, step), k, 2), pair_sem(pair_recv, turn(way, step), k, 2), pair)

    for step in range(1, half + 1):
        for way in range(2):
            index = owner(way, step)
            for k in range(count):
                for slot in slots(k):
                    if step > steps(way, slot):
                        continue
                    target = part(outs, k, index, slot)
                    arrived(target, ring_sem(ring_send, way, step, k, slot), ring_sem(ring_recv, way, step, k, slot))
                    if step + 1 <= steps(way, slot):
                        send(target, target, ring_sem(ring_send, way, step + 1, k, slot), ring_sem(ring_recv, way, step + 1, k, slot), ways[way])
                    if slot == 1:
                        send(target, target, far_sem(far_send, way, step, k), far_sem(far_recv, way, step, k), peer)
                    send(target, target, pair_sem(pair_send, turn(way, step), k, slot), pair_sem(pair_recv, turn(way, step), k, slot), pair)
        if step > 1:
            for way in range(2):
                from_peer(way, step - 1)
    for way in range(2):
        from_peer(way, half)
    for k in range(count):
        other = outs[k].at[me + 1 - 2 * core]
        arrived(other, pair_sem(pair_send, 0, k, 0), pair_sem(pair_recv, 0, k, 0))
    for step in range(1, half + 1):
        for way in range(2):
            index = owner(way, step) + 1 - 2 * core
            for k in range(count):
                for slot in slots(k) + (() if whole[k] else (2,)):
                    if step > steps(way, min(slot, 1)):
                        continue
                    if slot == 2:
                        target = outs[k].at[index, 2 - plane]
                    else:
                        target = part(outs, k, index, slot)
                    sems = turn(way, step), k, slot
                    arrived(target, pair_sem(pair_send, *sems), pair_sem(pair_recv, *sems))
    for copy in local:
        copy.wait()
    for copy in pending:
        copy.wait_send()


def gather(arrays, devices):
    count = len(arrays)
    chips = devices // 2
    half = chips // 2
    dma = pltpu.SemaphoreType.DMA
    return pl.pallas_call(
        functools.partial(gather_kernel, chips, count),
        in_specs=[pl.BlockSpec(memory_space=pl.ANY)] * count,
        out_specs=[pl.BlockSpec(memory_space=pl.ANY)] * count,
        out_shape=[jax.ShapeDtypeStruct((devices,) + a.shape, a.dtype) for a in arrays],
        scratch_shapes=[
            dma((4 * half * count,)), dma((4 * half * count,)),
            dma((2 * half * count,)), dma((2 * half * count,)),
            dma(((2 * half + 1) * count * 3,)), dma(((2 * half + 1) * count * 3,)),
            dma((count,)),
        ],
        compiler_params=pltpu.CompilerParams(collective_id=0, has_side_effects=True),
        name="gather_weights",
    )(*arrays)


QUARTERS = 4
TILE = 512


def reduce_kernel(chips, items, rounds, *refs):
    count = len(items)
    parts, small_in = refs[:count], refs[count]
    outs, small_out = refs[count + 1 : 2 * count + 1], refs[2 * count + 1]
    scratch = refs[2 * count + 2 :]
    held, ring_in, ring_out, peer_in, last_out, last_in = (scratch[i * count : (i + 1) * count] for i in range(6))
    (small_recv, small_sent, held_sem, ring_send, ring_recv, peer_send, peer_recv, last_send, last_recv, small_send, small_sem) = scratch[6 * count :]
    me = lax.axis_index("fsdp")
    plane = lax.axis_index("dp")
    chip, core = me // 2, me % 2
    place = ring_place(chip, chips)
    ways = (
        {"fsdp": 2 * ring_chip(place + 1, chips) + core},
        {"fsdp": 2 * ring_chip(place + chips - 1, chips) + core},
    )
    peer = {"dp": 1 - plane}
    turns = [{"fsdp": me + bit - 2 * bit * ((me // bit) % 2)} for bit in [1 << k for k in range(rounds - 1)]] + [peer]
    half = chips // 2

    barrier = pltpu.get_barrier_semaphore()
    greet = list(ways) + turns
    for other in greet:
        pl.semaphore_signal(barrier, inc=1, device_id=other, device_id_type=MESH)
    pl.semaphore_wait(barrier, len(greet))

    pending = []

    def send(source, target, send_sem, recv_sem, device):
        copy = pltpu.make_async_remote_copy(
            src_ref=source, dst_ref=target, send_sem=send_sem, recv_sem=recv_sem, device_id=device, device_id_type=MESH)
        copy.start()
        pending.append(copy)

    def arrived(target, send_sem, recv_sem):
        pltpu.make_async_remote_copy(
            src_ref=target, dst_ref=target, send_sem=send_sem, recv_sem=recv_sem, device_id=peer, device_id_type=MESH).wait_recv()

    def hops(k, way, slot):
        return half - (slot + (k if slot == 2 else 0) + way) % 2

    def target(k, way, slot, step):
        ahead = hops(k, way, slot) - step + 1
        return ring_chip(place + (ahead if way == 0 else chips - ahead), chips)

    def quarter(slot):
        return slot if slot < 2 else 2 + plane

    def ring_at(way, step, slot):
        return (way * half + step - 1) * 3 + slot

    def sems(k, way, step, slot):
        at = k * 6 * half + ring_at(way, step, slot)
        return ring_send.at[at], ring_recv.at[at]

    def add_up(k, sources, store, width):
        tile = min(TILE, width)
        def one(i, carry):
            cols = pl.ds(pl.multiple_of(i * tile, LANES), tile)
            total = sources[0][:, cols].astype(f32)
            for source in sources[1:]:
                total = total + source[:, cols].astype(f32)
            store[:, cols] = total.astype(store.dtype)
            return carry
        lax.fori_loop(0, width // tile, one, 0)
        rest = width % tile
        if rest:
            cols = slice(width - rest, width)
            total = sources[0][:, cols].astype(f32)
            for source in sources[1:]:
                total = total + source[:, cols].astype(f32)
            store[:, cols] = total.astype(store.dtype)

    for slot in (0, 1):
        for k in range(count):
            for way in range(2):
                send(parts[k].at[target(k, way, slot, 1), slot], ring_in[k].at[ring_at(way, 1, slot)], *sems(k, way, 1, slot), ways[way])
    order = []
    for ahead in range(half, -1, -1):
        order.append((place + ahead) % chips)
        if 0 < ahead < half:
            order.append((place + chips - ahead) % chips)
    for where in order:
        chunk = ring_chip(where, chips)
        for k in range(count):
            send(parts[k].at[chunk, 3 - plane], peer_in[k].at[where], peer_send.at[k * chips + where], peer_recv.at[k * chips + where], peer)
    loads = []
    for k in range(count):
        for slot in range(3):
            copy = pltpu.make_async_copy(parts[k].at[:, quarter(slot)], held[k].at[slot], held_sem.at[k * 3 + slot])
            copy.start()
            loads.append(copy)

    def small_round(turn):
        value = small_in if turn == 0 else small_sent.at[turn - 1]
        send(value, small_recv.at[turn], small_send.at[turn], small_sem.at[turn], turns[turn])

    def small_finish(turn):
        value = small_in if turn == 0 else small_sent.at[turn - 1]
        arrived(small_recv.at[turn], small_send.at[turn], small_sem.at[turn])
        store = small_out if turn == rounds - 1 else small_sent.at[turn]
        store[...] = value[...] + small_recv[turn]

    small_round(0)
    for copy in loads:
        copy.wait()

    def from_peer(k, chunk):
        where = ring_place(chunk, chips)
        arrived(peer_in[k].at[where], peer_send.at[k * chips + where], peer_recv.at[k * chips + where])
        return peer_in[k].at[where]

    awaited = [set() for _ in range(count)]
    done = 0
    for step in range(1, half + 1):
        for slot in (0, 1, 2):
            for k in range(count):
                for way in range(2):
                    if step > hops(k, way, slot) or (step == 1 and slot < 2):
                        continue
                    chunk = target(k, way, slot, step)
                    sources = [held[k].at[slot, chunk]]
                    if step > 1:
                        before = ring_at(way, step - 1, slot)
                        arrived(ring_in[k].at[before], *sems(k, way, step - 1, slot))
                        sources.append(ring_in[k].at[before])
                    if slot == 2:
                        sources.append(from_peer(k, chunk))
                    at = ring_at(way, step, slot)
                    add_up(k, sources, ring_out[k].at[at], items[k][1])
                    send(ring_out[k].at[at], ring_in[k].at[at], *sems(k, way, step, slot), ways[way])
        for _ in range(-(-rounds // half) if step < half else rounds):
            if done < rounds - 1:
                small_finish(done)
                done += 1
                small_round(done)
    for slot in (0, 1, 2):
        for k in range(count):
            sources = [held[k].at[slot, chip]]
            for way in range(2):
                last = hops(k, way, slot)
                at = ring_at(way, last, slot)
                arrived(ring_in[k].at[at], *sems(k, way, last, slot))
                sources.append(ring_in[k].at[at])
            if slot == 2:
                sources.append(from_peer(k, chip))
            add_up(k, sources, last_out[k].at[slot], items[k][1])
            send(last_out[k].at[slot], last_in[k].at[slot], last_send.at[k * 3 + slot], last_recv.at[k * 3 + slot], peer)
    while done < rounds:
        small_finish(done)
        done += 1
        if done < rounds:
            small_round(done)
    for slot in (0, 1, 2):
        for k in range(count):
            arrived(last_in[k].at[slot], last_send.at[k * 3 + slot], last_recv.at[k * 3 + slot])
            width = items[k][1]
            if slot < 2:
                add_up(k, [last_out[k].at[slot], last_in[k].at[slot]], outs[k].at[slot], width)
            else:
                add_up(k, [last_out[k].at[slot]], outs[k].at[2 + plane], width)
                add_up(k, [last_in[k].at[slot]], outs[k].at[3 - plane], width)
    for copy in pending:
        copy.wait_send()


def reduce_scatter(arrays, small, devices):
    count = len(arrays)
    chips = devices // 2
    half = chips // 2
    rounds = devices.bit_length()
    items = tuple(a.shape[2:] for a in arrays)
    dma = pltpu.SemaphoreType.DMA
    vm = lambda lead, dtype=bf16: [pltpu.VMEM(lead + item, dtype) for item in items]
    return pl.pallas_call(
        functools.partial(reduce_kernel, chips, items, rounds),
        in_specs=[pl.BlockSpec(memory_space=pl.ANY)] * count + [pl.BlockSpec(memory_space=pltpu.VMEM)],
        out_specs=[pl.BlockSpec(memory_space=pltpu.VMEM)] * (count + 1),
        out_shape=[jax.ShapeDtypeStruct((4,) + item, f32) for item in items] + [jax.ShapeDtypeStruct(small.shape, f32)],
        scratch_shapes=vm((3, chips)) + vm((6 * half,)) + vm((6 * half,)) + vm((chips,)) + vm((3,)) + vm((3,)) + [
            pltpu.VMEM((rounds,) + small.shape, f32), pltpu.VMEM((rounds,) + small.shape, f32),
            dma((3 * count,)),
            dma((6 * half * count,)), dma((6 * half * count,)),
            dma((chips * count,)), dma((chips * count,)),
            dma((3 * count,)), dma((3 * count,)),
            dma((rounds,)), dma((rounds,)),
        ],
        compiler_params=pltpu.CompilerParams(collective_id=1, has_side_effects=True, vmem_limit_bytes=62 << 20),
        name="reduce_gradients",
    )(*arrays, small)


def parts_kernel(a_ref, a2_ref, b_ref, b2_ref, o_ref):
    o_ref[...] = (dot(a_ref[...], b_ref[...]) + dot(a2_ref[...], b2_ref[...])).astype(bf16)


def grad_parts(left, left2, right, right2, name):
    rows, tokens = left.shape
    width = right.shape[1]
    tile = min(GROUP, width)
    return pl.pallas_call(
        parts_kernel,
        grid=(width // tile,),
        in_specs=[
            pl.BlockSpec((rows, tokens), lambda i: (0, 0)),
            pl.BlockSpec((rows, tokens), lambda i: (0, 0)),
            pl.BlockSpec((tokens, tile), lambda i: (0, i)),
            pl.BlockSpec((tokens, tile), lambda i: (0, i)),
        ],
        out_specs=pl.BlockSpec((rows, tile), lambda i: (0, i)),
        out_shape=jax.ShapeDtypeStruct((rows, width), bf16),
        compiler_params=pltpu.CompilerParams(vmem_limit_bytes=32 << 20),
        cost_estimate=pl.CostEstimate(flops=4 * rows * tokens * width, bytes_accessed=2 * (2 * rows * tokens + 2 * tokens * width + rows * width), transcendentals=0),
        name=name,
    )(left, left2, right, right2)


def input_kernel(groups, used, gz_ref, px_ref, pr_ref, w_ref, tok_ref, cot_ref, gain_ref, gt_ref, gn_ref, acc):
    step = pl.program_id(0)

    @pl.when(step == 0)
    def _():
        acc[...] = jnp.zeros_like(acc)

    @pl.when(step < groups)
    def _():
        acc[...] += dot(gz_ref[...], w_ref[...], NT)

    @pl.when((step >= groups) & (step < 2 * groups))
    def _():
        acc[...] += dot(px_ref[...], w_ref[...], NT)

    @pl.when(step == 2 * groups)
    def _():
        size = pr_ref.shape[1]
        col = lax.broadcasted_iota(jnp.int32, (w_ref.shape[0], size), 1)
        tail = jnp.where(col < used, w_ref[:, :size].astype(f32), 0.0).astype(bf16)
        acc[...] += dot(pr_ref[...], tail, NT)
        rows, width = acc.shape
        chunk = BLOCK
        total = jnp.zeros((1, width), f32)
        for i in range(rows // chunk):
            sl = slice(i * chunk, (i + 1) * chunk)
            u = tok_ref[sl].astype(f32)
            rstd = lax.rsqrt(jnp.mean(u * u, axis=1, keepdims=True) + epsilon)
            unit = u * rstd
            gn = acc[sl]
            total = total + jnp.sum(gn * unit, axis=0, keepdims=True)
            gu = gn * gain_ref[0:1, :]
            inward = jnp.mean(gu * unit, axis=1, keepdims=True)
            gt_ref[sl] = cot_ref[sl].astype(f32) + rstd * (gu - unit * inward)
        gn_ref[...] = jnp.broadcast_to(total, gn_ref.shape)


def grad_input(gz, px, pr, w_in_full, tokens, cot, gain, used):
    rows, width = tokens.shape
    groups = gz.shape[1] // GROUP
    return pl.pallas_call(
        functools.partial(input_kernel, groups, used),
        grid=(2 * groups + 1,),
        in_specs=[
            pl.BlockSpec((rows, GROUP), lambda i: (0, jnp.minimum(i, groups - 1))),
            pl.BlockSpec((rows, GROUP), lambda i: (0, jnp.clip(i - groups, 0, groups - 1))),
            pl.BlockSpec((rows, pr.shape[1]), lambda i: (0, 0)),
            pl.BlockSpec((width, GROUP), lambda i: (0, i)),
            pl.BlockSpec((rows, width), lambda i: (0, 0)),
            pl.BlockSpec((rows, width), lambda i: (0, 0)),
            pl.BlockSpec((8, width), lambda i: (0, 0)),
        ],
        out_specs=[pl.BlockSpec((rows, width), lambda i: (0, 0)), pl.BlockSpec((8, width), lambda i: (0, 0))],
        out_shape=[jax.ShapeDtypeStruct((rows, width), f32), jax.ShapeDtypeStruct((8, width), f32)],
        scratch_shapes=[pltpu.VMEM((rows, width), f32)],
        compiler_params=pltpu.CompilerParams(vmem_limit_bytes=48 << 20),
        cost_estimate=pl.CostEstimate(flops=2 * rows * width * w_in_full.shape[1], bytes_accessed=32 * 10**6, transcendentals=0),
        name="grad_input",
    )(gz, px, pr, w_in_full, tokens, cot, gain)


def small_rows(size):
    return 16 * (-(-size // (16 * LANES)))


def flat_pack(parts, rows):
    flat = jnp.concatenate([p.reshape(-1) for p in parts])
    return jnp.pad(flat, (0, rows * LANES - flat.shape[0])).reshape(rows, LANES)


def local(devices, tokens, segments, norm_gain, w_in, conv_weight, conv_bias, dt_bias, a_log, d_skip, gate_gain, w_out, cotangent):
    seqs, length, width = tokens.shape
    rows = seqs * length
    proj_width = w_in.shape[1]
    inner = devices * w_out.shape[0]
    taps = conv_weight.shape[0]
    heads = dt_bias.shape[0]
    share_n, share_c, share_g = norm_gain.shape[0], conv_bias.shape[0], gate_gain.shape[0]
    conv_width = devices * share_c
    state = (conv_width - inner) // 2
    chips = devices // 2
    me = lax.axis_index("fsdp")
    core = me % 2
    swap = [(i, i + 1 - 2 * (i % 2)) for i in range(devices)]
    partner = lambda value: lax.ppermute(value, "fsdp", swap)

    size = share_n + share_g + (taps + 1) * share_c
    pack = flat_pack([norm_gain, gate_gain, conv_weight, conv_bias], small_rows(size))
    win_all, wout_all, pack_all = gather(
        [w_in.reshape(PIECES, -1, proj_width), w_out.reshape(PIECES, -1, width), pack], devices)
    w_in_full = win_all.reshape(width, proj_width)
    w_out_full = wout_all.reshape(inner, width)
    pack_all = pack_all.reshape(devices, -1)
    cuts = [share_n, share_n + share_g, share_n + share_g + taps * share_c, size]
    gain_full = pack_all[:, : cuts[0]].reshape(width)
    gate_full = pack_all[:, cuts[0] : cuts[1]].reshape(inner)
    kernel_full = pack_all[:, cuts[1] : cuts[2]].reshape(devices, taps, share_c).transpose(1, 0, 2).reshape(taps, conv_width)
    shift_full = pack_all[:, cuts[2] : cuts[3]].reshape(conv_width)

    flat_tokens = tokens.reshape(rows, width)
    residual = flat_tokens.astype(f32)
    rstd = lax.rsqrt(jnp.mean(residual * residual, axis=-1, keepdims=True) + epsilon)
    gain_f = gain_full.astype(f32)
    normed = (residual * rstd * gain_f).astype(bf16)
    grad_rows = cotangent.reshape(rows, width)
    grad_rows2 = partner(grad_rows)

    def split_rows(value):
        turned = value.T.reshape(chips, 2, -1, rows)
        mine = lax.dynamic_index_in_dim(turned, core, 1, keepdims=False)
        theirs = lax.dynamic_index_in_dim(turned, 1 - core, 1, keepdims=False)
        return mine.reshape(-1, rows), partner(theirs).reshape(-1, rows)

    projected = dot(normed, w_in_full)
    gm = dot(grad_rows, w_out_full, NT)
    normed_t, normed_t2 = split_rows(normed)
    tables = mixer_tables(segments, kernel_full, shift_full, dt_bias, a_log, d_skip, gate_full)
    mixed, gz, gy, rs, gg = mixer_forward(projected, gm, *tables, heads, state)
    gz2 = partner(gz)
    mixed_t, mixed_t2 = split_rows(mixed)
    block_out = (residual + dot(mixed, w_out_full)).astype(bf16)
    px, pr, gp, gbc, gh = mixer_backward(projected, gy, rs, *tables, heads, state)
    px2, pr2 = partner(px), partner(pr)
    part_out = grad_parts(mixed_t, mixed_t2, grad_rows, grad_rows2, "grad_out")
    part_z = grad_parts(normed_t, normed_t2, gz, gz2, "grad_z")
    gain8 = jnp.broadcast_to(gain_f[None], (8, width))
    grad_tokens, grad_norm = grad_input(gz, px, pr, w_in_full, flat_tokens, grad_rows, gain8, 2 * state + heads)
    part_x = grad_parts(normed_t, normed_t2, px, px2, "grad_x")
    part_r = grad_parts(normed_t, normed_t2, pr, pr2, "grad_r")

    gp, gbc, gh = gp.sum(0), gbc.sum(0), gh.sum(0)
    grad_kernel = jnp.concatenate([gp[:taps], gbc[:taps]], axis=1)
    grad_shift = jnp.concatenate([gp[taps], gbc[taps]])
    grad_gate = gg[:, 0].sum(0)
    grad_skip = gp[taps + 1].reshape(heads, inner // heads).sum(1)
    small = jnp.concatenate([
        grad_norm[0].reshape(devices, share_n), grad_gate.reshape(devices, share_g),
        grad_kernel.reshape(taps, devices, share_c).transpose(1, 0, 2).reshape(devices, taps * share_c),
        grad_shift.reshape(devices, share_c)], axis=1)
    each = -(-size // LANES)
    small = jnp.pad(small, ((0, 0), (0, each * LANES - size))).reshape(devices * each, LANES)
    head = pad_lanes(jnp.stack([gh[0, :heads], gh[1, :heads], grad_skip]))
    small = jnp.concatenate([head, small])
    small = jnp.pad(small, ((0, -small.shape[0] % 8), (0, 0)))

    quarters = lambda part: part.reshape(chips, QUARTERS, -1, part.shape[1])
    own_out, own_z, own_x, own_r, small = reduce_scatter([quarters(p) for p in (part_out, part_z, part_x, part_r)], small, devices)
    grad_w_in = jnp.concatenate([o.reshape(-1, o.shape[2]) for o in (own_z, own_x, own_r)], axis=1)[:, :proj_width]
    head_grads = small[:3, :heads]
    mine = lax.dynamic_slice(small, (3 + me * each, 0), (each, LANES)).reshape(-1)
    return (
        block_out.reshape(seqs, length, width),
        grad_tokens.reshape(seqs, length, width),
        mine[: cuts[0]],
        grad_w_in,
        mine[cuts[1] : cuts[2]].reshape(taps, share_c),
        mine[cuts[2] : cuts[3]],
        head_grads[0],
        head_grads[1],
        head_grads[2],
        mine[cuts[0] : cuts[1]],
        own_out.reshape(-1, width),
    )


def solution(mesh):
    rows3, rows2 = P(("fsdp", "dp"), None, None), P(("fsdp", "dp"), None)
    return jax.shard_map(
        functools.partial(local, mesh.shape["fsdp"]),
        mesh=mesh,
        in_specs=(rows3, rows2, P("fsdp"), P("fsdp", None), P(None, "fsdp"), P("fsdp"), P(), P(), P(), P("fsdp"), P("fsdp", None), rows3),
        out_specs=(rows3, rows3, P("fsdp"), P("fsdp", None), P(None, "fsdp"), P("fsdp"), P(), P(), P(), P("fsdp"), P("fsdp", None)),
        check_vma=False,
    )
```

```python
import functools

import jax
import jax.numpy as jnp
from jax import lax
from jax.experimental import pallas as pl
from jax.experimental.pallas import tpu as pltpu
from jax.sharding import PartitionSpec as P

f32, bf16 = jnp.float32, jnp.bfloat16
highest = lax.Precision.HIGHEST
epsilon = 1e-05
LANES = 128
BLOCK = 128
GROUP = 512
PAIRS = GROUP // LANES
NT = (((1,), (1,)), ((), ()))
NN = (((1,), (0,)), ((), ()))


def dot(a, b, dims=NN, precision=None):
    return lax.dot_general(a, b, dims, precision=precision, preferred_element_type=f32)


def sigmoid(v):
    return 0.5 + 0.5 * jnp.tanh(0.5 * v)


def conv_taps(xin, masks):
    taps = []
    for shift in (3, 2, 1):
        taps.append(pltpu.roll(xin, shift, 0) * masks[3 - shift])
    taps.append(xin)
    return taps


def conv_sum(taps, cw):
    total = cw[4:5, :] + cw[3:4, :] * taps[3]
    for k in range(3):
        total = total + cw[k : k + 1, :] * taps[k]
    return total


def conv_back(gsum, xin, cw, masks, length):
    grads = []
    gx = cw[3:4, :] * gsum
    for shift in (3, 2, 1):
        masked = gsum * masks[3 - shift]
        grads.append(jnp.sum(masked * pltpu.roll(xin, shift, 0), axis=0, keepdims=True))
        gx = gx + cw[3 - shift : 4 - shift, :] * pltpu.roll(masked, length - shift, 0)
    grads.append(jnp.sum(gsum * xin, axis=0, keepdims=True))
    grads.append(jnp.sum(gsum, axis=0, keepdims=True))
    return gx, grads


def prologue(heads, bc_ref, dtr_ref, segr_ref, cwbc_ref, hp_ref, mask_s, b_s, c_s, dt_s, cum_s, cumt_s, ef_s, la_s, sp_s):
    length = bc_ref.shape[0]
    segc = segr_ref[0].T
    here = lax.broadcasted_iota(jnp.int32, segc.shape, 0)
    for shift in (1, 2, 3):
        alike = (pltpu.roll(segc, shift, 0) == segc) & (here >= shift)
        mask_s[3 - shift] = jnp.broadcast_to(jnp.where(alike, 1.0, 0.0)[:, 0:1], (length, LANES))
    masks = [mask_s[k] for k in range(3)]
    for half, ref in ((0, b_s), (1, c_s)):
        sl = slice(half * LANES, (half + 1) * LANES)
        taps = conv_taps(bc_ref[:, sl], masks)
        summed = conv_sum(taps, cwbc_ref[:, sl])
        ref[...] = summed * sigmoid(summed)
    lane = lax.broadcasted_iota(jnp.int32, (length, LANES), 1)
    raw = jnp.where(lane < heads, dtr_ref[...] + hp_ref[0:1, :], 0.0)
    soft = jnp.maximum(raw, 0.0) + jnp.log1p(jnp.exp(-jnp.abs(raw)))
    dt = jnp.where(lane < heads, soft, 0.0)
    la = -dt * jnp.exp(hp_ref[1:2, :])
    row = lax.broadcasted_iota(jnp.int32, (length, length), 0)
    col = lax.broadcasted_iota(jnp.int32, (length, length), 1)
    tri = jnp.where(row >= col, 1.0, 0.0).astype(f32)
    cum = dot(tri, la, precision=highest)
    dt_s[...] = dt
    la_s[...] = la
    cum_s[...] = cum
    cumt_s[...] = cum.T
    sp_s[...] = sigmoid(raw)
    mid = cum[BLOCK - 1 : BLOCK, :]
    ef_s[:BLOCK] = jnp.exp(jnp.minimum(mid - cum[:BLOCK], 0.0))
    ef_s[BLOCK:] = jnp.exp(jnp.minimum(cum[BLOCK:] - mid, 0.0))
    same = (segc[:, 0:1] == segr_ref[0, 0:1, :]).astype(f32)
    return row, col, same


def headpick(first, shape):
    source = lax.broadcasted_iota(jnp.int32, shape, 0) // 64
    target = lax.broadcasted_iota(jnp.int32, shape, 1)
    source = source - 2 * (source // 2)
    return jnp.where(target == source + first, 1.0, 0.0).astype(bf16)


def headsum(value, pick):
    hi = value.astype(bf16)
    lo = (value - hi.astype(f32)).astype(bf16)
    return dot(jnp.concatenate([hi, lo], axis=1), pick)


def fwd_kernel(heads, z_ref, x_ref, bc_ref, dtr_ref, gm_ref, segr_ref, cwx_ref, cwbc_ref, hp_ref, cp_ref,
               mixed_ref, mixt_ref, gz_ref, gy_ref, rs_ref, gg_ref,
               mask_s, b_s, c_s, dt_s, cum_s, cumt_s, ef_s, la_s, sp_s, sm_s, ssm_s, yd_s, u_s, st_s, rs_s):
    phase, group = pl.program_id(1), pl.program_id(2)
    length = z_ref.shape[0]
    lane = lax.broadcasted_iota(jnp.int32, (length, LANES), 1)
    first = lane < 64
    half = lax.broadcasted_iota(jnp.int32, (BLOCK, LANES), 1) < 64

    @pl.when((phase == 0) & (group == 0))
    def _():
        row, col, same = prologue(heads, bc_ref, dtr_ref, segr_ref, cwbc_ref, hp_ref, mask_s, b_s, c_s, dt_s, cum_s, cumt_s, ef_s, la_s, sp_s)
        scores = dot(c_s[...], b_s[...], NT, precision=highest)
        sm_s[...] = jnp.where(row >= col, scores * same, 0.0)
        st_s[...] = jnp.zeros_like(st_s)

    width = jnp.int32(8)
    shift = lax.rem(jnp.int32(LANES) - width * group, jnp.int32(LANES))

    @pl.when(phase == 0)
    def _():
        masks = [mask_s[k] for k in range(3)]
        dtg = pltpu.roll(dt_s[...], shift, 1)
        cumg = pltpu.roll(cum_s[...], shift, 1)
        efg = pltpu.roll(ef_s[...], shift, 1)
        cumt = cumt_s[pl.ds(pl.multiple_of(group * 8, 8), 8), :]
        square, across = st_s[0], st_s[1]
        for j in range(PAIRS):
            sl = slice(j * LANES, (j + 1) * LANES)
            place = pl.ds(pl.multiple_of(group * GROUP + j * LANES, LANES), LANES)
            xin = x_ref[:, sl]
            summed = conv_sum(conv_taps(xin, masks), cwx_ref[:, sl])
            xs = summed * sigmoid(summed)
            dtb = jnp.where(first, dtg[:, 2 * j : 2 * j + 1], dtg[:, 2 * j + 1 : 2 * j + 2])
            efb = jnp.where(first, efg[:, 2 * j : 2 * j + 1], efg[:, 2 * j + 1 : 2 * j + 2])
            xd = xs * dtb
            for i in range(2):
                rows = slice(i * BLOCK, (i + 1) * BLOCK)
                part = xd[rows]
                stack = jnp.concatenate([jnp.where(half, part, 0.0), jnp.where(half, 0.0, part)], axis=0).astype(bf16)
                decays = []
                for h in range(2):
                    arg = cumg[rows, 2 * j + h : 2 * j + h + 1] - cumt[2 * j + h : 2 * j + h + 1, rows]
                    decays.append((jnp.exp(jnp.minimum(arg, 0.0)) * sm_s[rows, rows]).astype(bf16))
                yd_s[rows, place] = dot(jnp.concatenate(decays, axis=1), stack)
            far = (xd[:BLOCK] * efb[:BLOCK]).astype(bf16)
            u = dot(sm_s[BLOCK:, :BLOCK].astype(bf16), far)
            u_s[:, place] = u
            base = yd_s[:, place] + cp_ref[0:1, sl] * xs
            ssm = jnp.concatenate([base[:BLOCK], base[BLOCK:] + efb[BLOCK:] * u], axis=0)
            ssm_s[:, place] = ssm
            zin = z_ref[:, sl]
            gated = ssm * (zin * sigmoid(zin))
            square = square + gated * gated
            across = across + gm_ref[:, sl] * cp_ref[1:2, sl] * gated
        st_s[0] = square
        st_s[1] = across

    @pl.when((phase == 1) & (group == 0))
    def _():
        inner = heads * 64
        mean = jnp.sum(st_s[0], axis=1, keepdims=True) / inner
        scale = lax.rsqrt(mean + epsilon)
        inward = jnp.sum(st_s[1], axis=1, keepdims=True) / inner
        st_s[0] = jnp.broadcast_to(scale, (length, LANES))
        st_s[1] = jnp.broadcast_to(scale * scale * scale * inward, (length, LANES))
        rs_s[...] = jnp.zeros_like(rs_s)

    @pl.when(phase == 1)
    def _():
        scale, lean = st_s[0], st_s[1]
        efg = pltpu.roll(ef_s[...], shift, 1)
        total = rs_s[...]
        for j in range(PAIRS):
            sl = slice(j * LANES, (j + 1) * LANES)
            place = pl.ds(pl.multiple_of(group * GROUP + j * LANES, LANES), LANES)
            zin = z_ref[:, sl]
            sg = sigmoid(zin)
            silu = zin * sg
            dsilu = sg + silu * (1.0 - sg)
            ssm = ssm_s[:, place]
            gated = ssm * silu
            unit = gated * scale
            gain = cp_ref[1:2, sl]
            gm = gm_ref[:, sl]
            mixed = unit * gain
            mixed_ref[:, sl] = mixed.astype(bf16)
            mixt_ref[sl, :] = mixed.T.astype(bf16)
            gain_sum = jnp.sum(gm * unit, axis=0, keepdims=True)
            old = gg_ref[0:1, place]
            gg_ref[:, place] = jnp.broadcast_to(jnp.where(pl.program_id(0) == 0, gain_sum, old + gain_sum), (8, LANES))
            ggated = scale * (gm * gain) - gated * lean
            gz_ref[:, sl] = (ggated * ssm * dsilu).astype(bf16)
            gy = ggated * silu
            gy_ref[:, sl] = gy
            efb = jnp.where(first, efg[:, 2 * j : 2 * j + 1], efg[:, 2 * j + 1 : 2 * j + 2])
            near = gy.astype(bf16).astype(f32) * yd_s[:, place]
            fare = (gy[BLOCK:] * efb[BLOCK:]).astype(bf16).astype(f32) * u_s[:, place]
            value = jnp.concatenate([near[:BLOCK], near[BLOCK:] + fare], axis=0)
            total = total + headsum(value, headpick(8 * group + 2 * j, (2 * LANES, LANES)))
        rs_s[...] = total
        rs_ref[0] = total


def mixer_back(heads, groups, group, opening, x_ref, bc_ref, dtr_ref, gy_ref, rs_ref, segr_ref, cwx_ref, cwbc_ref, hp_ref, cp_ref,
               px_ref, pr_ref, sg_ref,
               mask_s, b_s, c_s, dt_s, cum_s, cumt_s, ef_s, la_s, sp_s, smt_s, gst_s, gc_s, gd_s):
    length = x_ref.shape[0]
    inner_width = groups * GROUP

    def keep(row, cols, value):
        sg_ref[row : row + 1, cols] = sg_ref[row : row + 1, cols] + value

    @pl.when(opening)
    def _():
        sg_ref[...] = jnp.zeros_like(sg_ref)

    lane = lax.broadcasted_iota(jnp.int32, (length, LANES), 1)
    first = lane < 64
    half = lax.broadcasted_iota(jnp.int32, (BLOCK, LANES), 1) < 64

    @pl.when(group == 0)
    def _():
        row, col, same = prologue(heads, bc_ref, dtr_ref, segr_ref, cwbc_ref, hp_ref, mask_s, b_s, c_s, dt_s, cum_s, cumt_s, ef_s, la_s, sp_s)
        scores = dot(b_s[...], c_s[...], NT, precision=highest)
        smt_s[...] = jnp.where(row <= col, scores * same, 0.0)
        gst_s[...] = jnp.zeros_like(gst_s)
        gc_s[...] = jnp.zeros_like(gc_s)
        gd_s[...] = jnp.zeros_like(gd_s)

    shift = lax.rem(jnp.int32(LANES) - jnp.int32(8) * group, jnp.int32(LANES))
    masks = [mask_s[k] for k in range(3)]
    dtg = pltpu.roll(dt_s[...], shift, 1)
    cumg = pltpu.roll(cum_s[...], shift, 1)
    efg = pltpu.roll(ef_s[...], shift, 1)
    cumt = cumt_s[pl.ds(pl.multiple_of(group * 8, 8), 8), :]
    gcum, gdir = gc_s[...], gd_s[...]
    for j in range(PAIRS):
        sl = slice(j * LANES, (j + 1) * LANES)
        xin = x_ref[:, sl]
        cw = cwx_ref[:, sl]
        summed = conv_sum(conv_taps(xin, masks), cw)
        sg = sigmoid(summed)
        xs = summed * sg
        dtb = jnp.where(first, dtg[:, 2 * j : 2 * j + 1], dtg[:, 2 * j + 1 : 2 * j + 2])
        efb = jnp.where(first, efg[:, 2 * j : 2 * j + 1], efg[:, 2 * j + 1 : 2 * j + 2])
        xd = xs * dtb
        gy = gy_ref[:, sl]
        gyb = gy.astype(bf16)
        inner = []
        for i in range(2):
            rows = slice(i * BLOCK, (i + 1) * BLOCK)
            part, gpart = xd[rows], gy[rows]
            stack = jnp.concatenate([jnp.where(half, part, 0.0), jnp.where(half, 0.0, part)], axis=0).astype(bf16)
            gstack = jnp.concatenate([jnp.where(half, gpart, 0.0), jnp.where(half, 0.0, gpart)], axis=0).astype(bf16)
            gw = dot(stack, gyb[rows], NT)
            weights = []
            gscore = gst_s[rows, rows]
            for h in range(2):
                arg = cumt[2 * j + h : 2 * j + h + 1, rows] - cumg[rows, 2 * j + h : 2 * j + h + 1]
                decay = jnp.exp(jnp.minimum(arg, 0.0))
                weights.append((decay * smt_s[rows, rows]).astype(bf16))
                gscore = gscore + gw[h * BLOCK : (h + 1) * BLOCK] * decay
            gst_s[rows, rows] = gscore
            inner.append(dot(jnp.concatenate(weights, axis=1), gstack))
        far = (xd[:BLOCK] * efb[:BLOCK]).astype(bf16)
        ge = (gy[BLOCK:] * efb[BLOCK:]).astype(bf16)
        gst_s[:BLOCK, BLOCK:] += dot(far, ge, NT)
        gfar = dot(smt_s[:BLOCK, BLOCK:].astype(bf16), ge)
        xdb = xd.astype(bf16).astype(f32)
        fall0 = xdb[:BLOCK] * inner[0] + far.astype(f32) * gfar
        fall = jnp.concatenate([fall0, xdb[BLOCK:] * inner[1]], axis=0)
        gxd = jnp.concatenate([inner[0] + efb[:BLOCK] * gfar, inner[1]], axis=0)
        sums = headsum(jnp.concatenate([fall, xs * gxd], axis=0), headpick(8 * group + 2 * j, (2 * LANES, LANES)))
        gcum = gcum - sums[:length]
        gdir = gdir + sums[length:]
        gxs = cp_ref[0:1, sl] * gy + dtb * gxd
        gsum = gxs * (sg + xs * (1.0 - sg))
        gx, grads = conv_back(gsum, xin, cw, masks, length)
        px_ref[:, sl] = gx.astype(bf16)
        grads.append(jnp.sum(gy * xs, axis=0, keepdims=True))
        place = pl.ds(pl.multiple_of(group * GROUP + j * LANES, LANES), LANES)
        for k, value in enumerate(grads):
            keep(k, place, value)
    gc_s[...] = gcum
    gd_s[...] = gdir

    @pl.when(group == groups - 1)
    def _():
        row = lax.broadcasted_iota(jnp.int32, (length, length), 0)
        col = lax.broadcasted_iota(jnp.int32, (length, length), 1)
        same = segr_ref[0].T[:, 0:1] == segr_ref[0, 0:1, :]
        gscore = jnp.where((row <= col) & same, gst_s[...], 0.0)
        backs = (dot(gscore, c_s[...], precision=highest), dot(gscore.T, b_s[...], precision=highest))
        for part in range(2):
            sl = slice(part * LANES, (part + 1) * LANES)
            xin = bc_ref[:, sl]
            cw = cwbc_ref[:, sl]
            summed = conv_sum(conv_taps(xin, masks), cw)
            sg = sigmoid(summed)
            gsum = backs[part] * (sg + summed * sg * (1.0 - sg))
            gx, grads = conv_back(gsum, xin, cw, masks, length)
            pr_ref[:, sl] = gx.astype(bf16)
            for k, value in enumerate(grads):
                keep(k, slice(inner_width + part * LANES, inner_width + (part + 1) * LANES), value)
        upper = jnp.where(row <= col, 1.0, 0.0).astype(f32)
        gla = dot(upper, gc_s[...] + rs_ref[0], precision=highest)
        graw = (gd_s[...] - gla * jnp.exp(hp_ref[1:2, :])) * sp_s[...]
        graw = jnp.where(lane < heads, graw, 0.0)
        pr_ref[:, 2 * LANES :] = graw.astype(bf16)
        tail = slice(inner_width + 2 * LANES, inner_width + 3 * LANES)
        keep(0, tail, jnp.sum(graw, axis=0, keepdims=True))
        keep(1, tail, jnp.sum(jnp.where(lane < heads, gla * la_s[...], 0.0), axis=0, keepdims=True))


def small_scratch(length):
    return [
        pltpu.VMEM((3, length, LANES), f32),
        pltpu.VMEM((length, LANES), f32),
        pltpu.VMEM((length, LANES), f32),
        pltpu.VMEM((length, LANES), f32),
        pltpu.VMEM((length, LANES), f32),
        pltpu.VMEM((LANES, length), f32),
        pltpu.VMEM((length, LANES), f32),
        pltpu.VMEM((length, LANES), f32),
        pltpu.VMEM((length, LANES), f32),
    ]


def mixer_forward(projected, gm, segr, cw, hp, cp, heads, state):
    seqs, _, length = segr.shape
    inner = gm.shape[1]
    groups = inner // GROUP
    rows = seqs * length
    kernel = functools.partial(fwd_kernel, heads)
    out_row = lambda b, p, g: (b, g * p)
    return pl.pallas_call(
        kernel,
        grid=(seqs, 2, groups),
        in_specs=[
            pl.BlockSpec((length, GROUP), lambda b, p, g: (b, g)),
            pl.BlockSpec((length, GROUP), lambda b, p, g: (b, groups + g * (1 - p) + (groups - 1) * p)),
            pl.BlockSpec((length, 2 * state), lambda b, p, g: (b, 2 * inner // (2 * state))),
            pl.BlockSpec((length, LANES), lambda b, p, g: (b, (2 * inner + 2 * state) // LANES)),
            pl.BlockSpec((length, GROUP), lambda b, p, g: (b, g)),
            pl.BlockSpec((1, 8, length), lambda b, p, g: (b, 0, 0)),
            pl.BlockSpec((8, GROUP), lambda b, p, g: (0, g)),
            pl.BlockSpec((8, 2 * state), lambda b, p, g: (0, inner // (2 * state))),
            pl.BlockSpec((8, LANES), lambda b, p, g: (0, 0)),
            pl.BlockSpec((8, GROUP), lambda b, p, g: (0, g)),
        ],
        out_specs=[
            pl.BlockSpec((length, GROUP), out_row),
            pl.BlockSpec((GROUP, length), lambda b, p, g: (g * p, b)),
            pl.BlockSpec((length, GROUP), out_row),
            pl.BlockSpec((length, GROUP), out_row),
            pl.BlockSpec((1, length, LANES), lambda b, p, g: (b, 0, 0)),
            pl.BlockSpec((8, inner), lambda b, p, g: (0, 0)),
        ],
        out_shape=[
            jax.ShapeDtypeStruct((rows, inner), bf16),
            jax.ShapeDtypeStruct((inner, rows), bf16),
            jax.ShapeDtypeStruct((rows, inner), bf16),
            jax.ShapeDtypeStruct((rows, inner), f32),
            jax.ShapeDtypeStruct((seqs, length, LANES), f32),
            jax.ShapeDtypeStruct((8, inner), f32),
        ],
        scratch_shapes=small_scratch(length) + [
            pltpu.VMEM((length, length), f32),
            pltpu.VMEM((length, inner), f32),
            pltpu.VMEM((length, inner), f32),
            pltpu.VMEM((length - BLOCK, inner), f32),
            pltpu.VMEM((2, length, LANES), f32),
            pltpu.VMEM((length, LANES), f32),
        ],
        compiler_params=pltpu.CompilerParams(vmem_limit_bytes=48 << 20),
        cost_estimate=pl.CostEstimate(flops=10**10, bytes_accessed=45 * 10**6, transcendentals=10**7),
        name="mixer_forward",
    )(projected, projected, projected, projected, gm, segr, cw, cw, hp, cp)


def pad_lanes(v, width=LANES):
    return jnp.pad(v, ((0, 0), (0, width - v.shape[1])))


def mixer_tables(segments, kernel_full, shift_full, dt_bias, a_log, d_skip, gate_full):
    taps = kernel_full.shape[0]
    seqs, length = segments.shape
    segr = jnp.broadcast_to(segments.astype(f32)[:, None, :], (seqs, 8, length))
    cw = jnp.concatenate([kernel_full.astype(f32), jnp.broadcast_to(shift_full.astype(f32)[None], (8 - taps, shift_full.shape[0]))])
    hp = pad_lanes(jnp.concatenate([dt_bias[None], jnp.broadcast_to(a_log[None], (7, a_log.shape[0]))]))
    heads = dt_bias.shape[0]
    size = gate_full.shape[0] // heads
    cp = jnp.concatenate([jnp.repeat(d_skip, size)[None], jnp.broadcast_to(gate_full.astype(f32)[None], (7, gate_full.shape[0]))])
    return segr, cw, hp, cp


MESH = pl.DeviceIdType.MESH
PIECES = 3


def ring_place(chip, chips):
    wide = chips // 4
    z, q = chip // wide, chip % wide
    up = 1 + 3 * q + jnp.where(q % 2 == 0, z - 1, 3 - z)
    back = jnp.where(q == 0, 0, 4 * wide - q)
    return jnp.where(z == 0, back, up)


def ring_chip(place, chips):
    wide = chips // 4
    place = place % chips
    q = (place - 1 + chips) % chips // 3
    r = (place - 1 + chips) % chips % 3
    z = jnp.where(q % 2 == 0, 1 + r, 3 - r)
    inner = z * wide + q
    outer = (4 * wide - place) % (4 * wide)
    return jnp.where((place == 0) | (place > 3 * wide), outer, inner)


def gather_kernel(chips, count, *refs):
    ins, outs = refs[:count], refs[count : 2 * count]
    ring_send, ring_recv, far_send, far_recv, pair_send, pair_recv, own_sem = refs[2 * count :]
    me = lax.axis_index("fsdp")
    plane = lax.axis_index("dp")
    chip, core = me // 2, me % 2
    place = ring_place(chip, chips)
    right = 2 * ring_chip(place + 1, chips) + core
    left = 2 * ring_chip(place + chips - 1, chips) + core
    pair = {"fsdp": me + 1 - 2 * core}
    peer = {"dp": 1 - plane}
    ways = ({"fsdp": right}, {"fsdp": left})

    barrier = pltpu.get_barrier_semaphore()
    for other in (ways[0], ways[1], pair, peer):
        pl.semaphore_signal(barrier, inc=1, device_id=other, device_id_type=MESH)
    pl.semaphore_wait(barrier, 4)

    half = chips // 2
    whole = [k == count - 1 for k in range(count)]

    def steps(way, slot):
        return half if way == slot else half - 1

    def owner(way, step):
        move = -step if way == 0 else step
        return 2 * ring_chip(place + move + chips, chips) + core

    def part(refs, k, index, slot):
        if whole[k]:
            return refs[k].at[index]
        piece = 0 if slot == 0 else 1 + plane
        return refs[k].at[index, piece]

    def mine(k, slot):
        if whole[k]:
            return ins[k]
        piece = 0 if slot == 0 else 1 + plane
        return ins[k].at[piece]

    def slots(k):
        return (0,) if whole[k] else (0, 1)

    pending = []

    def send(source, target, send_sem, recv_sem, device):
        copy = pltpu.make_async_remote_copy(
            src_ref=source, dst_ref=target, send_sem=send_sem, recv_sem=recv_sem, device_id=device, device_id_type=MESH)
        copy.start()
        pending.append(copy)

    def arrived(target, send_sem, recv_sem):
        pltpu.make_async_remote_copy(
            src_ref=target, dst_ref=target, send_sem=send_sem, recv_sem=recv_sem, device_id=pair, device_id_type=MESH).wait_recv()

    def ring_sem(sem, way, step, k, slot):
        return sem.at[(way * half + step - 1) * 2 * count + 2 * k + slot]

    def far_sem(sem, way, step, k):
        return sem.at[(way * half + step - 1) * count + k]

    def pair_sem(sem, turn, k, slot):
        return sem.at[(turn * count + k) * 3 + slot]

    def turn(way, step):
        return 1 + (step - 1) * 2 + way

    local = []
    for k in range(count):
        for slot in slots(k):
            for way in range(2):
                send(mine(k, slot), part(outs, k, me, slot), ring_sem(ring_send, way, 1, k, slot), ring_sem(ring_recv, way, 1, k, slot), ways[way])
        send(ins[k], outs[k].at[me], pair_sem(pair_send, 0, k, 0), pair_sem(pair_recv, 0, k, 0), pair)
        copy = pltpu.make_async_copy(ins[k], outs[k].at[me], own_sem.at[k])
        copy.start()
        local.append(copy)

    def from_peer(way, step):
        index = owner(way, step)
        for k in range(count):
            if whole[k] or step > steps(way, 1):
                continue
            target = outs[k].at[index, 2 - plane]
            arrived(target, far_sem(far_send, way, step, k), far_sem(far_recv, way, step, k))
            send(target, target, pair_sem(pair_send, turn(way, step), k, 2), pair_sem(pair_recv, turn(way, step), k, 2), pair)

    for step in range(1, half + 1):
        for way in range(2):
            index = owner(way, step)
            for k in range(count):
                for slot in slots(k):
                    if step > steps(way, slot):
                        continue
                    target = part(outs, k, index, slot)
                    arrived(target, ring_sem(ring_send, way, step, k, slot), ring_sem(ring_recv, way, step, k, slot))
                    if step + 1 <= steps(way, slot):
                        send(target, target, ring_sem(ring_send, way, step + 1, k, slot), ring_sem(ring_recv, way, step + 1, k, slot), ways[way])
                    if slot == 1:
                        send(target, target, far_sem(far_send, way, step, k), far_sem(far_recv, way, step, k), peer)
                    send(target, target, pair_sem(pair_send, turn(way, step), k, slot), pair_sem(pair_recv, turn(way, step), k, slot), pair)
        if step > 1:
            for way in range(2):
                from_peer(way, step - 1)
    for way in range(2):
        from_peer(way, half)
    for k in range(count):
        other = outs[k].at[me + 1 - 2 * core]
        arrived(other, pair_sem(pair_send, 0, k, 0), pair_sem(pair_recv, 0, k, 0))
    for step in range(1, half + 1):
        for way in range(2):
            index = owner(way, step) + 1 - 2 * core
            for k in range(count):
                for slot in slots(k) + (() if whole[k] else (2,)):
                    if step > steps(way, min(slot, 1)):
                        continue
                    if slot == 2:
                        target = outs[k].at[index, 2 - plane]
                    else:
                        target = part(outs, k, index, slot)
                    sems = turn(way, step), k, slot
                    arrived(target, pair_sem(pair_send, *sems), pair_sem(pair_recv, *sems))
    for copy in local:
        copy.wait()
    for copy in pending:
        copy.wait_send()


def gather(arrays, devices):
    count = len(arrays)
    chips = devices // 2
    half = chips // 2
    dma = pltpu.SemaphoreType.DMA
    return pl.pallas_call(
        functools.partial(gather_kernel, chips, count),
        in_specs=[pl.BlockSpec(memory_space=pl.ANY)] * count,
        out_specs=[pl.BlockSpec(memory_space=pl.ANY)] * count,
        out_shape=[jax.ShapeDtypeStruct((devices,) + a.shape, a.dtype) for a in arrays],
        scratch_shapes=[
            dma((4 * half * count,)), dma((4 * half * count,)),
            dma((2 * half * count,)), dma((2 * half * count,)),
            dma(((2 * half + 1) * count * 3,)), dma(((2 * half + 1) * count * 3,)),
            dma((count,)),
        ],
        compiler_params=pltpu.CompilerParams(collective_id=0, has_side_effects=True),
        name="gather_weights",
    )(*arrays)


QUARTERS = 4
TILE = 512
FULL = 62 << 20


def add_up(sources, store, width):
    tile = min(TILE, width)

    def total(cols):
        value = sources[0][:, cols].astype(f32)
        for source in sources[1:]:
            value = value + source[:, cols].astype(f32)
        store[:, cols] = value.astype(store.dtype)

    def one(i, carry):
        total(pl.ds(pl.multiple_of(i * tile, LANES), tile))
        return carry

    lax.fori_loop(0, width // tile, one, 0)
    if width % tile:
        total(slice(width - width % tile, width))


class Links:
    def __init__(self, chips):
        self.chips, self.half = chips, chips // 2
        me = lax.axis_index("fsdp")
        self.plane = lax.axis_index("dp")
        self.chip, self.core = me // 2, me % 2
        self.place = ring_place(self.chip, chips)
        self.ways = tuple(
            {"fsdp": 2 * ring_chip(self.place + move, chips) + self.core} for move in (1, chips - 1))
        self.peer = {"dp": 1 - self.plane}
        self.pair = {"fsdp": me + 1 - 2 * self.core}
        self.turns = [{"fsdp": me + bit - 2 * bit * ((me // bit) % 2)} for bit in (1 << k for k in range(chips.bit_length()))] + [self.peer]
        self.sent = []

    def greet(self, others):
        barrier = pltpu.get_barrier_semaphore()
        for other in others:
            pl.semaphore_signal(barrier, inc=1, device_id=other, device_id_type=MESH)
        pl.semaphore_wait(barrier, len(others))

    def send(self, source, target, send_sem, recv_sem, device):
        make = lambda: pltpu.make_async_remote_copy(
            src_ref=source(), dst_ref=target(), send_sem=send_sem(), recv_sem=recv_sem(), device_id=device, device_id_type=MESH)
        make().start()
        self.sent.append(make)

    def arrived(self, target, send_sem, recv_sem):
        pltpu.make_async_remote_copy(
            src_ref=target, dst_ref=target, send_sem=send_sem, recv_sem=recv_sem, device_id=self.peer, device_id_type=MESH).wait_recv()

    def finish(self):
        for make in self.sent:
            make().wait_send()


class Ring:
    def __init__(self, links, items, shift, parts, held, ring_in, ring_out, peer_in, held_sem, ring_send, ring_recv, peer_send, peer_recv):
        self.links, self.items, self.shift, self.parts = links, items, shift, parts
        self.held, self.ring_in, self.ring_out, self.peer_in = held, ring_in, ring_out, peer_in
        self.held_sem, self.ring_send, self.ring_recv = held_sem, ring_send, ring_recv
        self.peer_send, self.peer_recv = peer_send, peer_recv

    def hops(self, k, way, slot):
        return self.links.half - (slot + (k + self.shift if slot == 2 else 0) + way) % 2

    def target(self, k, way, slot, step):
        chips = self.links.chips
        ahead = self.hops(k, way, slot) - step + 1
        return ring_chip(self.links.place + (ahead if way == 0 else chips - ahead), chips)

    def quarter(self, slot):
        return slot if slot < 2 else 2 + self.links.plane

    def at(self, way, step, slot):
        return (way * self.links.half + step - 1) * 3 + slot

    def sems(self, k, way, step, slot):
        at = k * 6 * self.links.half + self.at(way, step, slot)
        return self.ring_send.at[at], self.ring_recv.at[at]

    def push(self, k, way, step, slot, source):
        at = self.at(way, step, slot)
        self.links.send(
            source, lambda: self.ring_in[k].at[at],
            lambda: self.sems(k, way, step, slot)[0], lambda: self.sems(k, way, step, slot)[1], self.links.ways[way])

    def start(self):
        links, count = self.links, len(self.items)
        for slot in (0, 1):
            for k in range(count):
                for way in range(2):
                    self.push(k, way, 1, slot, lambda k=k, way=way, slot=slot: self.parts[k].at[self.target(k, way, slot, 1), slot])
        for move in self.order():
            for k in range(count):
                def where(move=move):
                    return (links.place + move) % links.chips
                links.send(
                    lambda k=k, where=where: self.parts[k].at[ring_chip(where(), links.chips), 3 - links.plane],
                    lambda k=k, where=where: self.peer_in[k].at[where()],
                    lambda k=k, where=where: self.peer_send.at[k * links.chips + where()],
                    lambda k=k, where=where: self.peer_recv.at[k * links.chips + where()], links.peer)
        for copy in self.loads():
            copy.start()

    def order(self):
        chips, half = self.links.chips, self.links.half
        moves = []
        for ahead in range(half, -1, -1):
            moves.append(ahead)
            if 0 < ahead < half:
                moves.append(chips - ahead)
        return moves

    def loads(self):
        return [
            pltpu.make_async_copy(self.parts[k].at[:, self.quarter(slot)], self.held[k].at[slot], self.held_sem.at[k * 3 + slot])
            for k in range(len(self.items)) for slot in range(3)]

    def from_peer(self, k, chunk):
        where = ring_place(chunk, self.links.chips)
        at = k * self.links.chips + where
        self.links.arrived(self.peer_in[k].at[where], self.peer_send.at[at], self.peer_recv.at[at])
        return self.peer_in[k].at[where]

    def hop(self, step, slot):
        for k in range(len(self.items)):
            for way in range(2):
                if step > self.hops(k, way, slot) or (step == 1 and slot < 2):
                    continue
                chunk = self.target(k, way, slot, step)
                sources = [self.held[k].at[slot, chunk]]
                if step > 1:
                    before = self.at(way, step - 1, slot)
                    self.links.arrived(self.ring_in[k].at[before], *self.sems(k, way, step - 1, slot))
                    sources.append(self.ring_in[k].at[before])
                if slot == 2:
                    sources.append(self.from_peer(k, chunk))
                at = self.at(way, step, slot)
                add_up(sources, self.ring_out[k].at[at], self.items[k][1])
                self.push(k, way, step, slot, lambda k=k, at=at: self.ring_out[k].at[at])

    def land(self, k, slot, store):
        links = self.links
        sources = [self.held[k].at[slot, links.chip]]
        for way in range(2):
            last = self.hops(k, way, slot)
            at = self.at(way, last, slot)
            links.arrived(self.ring_in[k].at[at], *self.sems(k, way, last, slot))
            sources.append(self.ring_in[k].at[at])
        if slot == 2:
            sources.append(self.from_peer(k, links.chip))
        add_up(sources, store, self.items[k][1])


def ring_scratch(items, chips):
    dma = pltpu.SemaphoreType.DMA
    half, count = chips // 2, len(items)
    vm = lambda *lead: [pltpu.VMEM(lead + item, bf16) for item in items]
    return vm(3, chips) + vm(6 * half) + vm(6 * half) + vm(chips) + [
        dma((3 * count,)), dma((6 * half * count,)), dma((6 * half * count,)), dma((chips * count,)), dma((chips * count,))]


def split_scratch(refs, count):
    return [refs[i * count : (i + 1) * count] for i in range(4)], refs[4 * count : 4 * count + 5]


def middle_kernel(heads, chips, seqs, groups, items, x_ref, bc_ref, dtr_ref, gy_ref, rs_ref, segr_ref, cwx_ref, cwbc_ref, hp_ref, cp_ref,
                  gg_ref, mixed_ref, wout_ref, tok_ref, gz_ref, win_ref, *refs):
    count = len(items)
    parts, refs = refs[:count], refs[count:]
    px_ref, pr_ref, px2_ref, pr2_ref, sg_ref, bo_ref, gn_ref = refs[:7]
    owns, refs = refs[7 : 7 + count], refs[7 + count :]
    back, (acc, pxs, prs, px_send, px_recv, pr_send, pr_recv), refs = refs[:13], refs[13:20], refs[20:]
    (held, ring_in, ring_out, peer_in), sems = split_scratch(refs, count)
    step = pl.program_id(0)
    turns = seqs * groups
    last = turns + 2 * groups - 1
    length = x_ref.shape[0]
    links = Links(chips)
    ring = Ring(links, items, 0, parts, held, ring_in, ring_out, peer_in, *sems)

    @pl.when(step == 0)
    def _():
        links.greet([links.ways[0], links.ways[1], links.peer, links.pair])
        ring.start()

    plan = {}
    for q in range(2, 3 * links.half):
        plan.setdefault(min(last, max(3, (24 // (links.half * 2)) * (q - 1))), []).append((q // 3 + 1, q % 3))

    def px_copy(turn):
        rows = pl.ds(pl.multiple_of(turn // groups * length, length), length)
        cols = pl.ds(pl.multiple_of(turn % groups * GROUP, GROUP), GROUP)
        return pltpu.make_async_remote_copy(
            src_ref=pxs.at[turn], dst_ref=px2_ref.at[rows, cols], send_sem=px_send.at[turn], recv_sem=px_recv.at[turn],
            device_id=links.pair, device_id_type=MESH)

    def pr_copy(seq):
        rows = pl.ds(pl.multiple_of(seq * length, length), length)
        return pltpu.make_async_remote_copy(
            src_ref=prs.at[seq], dst_ref=pr2_ref.at[rows, :], send_sem=pr_send.at[seq], recv_sem=pr_recv.at[seq],
            device_id=links.pair, device_id_type=MESH)

    @pl.when(step < turns)
    def _():
        group = step % groups
        mixer_back(heads, groups, group, step == 0, x_ref, bc_ref, dtr_ref, gy_ref, rs_ref, segr_ref, cwx_ref, cwbc_ref, hp_ref, cp_ref,
                   px_ref, pr_ref, sg_ref, *back)
        pxs[step] = px_ref[...]
        px_copy(step).start()

        @pl.when(group == groups - 1)
        def _():
            seq = step // groups
            prs[seq] = pr_ref[...]
            pr_copy(seq).start()

    @pl.when((step >= turns) & (step < turns + groups))
    def _():
        part = dot(mixed_ref[...], wout_ref[...])

        @pl.when(step == turns)
        def _():
            acc[...] = tok_ref[...].astype(f32) + part

        @pl.when((step > turns) & (step < turns + groups - 1))
        def _():
            acc[...] += part

        @pl.when(step == turns + groups - 1)
        def _():
            bo_ref[...] = (acc[...] + part).astype(bf16)

    @pl.when(step >= turns + groups)
    def _():
        part = dot(gz_ref[...], win_ref[...], NT)

        @pl.when(step == turns + groups)
        def _():
            gn_ref[...] = part

        @pl.when(step > turns + groups)
        def _():
            gn_ref[...] += part

    for when in sorted(plan):
        @pl.when(step == when)
        def _(when=when):
            if when == min(plan):
                for copy in ring.loads():
                    copy.wait()
            for hop, slot in plan[when]:
                ring.hop(hop, slot)

    @pl.when(step == last)
    def _():
        sg_ref[6:7, : gg_ref.shape[1]] = gg_ref[0:1, :]
        for slot in range(3):
            for k in range(count):
                ring.land(k, slot, owns[k].at[slot])
        for turn in range(turns):
            px_copy(turn).wait()
        for seq in range(seqs):
            pr_copy(seq).wait()
        links.finish()


def middle(projected, gy, rs, segr, cw, hp, cp, gg, mixed, w_out_full, tokens, gz, w_in_full, arrays, heads, state, devices):
    seqs, _, length = segr.shape
    inner = gy.shape[1]
    width = tokens.shape[1]
    groups = inner // GROUP
    rows = seqs * length
    turns = seqs * groups
    chips = devices // 2
    items = tuple(a.shape[2:] for a in arrays)
    count = len(items)
    dma = pltpu.SemaphoreType.DMA
    seq = lambda i: jnp.minimum(i // groups, seqs - 1)
    grp = lambda i: jnp.where(i < turns, i % groups, groups - 1)
    out_at = lambda i: jnp.clip(i - turns, 0, groups - 1)
    in_at = lambda i: jnp.clip(i - turns - groups, 0, groups - 1)
    const = lambda *shape: pl.BlockSpec(shape, lambda i: (0,) * len(shape), pipeline_mode=pl.Buffered(1))
    any_spec = pl.BlockSpec(memory_space=pl.ANY)
    small_width = inner + 3 * LANES
    return pl.pallas_call(
        functools.partial(middle_kernel, heads, chips, seqs, groups, items),
        grid=(turns + 2 * groups,),
        in_specs=[
            pl.BlockSpec((length, GROUP), lambda i: (seq(i), groups + grp(i))),
            pl.BlockSpec((length, 2 * state), lambda i: (seq(i), 2 * inner // (2 * state))),
            pl.BlockSpec((length, LANES), lambda i: (seq(i), (2 * inner + 2 * state) // LANES)),
            pl.BlockSpec((length, GROUP), lambda i: (seq(i), grp(i))),
            pl.BlockSpec((1, length, LANES), lambda i: (seq(i), 0, 0)),
            pl.BlockSpec((1, 8, length), lambda i: (seq(i), 0, 0)),
            pl.BlockSpec((8, GROUP), lambda i: (0, grp(i))),
            pl.BlockSpec((8, 2 * state), lambda i: (0, inner // (2 * state))),
            pl.BlockSpec((8, LANES), lambda i: (0, 0)),
            pl.BlockSpec((8, GROUP), lambda i: (0, grp(i))),
            const(8, inner),
            pl.BlockSpec((rows, GROUP), lambda i: (0, out_at(i))),
            pl.BlockSpec((GROUP, width), lambda i: (out_at(i), 0)),
            const(rows, width),
            pl.BlockSpec((rows, GROUP), lambda i: (0, in_at(i))),
            pl.BlockSpec((width, GROUP), lambda i: (0, in_at(i))),
        ] + [any_spec] * count,
        out_specs=[
            pl.BlockSpec((length, GROUP), lambda i: (seq(i), grp(i))),
            pl.BlockSpec((length, 3 * LANES), lambda i: (seq(i), 0)),
            any_spec,
            any_spec,
            const(8, small_width),
            const(rows, width),
            const(rows, width),
        ] + [const(3, *item) for item in items],
        out_shape=[
            jax.ShapeDtypeStruct((rows, inner), bf16),
            jax.ShapeDtypeStruct((rows, 3 * LANES), bf16),
            jax.ShapeDtypeStruct((rows, inner), bf16),
            jax.ShapeDtypeStruct((rows, 3 * LANES), bf16),
            jax.ShapeDtypeStruct((8, small_width), f32),
            jax.ShapeDtypeStruct((rows, width), bf16),
            jax.ShapeDtypeStruct((rows, width), f32),
        ] + [jax.ShapeDtypeStruct((3,) + item, bf16) for item in items],
        scratch_shapes=small_scratch(length) + [
            pltpu.VMEM((length, length), f32),
            pltpu.VMEM((length, length), f32),
            pltpu.VMEM((length, LANES), f32),
            pltpu.VMEM((length, LANES), f32),
            pltpu.VMEM((rows, width), f32),
            pltpu.VMEM((turns, length, GROUP), bf16),
            pltpu.VMEM((seqs, length, 3 * LANES), bf16),
            dma((turns,)), dma((turns,)), dma((seqs,)), dma((seqs,)),
        ] + ring_scratch(items, chips),
        compiler_params=pltpu.CompilerParams(collective_id=1, has_side_effects=True, vmem_limit_bytes=FULL),
        name="middle",
    )(projected, projected, projected, gy, rs, segr, cw, cw, hp, cp, gg, mixed, w_out_full, tokens, gz, w_in_full, *arrays)


def tail_kernel(chips, groups, used, items, early, px_ref, pr_ref, win_ref, gacc_ref, tok_ref, cot_ref, gain_ref, sg_ref, *refs):
    count, first = len(items), len(early)
    parts, halves, refs = refs[:count], refs[count : count + first], refs[count + first :]
    gt_ref, small_ref, refs = refs[0], refs[1], refs[2:]
    outs, refs = refs[: first + count], refs[first + count :]
    last_in, last_out, refs = refs[: first + count], refs[first + count : first + 2 * count], refs[first + 2 * count :]
    (small_in, small_sent, small_recv, small_send, small_sem, last_send, last_recv, half_sem), refs = refs[:8], refs[8:]
    early_held, refs = refs[:first], refs[first:]
    (held, ring_in, ring_out, peer_in), sems = split_scratch(refs, count)
    step = pl.program_id(0)
    links = Links(chips)
    ring = Ring(links, items, 0, parts, held, ring_in, ring_out, peer_in, *sems)
    rounds = len(links.turns)

    def swap(k, slot, source):
        at = k * 3 + slot
        links.send(source, lambda: last_in[k].at[slot], lambda: last_send.at[at], lambda: last_recv.at[at], links.peer)

    def settle(k, slot, mine):
        at = k * 3 + slot
        width = outs[k].shape[2]
        links.arrived(last_in[k].at[slot], last_send.at[at], last_recv.at[at])
        if slot < 2:
            add_up([mine, last_in[k].at[slot]], outs[k].at[slot], width)
        else:
            add_up([mine], outs[k].at[2 + links.plane], width)
            add_up([last_in[k].at[slot]], outs[k].at[3 - links.plane], width)

    halves_in = lambda: [pltpu.make_async_copy(halves[k], early_held[k], half_sem.at[k]) for k in range(first)]

    @pl.when(step == 0)
    def _():
        links.greet(list(links.ways) + links.turns)
        ring.start()
        for slot in range(3):
            for k in range(first):
                swap(k, slot, lambda k=k, slot=slot: halves[k].at[slot])
        for copy in halves_in():
            copy.start()
        gt_ref[...] = gacc_ref[...] + dot(px_ref[...], win_ref[...], NT)

    @pl.when((step > 0) & (step < groups))
    def _():
        gt_ref[...] += dot(px_ref[...], win_ref[...], NT)

    @pl.when(step == 2)
    def _():
        for copy in ring.loads():
            copy.wait()
        ring.hop(1, 2)

    @pl.when(step == groups - 1)
    def _():
        ring.hop(2, 0)

    def small_round(turn):
        links.send(
            lambda: small_in if turn == 0 else small_sent.at[turn - 1], lambda: small_recv.at[turn],
            lambda: small_send.at[turn], lambda: small_sem.at[turn], links.turns[turn])

    def small_finish(turn):
        value = small_in if turn == 0 else small_sent.at[turn - 1]
        links.arrived(small_recv.at[turn], small_send.at[turn], small_sem.at[turn])
        store = small_ref if turn == rounds - 1 else small_sent.at[turn]
        store[...] = value[...] + small_recv[turn]

    @pl.when(step == groups)
    def _():
        size = pr_ref.shape[1]
        col = lax.broadcasted_iota(jnp.int32, (win_ref.shape[0], size), 1)
        rest = jnp.where(col < used, win_ref[:, :size].astype(f32), 0.0).astype(bf16)
        rows, width = gt_ref.shape
        total = jnp.zeros((1, width), f32)
        for i in range(rows // BLOCK):
            sl = slice(i * BLOCK, (i + 1) * BLOCK)
            u = tok_ref[sl].astype(f32)
            rstd = lax.rsqrt(jnp.mean(u * u, axis=1, keepdims=True) + epsilon)
            unit = u * rstd
            gn = gt_ref[sl] + dot(pr_ref[sl], rest, NT)
            total = total + jnp.sum(gn * unit, axis=0, keepdims=True)
            gu = gn * gain_ref[0:1, :]
            inward = jnp.mean(gu * unit, axis=1, keepdims=True)
            gt_ref[sl] = cot_ref[sl].astype(f32) + rstd * (gu - unit * inward)
        small_in[...] = sg_ref[...]
        small_in[7:8, :width] = total
        small_round(0)
        done = 0
        hops = [(q // 3 + 1, q % 3) for q in range(4, 3 * links.half)]
        every = max(1, len(hops) // rounds)
        for n, (hop, slot) in enumerate(hops):
            ring.hop(hop, slot)
            if n % every == every - 1 and done < rounds - 1:
                small_finish(done)
                done += 1
                small_round(done)
        for slot in range(3):
            for k in range(count):
                ring.land(k, slot, last_out[k].at[slot])
                swap(first + k, slot, lambda k=k, slot=slot: last_out[k].at[slot])
        while done < rounds:
            small_finish(done)
            done += 1
            if done < rounds:
                small_round(done)
        for copy in halves_in():
            copy.wait()
        for slot in range(3):
            for k in range(first):
                settle(k, slot, early_held[k].at[slot])
        for slot in range(3):
            for k in range(count):
                settle(first + k, slot, last_out[k].at[slot])
        links.finish()


def tail(px, pr, w_in_full, gacc, tokens, cot, gain, sg, arrays, halves, used, devices):
    rows, width = tokens.shape
    groups = px.shape[1] // GROUP
    chips = devices // 2
    items = tuple(a.shape[2:] for a in arrays)
    early = tuple(h.shape[1:] for h in halves)
    count, first = len(items), len(early)
    rounds = chips.bit_length() + 1
    dma = pltpu.SemaphoreType.DMA
    const = lambda *shape: pl.BlockSpec(shape, lambda i: (0,) * len(shape), pipeline_mode=pl.Buffered(1))
    any_spec = pl.BlockSpec(memory_space=pl.ANY)
    every = early + items
    return pl.pallas_call(
        functools.partial(tail_kernel, chips, groups, used, items, early),
        grid=(groups + 1,),
        in_specs=[
            pl.BlockSpec((rows, GROUP), lambda i: (0, jnp.minimum(i, groups - 1))),
            const(rows, pr.shape[1]),
            pl.BlockSpec((width, GROUP), lambda i: (0, groups + i)),
            const(rows, width),
            const(rows, width),
            const(rows, width),
            const(8, width),
            const(*sg.shape),
        ] + [any_spec] * (count + first),
        out_specs=[const(rows, width), const(*sg.shape)] + [const(4, *item) for item in every],
        out_shape=[jax.ShapeDtypeStruct((rows, width), f32), jax.ShapeDtypeStruct(sg.shape, f32)]
        + [jax.ShapeDtypeStruct((4,) + item, f32) for item in every],
        scratch_shapes=[pltpu.VMEM((3,) + item, bf16) for item in every] + [pltpu.VMEM((3,) + item, bf16) for item in items] + [
            pltpu.VMEM(sg.shape, f32), pltpu.VMEM((rounds,) + sg.shape, f32), pltpu.VMEM((rounds,) + sg.shape, f32),
            dma((rounds,)), dma((rounds,)), dma((3 * (first + count),)), dma((3 * (first + count),)), dma((first,)),
        ] + [pltpu.VMEM((3,) + item, bf16) for item in early] + ring_scratch(items, chips),
        compiler_params=pltpu.CompilerParams(collective_id=2, has_side_effects=True, vmem_limit_bytes=FULL),
        name="tail",
    )(px, pr, w_in_full, gacc, tokens, cot, gain, sg, *arrays, *halves)


def parts_kernel(core_ref, a_ref, a2_ref, b_ref, b2_ref, o_ref):
    rows = o_ref.shape[0]
    a = a_ref[...].reshape(rows, a_ref.shape[3])
    a2 = a2_ref[...].reshape(rows, a2_ref.shape[3])
    o_ref[...] = (dot(a, b_ref[...]) + dot(a2, b2_ref[...])).astype(bf16)


def grad_parts(core, left, left2, right, right2, name):
    chips, _, rows, tokens = left.shape
    if rows % 16:
        pick = lambda v: lax.dynamic_index_in_dim(v, core, 1, keepdims=False).reshape(1, 1, chips * rows, tokens)
        left, left2, core, chips, rows = pick(left), pick(left2), 0, 1, chips * rows
    width = right.shape[1]
    tile = min(GROUP, width)
    left_spec = pl.BlockSpec((chips, 1, rows, tokens), lambda i, c: (0, c[0], 0, 0), pipeline_mode=pl.Buffered(1))
    total = chips * rows
    return pl.pallas_call(
        parts_kernel,
        grid_spec=pltpu.PrefetchScalarGridSpec(
            num_scalar_prefetch=1,
            grid=(width // tile,),
            in_specs=[
                left_spec, left_spec,
                pl.BlockSpec((tokens, tile), lambda i, c: (0, i)),
                pl.BlockSpec((tokens, tile), lambda i, c: (0, i)),
            ],
            out_specs=pl.BlockSpec((total, tile), lambda i, c: (0, i)),
        ),
        out_shape=jax.ShapeDtypeStruct((total, width), bf16),
        compiler_params=pltpu.CompilerParams(vmem_limit_bytes=FULL),
        cost_estimate=pl.CostEstimate(flops=4 * total * tokens * width, bytes_accessed=2 * (2 * total * tokens + 2 * tokens * width + total * width), transcendentals=0),
        name=name,
    )(jnp.full((1,), core, jnp.int32), left, left2, right, right2)


def small_rows(size):
    return 16 * (-(-size // (16 * LANES)))


def flat_pack(parts, rows):
    flat = jnp.concatenate([p.reshape(-1) for p in parts])
    return jnp.pad(flat, (0, rows * LANES - flat.shape[0])).reshape(rows, LANES)


def local(devices, tokens, segments, norm_gain, w_in, conv_weight, conv_bias, dt_bias, a_log, d_skip, gate_gain, w_out, cotangent):
    seqs, length, width = tokens.shape
    rows = seqs * length
    proj_width = w_in.shape[1]
    inner = devices * w_out.shape[0]
    taps = conv_weight.shape[0]
    heads = dt_bias.shape[0]
    share_n, share_c, share_g = norm_gain.shape[0], conv_bias.shape[0], gate_gain.shape[0]
    conv_width = devices * share_c
    state = (conv_width - inner) // 2
    chips = devices // 2
    me = lax.axis_index("fsdp")
    core = me % 2
    swap = [(i, i + 1 - 2 * (i % 2)) for i in range(devices)]
    partner = lambda value: lax.ppermute(value, "fsdp", swap)

    size = share_n + share_g + (taps + 1) * share_c
    pack = flat_pack([norm_gain, gate_gain, conv_weight, conv_bias], small_rows(size))
    win_all, wout_all, pack_all = gather(
        [w_in.reshape(PIECES, -1, proj_width), w_out.reshape(PIECES, -1, width), pack], devices)
    w_in_full = win_all.reshape(width, proj_width)
    w_out_full = wout_all.reshape(inner, width)
    pack_all = pack_all.reshape(devices, -1)
    cuts = [share_n, share_n + share_g, share_n + share_g + taps * share_c, size]
    gain_full = pack_all[:, : cuts[0]].reshape(width)
    gate_full = pack_all[:, cuts[0] : cuts[1]].reshape(inner)
    kernel_full = pack_all[:, cuts[1] : cuts[2]].reshape(devices, taps, share_c).transpose(1, 0, 2).reshape(taps, conv_width)
    shift_full = pack_all[:, cuts[2] : cuts[3]].reshape(conv_width)

    flat_tokens = tokens.reshape(rows, width)
    residual = flat_tokens.astype(f32)
    rstd = lax.rsqrt(jnp.mean(residual * residual, axis=-1, keepdims=True) + epsilon)
    gain_f = gain_full.astype(f32)
    normed = (residual * rstd * gain_f).astype(bf16)
    grad_rows = cotangent.reshape(rows, width)
    grad_rows2 = partner(grad_rows)
    normed_t = normed.T.reshape(chips, 2, -1, rows)
    normed_t2 = partner(normed_t)
    projected = dot(normed, w_in_full)
    gm = dot(grad_rows, w_out_full, NT)
    tables = mixer_tables(segments, kernel_full, shift_full, dt_bias, a_log, d_skip, gate_full)
    mixed, mixed_t, gz, gy, rs, gg = mixer_forward(projected, gm, *tables, heads, state)
    mixed_t = mixed_t.reshape(chips, 2, -1, rows)
    gz2, mixed_t2 = partner(gz), partner(mixed_t)
    quarters = lambda part: part.reshape(chips, QUARTERS, -1, part.shape[1])
    part_out = quarters(grad_parts(core, mixed_t, mixed_t2, grad_rows, grad_rows2, "grad_out"))
    part_z = quarters(grad_parts(core, normed_t, normed_t2, gz, gz2, "grad_z"))
    px, pr, px2, pr2, sg, block_out, gacc, half_out, half_z = middle(
        projected, gy, rs, *tables, gg, mixed, w_out_full, flat_tokens, gz, w_in_full, [part_out, part_z], heads, state, devices)
    part_x = quarters(grad_parts(core, normed_t, normed_t2, px, px2, "grad_x"))
    part_r = quarters(grad_parts(core, normed_t, normed_t2, pr, pr2, "grad_r"))
    gain8 = jnp.broadcast_to(gain_f[None], (8, width))
    grad_tokens, small, own_out, own_z, own_x, own_r = tail(
        px, pr, w_in_full, gacc, flat_tokens, grad_rows, gain8, sg, [part_x, part_r], [half_out, half_z], 2 * state + heads, devices)

    grad_w_in = jnp.concatenate([o.reshape(-1, o.shape[2]) for o in (own_z, own_x, own_r)], axis=1)[:, :proj_width]
    conv = lax.dynamic_slice(small, (0, me * share_c), (taps + 1, share_c))
    gate = lax.dynamic_slice(small, (6, me * share_g), (1, share_g))
    norm = lax.dynamic_slice(small, (7, me * share_n), (1, share_n))
    skip = small[taps + 1, :inner].reshape(heads, inner // heads).sum(1)
    return (
        block_out.reshape(seqs, length, width),
        grad_tokens.reshape(seqs, length, width),
        norm[0],
        grad_w_in,
        conv[:taps],
        conv[taps],
        small[0, conv_width : conv_width + heads],
        small[1, conv_width : conv_width + heads],
        skip,
        gate[0],
        own_out.reshape(-1, width),
    )


def solution(mesh):
    rows3, rows2 = P(("fsdp", "dp"), None, None), P(("fsdp", "dp"), None)
    return jax.shard_map(
        functools.partial(local, mesh.shape["fsdp"]),
        mesh=mesh,
        in_specs=(rows3, rows2, P("fsdp"), P("fsdp", None), P(None, "fsdp"), P("fsdp"), P(), P(), P(), P("fsdp"), P("fsdp", None), rows3),
        out_specs=(rows3, rows3, P("fsdp"), P("fsdp", None), P(None, "fsdp"), P("fsdp"), P(), P(), P(), P("fsdp"), P("fsdp", None)),
        check_vma=False,
    )
```

```python
import functools

import jax
import jax.numpy as jnp
from jax import lax
from jax.experimental import pallas as pl
from jax.experimental.pallas import tpu as pltpu
from jax.sharding import PartitionSpec as P

f32, bf16 = jnp.float32, jnp.bfloat16
highest = lax.Precision.HIGHEST
epsilon = 1e-05
LANES = 128
BLOCK = 128
GROUP = 512
PAIRS = GROUP // LANES
NT = (((1,), (1,)), ((), ()))
NN = (((1,), (0,)), ((), ()))


def dot(a, b, dims=NN, precision=None):
    return lax.dot_general(a, b, dims, precision=precision, preferred_element_type=f32)


def sigmoid(v):
    return 0.5 + 0.5 * jnp.tanh(0.5 * v)


def conv_taps(xin, masks):
    taps = []
    for shift in (3, 2, 1):
        taps.append(pltpu.roll(xin, shift, 0) * masks[3 - shift])
    taps.append(xin)
    return taps


def conv_sum(taps, cw):
    total = cw[4:5, :] + cw[3:4, :] * taps[3]
    for k in range(3):
        total = total + cw[k : k + 1, :] * taps[k]
    return total


def conv_back(gsum, xin, cw, masks, length):
    grads = []
    gx = cw[3:4, :] * gsum
    for shift in (3, 2, 1):
        masked = gsum * masks[3 - shift]
        grads.append(jnp.sum(masked * pltpu.roll(xin, shift, 0), axis=0, keepdims=True))
        gx = gx + cw[3 - shift : 4 - shift, :] * pltpu.roll(masked, length - shift, 0)
    grads.append(jnp.sum(gsum * xin, axis=0, keepdims=True))
    grads.append(jnp.sum(gsum, axis=0, keepdims=True))
    return gx, grads


def prologue(heads, bc_ref, dtr_ref, segr_ref, cwbc_ref, hp_ref, mask_s, b_s, c_s, dt_s, cum_s, cumt_s, ef_s, la_s, sp_s):
    length = bc_ref.shape[0]
    segc = segr_ref[0].T
    here = lax.broadcasted_iota(jnp.int32, segc.shape, 0)
    for shift in (1, 2, 3):
        alike = (pltpu.roll(segc, shift, 0) == segc) & (here >= shift)
        mask_s[3 - shift] = jnp.broadcast_to(jnp.where(alike, 1.0, 0.0)[:, 0:1], (length, LANES))
    masks = [mask_s[k] for k in range(3)]
    for half, ref in ((0, b_s), (1, c_s)):
        sl = slice(half * LANES, (half + 1) * LANES)
        taps = conv_taps(bc_ref[:, sl], masks)
        summed = conv_sum(taps, cwbc_ref[:, sl])
        ref[...] = summed * sigmoid(summed)
    lane = lax.broadcasted_iota(jnp.int32, (length, LANES), 1)
    raw = jnp.where(lane < heads, dtr_ref[...] + hp_ref[0:1, :], 0.0)
    soft = jnp.maximum(raw, 0.0) + jnp.log1p(jnp.exp(-jnp.abs(raw)))
    dt = jnp.where(lane < heads, soft, 0.0)
    la = -dt * jnp.exp(hp_ref[1:2, :])
    row = lax.broadcasted_iota(jnp.int32, (length, length), 0)
    col = lax.broadcasted_iota(jnp.int32, (length, length), 1)
    tri = jnp.where(row >= col, 1.0, 0.0).astype(f32)
    cum = dot(tri, la, precision=highest)
    dt_s[...] = dt
    la_s[...] = la
    cum_s[...] = cum
    cumt_s[...] = cum.T
    sp_s[...] = sigmoid(raw)
    mid = cum[BLOCK - 1 : BLOCK, :]
    ef_s[:BLOCK] = jnp.exp(jnp.minimum(mid - cum[:BLOCK], 0.0))
    ef_s[BLOCK:] = jnp.exp(jnp.minimum(cum[BLOCK:] - mid, 0.0))
    same = (segc[:, 0:1] == segr_ref[0, 0:1, :]).astype(f32)
    return row, col, same


def headpick(first, shape):
    source = lax.broadcasted_iota(jnp.int32, shape, 0) // 64
    target = lax.broadcasted_iota(jnp.int32, shape, 1)
    source = source - 2 * (source // 2)
    return jnp.where(target == source + first, 1.0, 0.0).astype(bf16)


def headsum(value, pick):
    hi = value.astype(bf16)
    lo = (value - hi.astype(f32)).astype(bf16)
    return dot(jnp.concatenate([hi, lo], axis=1), pick)


def fwd_kernel(heads, z_ref, x_ref, bc_ref, dtr_ref, gm_ref, segr_ref, cwx_ref, cwbc_ref, hp_ref, cp_ref,
               mixed_ref, mixt_ref, gz_ref, gy_ref, rs_ref, gg_ref,
               mask_s, b_s, c_s, dt_s, cum_s, cumt_s, ef_s, la_s, sp_s, sm_s, ssm_s, yd_s, u_s, st_s, rs_s):
    phase, group = pl.program_id(1), pl.program_id(2)
    length = z_ref.shape[0]
    lane = lax.broadcasted_iota(jnp.int32, (length, LANES), 1)
    first = lane < 64
    half = lax.broadcasted_iota(jnp.int32, (BLOCK, LANES), 1) < 64

    @pl.when((phase == 0) & (group == 0))
    def _():
        row, col, same = prologue(heads, bc_ref, dtr_ref, segr_ref, cwbc_ref, hp_ref, mask_s, b_s, c_s, dt_s, cum_s, cumt_s, ef_s, la_s, sp_s)
        scores = dot(c_s[...], b_s[...], NT, precision=highest)
        sm_s[...] = jnp.where(row >= col, scores * same, 0.0)
        st_s[...] = jnp.zeros_like(st_s)

    width = jnp.int32(8)
    shift = lax.rem(jnp.int32(LANES) - width * group, jnp.int32(LANES))

    @pl.when(phase == 0)
    def _():
        masks = [mask_s[k] for k in range(3)]
        dtg = pltpu.roll(dt_s[...], shift, 1)
        cumg = pltpu.roll(cum_s[...], shift, 1)
        efg = pltpu.roll(ef_s[...], shift, 1)
        cumt = cumt_s[pl.ds(pl.multiple_of(group * 8, 8), 8), :]
        square, across = st_s[0], st_s[1]
        for j in range(PAIRS):
            sl = slice(j * LANES, (j + 1) * LANES)
            place = pl.ds(pl.multiple_of(group * GROUP + j * LANES, LANES), LANES)
            xin = x_ref[:, sl]
            summed = conv_sum(conv_taps(xin, masks), cwx_ref[:, sl])
            xs = summed * sigmoid(summed)
            dtb = jnp.where(first, dtg[:, 2 * j : 2 * j + 1], dtg[:, 2 * j + 1 : 2 * j + 2])
            efb = jnp.where(first, efg[:, 2 * j : 2 * j + 1], efg[:, 2 * j + 1 : 2 * j + 2])
            xd = xs * dtb
            for i in range(2):
                rows = slice(i * BLOCK, (i + 1) * BLOCK)
                part = xd[rows]
                stack = jnp.concatenate([jnp.where(half, part, 0.0), jnp.where(half, 0.0, part)], axis=0).astype(bf16)
                decays = []
                for h in range(2):
                    arg = cumg[rows, 2 * j + h : 2 * j + h + 1] - cumt[2 * j + h : 2 * j + h + 1, rows]
                    decays.append((jnp.exp(jnp.minimum(arg, 0.0)) * sm_s[rows, rows]).astype(bf16))
                yd_s[rows, place] = dot(jnp.concatenate(decays, axis=1), stack)
            far = (xd[:BLOCK] * efb[:BLOCK]).astype(bf16)
            u = dot(sm_s[BLOCK:, :BLOCK].astype(bf16), far)
            u_s[:, place] = u
            base = yd_s[:, place] + cp_ref[0:1, sl] * xs
            ssm = jnp.concatenate([base[:BLOCK], base[BLOCK:] + efb[BLOCK:] * u], axis=0)
            ssm_s[:, place] = ssm
            zin = z_ref[:, sl]
            gated = ssm * (zin * sigmoid(zin))
            square = square + gated * gated
            across = across + gm_ref[:, sl] * cp_ref[1:2, sl] * gated
        st_s[0] = square
        st_s[1] = across

    @pl.when((phase == 1) & (group == 0))
    def _():
        inner = heads * 64
        mean = jnp.sum(st_s[0], axis=1, keepdims=True) / inner
        scale = lax.rsqrt(mean + epsilon)
        inward = jnp.sum(st_s[1], axis=1, keepdims=True) / inner
        st_s[0] = jnp.broadcast_to(scale, (length, LANES))
        st_s[1] = jnp.broadcast_to(scale * scale * scale * inward, (length, LANES))
        rs_s[...] = jnp.zeros_like(rs_s)

    @pl.when(phase == 1)
    def _():
        scale, lean = st_s[0], st_s[1]
        efg = pltpu.roll(ef_s[...], shift, 1)
        total = rs_s[...]
        for j in range(PAIRS):
            sl = slice(j * LANES, (j + 1) * LANES)
            place = pl.ds(pl.multiple_of(group * GROUP + j * LANES, LANES), LANES)
            zin = z_ref[:, sl]
            sg = sigmoid(zin)
            silu = zin * sg
            dsilu = sg + silu * (1.0 - sg)
            ssm = ssm_s[:, place]
            gated = ssm * silu
            unit = gated * scale
            gain = cp_ref[1:2, sl]
            gm = gm_ref[:, sl]
            mixed = unit * gain
            mixed_ref[:, sl] = mixed.astype(bf16)
            mixt_ref[sl, :] = mixed.T.astype(bf16)
            gain_sum = jnp.sum(gm * unit, axis=0, keepdims=True)
            old = gg_ref[0:1, place]
            gg_ref[:, place] = jnp.broadcast_to(jnp.where(pl.program_id(0) == 0, gain_sum, old + gain_sum), (8, LANES))
            ggated = scale * (gm * gain) - gated * lean
            gz_ref[:, sl] = (ggated * ssm * dsilu).astype(bf16)
            gy = ggated * silu
            gy_ref[:, sl] = gy
            efb = jnp.where(first, efg[:, 2 * j : 2 * j + 1], efg[:, 2 * j + 1 : 2 * j + 2])
            near = gy.astype(bf16).astype(f32) * yd_s[:, place]
            fare = (gy[BLOCK:] * efb[BLOCK:]).astype(bf16).astype(f32) * u_s[:, place]
            value = jnp.concatenate([near[:BLOCK], near[BLOCK:] + fare], axis=0)
            total = total + headsum(value, headpick(8 * group + 2 * j, (2 * LANES, LANES)))
        rs_s[...] = total
        rs_ref[0] = total


def mixer_back(heads, groups, group, opening, x_ref, bc_ref, dtr_ref, gy_ref, rs_ref, segr_ref, cwx_ref, cwbc_ref, hp_ref, cp_ref,
               px_ref, pr_ref, sg_ref,
               mask_s, b_s, c_s, dt_s, cum_s, cumt_s, ef_s, la_s, sp_s, smt_s, gst_s, gc_s, gd_s):
    length = x_ref.shape[0]
    inner_width = groups * GROUP

    def keep(row, cols, value):
        sg_ref[row : row + 1, cols] = sg_ref[row : row + 1, cols] + value

    @pl.when(opening)
    def _():
        sg_ref[...] = jnp.zeros_like(sg_ref)

    lane = lax.broadcasted_iota(jnp.int32, (length, LANES), 1)
    first = lane < 64
    half = lax.broadcasted_iota(jnp.int32, (BLOCK, LANES), 1) < 64

    @pl.when(group == 0)
    def _():
        row, col, same = prologue(heads, bc_ref, dtr_ref, segr_ref, cwbc_ref, hp_ref, mask_s, b_s, c_s, dt_s, cum_s, cumt_s, ef_s, la_s, sp_s)
        scores = dot(b_s[...], c_s[...], NT, precision=highest)
        smt_s[...] = jnp.where(row <= col, scores * same, 0.0)
        gst_s[...] = jnp.zeros_like(gst_s)
        gc_s[...] = jnp.zeros_like(gc_s)
        gd_s[...] = jnp.zeros_like(gd_s)

    shift = lax.rem(jnp.int32(LANES) - jnp.int32(8) * group, jnp.int32(LANES))
    masks = [mask_s[k] for k in range(3)]
    dtg = pltpu.roll(dt_s[...], shift, 1)
    cumg = pltpu.roll(cum_s[...], shift, 1)
    efg = pltpu.roll(ef_s[...], shift, 1)
    cumt = cumt_s[pl.ds(pl.multiple_of(group * 8, 8), 8), :]
    gcum, gdir = gc_s[...], gd_s[...]
    for j in range(PAIRS):
        sl = slice(j * LANES, (j + 1) * LANES)
        xin = x_ref[:, sl]
        cw = cwx_ref[:, sl]
        summed = conv_sum(conv_taps(xin, masks), cw)
        sg = sigmoid(summed)
        xs = summed * sg
        dtb = jnp.where(first, dtg[:, 2 * j : 2 * j + 1], dtg[:, 2 * j + 1 : 2 * j + 2])
        efb = jnp.where(first, efg[:, 2 * j : 2 * j + 1], efg[:, 2 * j + 1 : 2 * j + 2])
        xd = xs * dtb
        gy = gy_ref[:, sl]
        gyb = gy.astype(bf16)
        inner = []
        for i in range(2):
            rows = slice(i * BLOCK, (i + 1) * BLOCK)
            part, gpart = xd[rows], gy[rows]
            stack = jnp.concatenate([jnp.where(half, part, 0.0), jnp.where(half, 0.0, part)], axis=0).astype(bf16)
            gstack = jnp.concatenate([jnp.where(half, gpart, 0.0), jnp.where(half, 0.0, gpart)], axis=0).astype(bf16)
            gw = dot(stack, gyb[rows], NT)
            weights = []
            gscore = gst_s[rows, rows]
            for h in range(2):
                arg = cumt[2 * j + h : 2 * j + h + 1, rows] - cumg[rows, 2 * j + h : 2 * j + h + 1]
                decay = jnp.exp(jnp.minimum(arg, 0.0))
                weights.append((decay * smt_s[rows, rows]).astype(bf16))
                gscore = gscore + gw[h * BLOCK : (h + 1) * BLOCK] * decay
            gst_s[rows, rows] = gscore
            inner.append(dot(jnp.concatenate(weights, axis=1), gstack))
        far = (xd[:BLOCK] * efb[:BLOCK]).astype(bf16)
        ge = (gy[BLOCK:] * efb[BLOCK:]).astype(bf16)
        gst_s[:BLOCK, BLOCK:] += dot(far, ge, NT)
        gfar = dot(smt_s[:BLOCK, BLOCK:].astype(bf16), ge)
        xdb = xd.astype(bf16).astype(f32)
        fall0 = xdb[:BLOCK] * inner[0] + far.astype(f32) * gfar
        fall = jnp.concatenate([fall0, xdb[BLOCK:] * inner[1]], axis=0)
        gxd = jnp.concatenate([inner[0] + efb[:BLOCK] * gfar, inner[1]], axis=0)
        sums = headsum(jnp.concatenate([fall, xs * gxd], axis=0), headpick(8 * group + 2 * j, (2 * LANES, LANES)))
        gcum = gcum - sums[:length]
        gdir = gdir + sums[length:]
        gxs = cp_ref[0:1, sl] * gy + dtb * gxd
        gsum = gxs * (sg + xs * (1.0 - sg))
        gx, grads = conv_back(gsum, xin, cw, masks, length)
        px_ref[:, sl] = gx.astype(bf16)
        grads.append(jnp.sum(gy * xs, axis=0, keepdims=True))
        place = pl.ds(pl.multiple_of(group * GROUP + j * LANES, LANES), LANES)
        for k, value in enumerate(grads):
            keep(k, place, value)
    gc_s[...] = gcum
    gd_s[...] = gdir

    @pl.when(group == groups - 1)
    def _():
        row = lax.broadcasted_iota(jnp.int32, (length, length), 0)
        col = lax.broadcasted_iota(jnp.int32, (length, length), 1)
        same = segr_ref[0].T[:, 0:1] == segr_ref[0, 0:1, :]
        gscore = jnp.where((row <= col) & same, gst_s[...], 0.0)
        backs = (dot(gscore, c_s[...], precision=highest), dot(gscore.T, b_s[...], precision=highest))
        for part in range(2):
            sl = slice(part * LANES, (part + 1) * LANES)
            xin = bc_ref[:, sl]
            cw = cwbc_ref[:, sl]
            summed = conv_sum(conv_taps(xin, masks), cw)
            sg = sigmoid(summed)
            gsum = backs[part] * (sg + summed * sg * (1.0 - sg))
            gx, grads = conv_back(gsum, xin, cw, masks, length)
            pr_ref[:, sl] = gx.astype(bf16)
            for k, value in enumerate(grads):
                keep(k, slice(inner_width + part * LANES, inner_width + (part + 1) * LANES), value)
        upper = jnp.where(row <= col, 1.0, 0.0).astype(f32)
        gla = dot(upper, gc_s[...] + rs_ref[0], precision=highest)
        graw = (gd_s[...] - gla * jnp.exp(hp_ref[1:2, :])) * sp_s[...]
        graw = jnp.where(lane < heads, graw, 0.0)
        pr_ref[:, 2 * LANES :] = graw.astype(bf16)
        tail = slice(inner_width + 2 * LANES, inner_width + 3 * LANES)
        keep(0, tail, jnp.sum(graw, axis=0, keepdims=True))
        keep(1, tail, jnp.sum(jnp.where(lane < heads, gla * la_s[...], 0.0), axis=0, keepdims=True))


def small_scratch(length):
    return [
        pltpu.VMEM((3, length, LANES), f32),
        pltpu.VMEM((length, LANES), f32),
        pltpu.VMEM((length, LANES), f32),
        pltpu.VMEM((length, LANES), f32),
        pltpu.VMEM((length, LANES), f32),
        pltpu.VMEM((LANES, length), f32),
        pltpu.VMEM((length, LANES), f32),
        pltpu.VMEM((length, LANES), f32),
        pltpu.VMEM((length, LANES), f32),
    ]


def mixer_forward(projected, gm, segr, cw, hp, cp, heads, state):
    seqs, _, length = segr.shape
    inner = gm.shape[1]
    groups = inner // GROUP
    rows = seqs * length
    kernel = functools.partial(fwd_kernel, heads)
    out_row = lambda b, p, g: (b, g * p)
    return pl.pallas_call(
        kernel,
        grid=(seqs, 2, groups),
        in_specs=[
            pl.BlockSpec((length, GROUP), lambda b, p, g: (b, g)),
            pl.BlockSpec((length, GROUP), lambda b, p, g: (b, groups + g * (1 - p) + (groups - 1) * p)),
            pl.BlockSpec((length, 2 * state), lambda b, p, g: (b, 2 * inner // (2 * state))),
            pl.BlockSpec((length, LANES), lambda b, p, g: (b, (2 * inner + 2 * state) // LANES)),
            pl.BlockSpec((length, GROUP), lambda b, p, g: (b, g)),
            pl.BlockSpec((1, 8, length), lambda b, p, g: (b, 0, 0)),
            pl.BlockSpec((8, GROUP), lambda b, p, g: (0, g)),
            pl.BlockSpec((8, 2 * state), lambda b, p, g: (0, inner // (2 * state))),
            pl.BlockSpec((8, LANES), lambda b, p, g: (0, 0)),
            pl.BlockSpec((8, GROUP), lambda b, p, g: (0, g)),
        ],
        out_specs=[
            pl.BlockSpec((length, GROUP), out_row),
            pl.BlockSpec((GROUP, length), lambda b, p, g: (g * p, b)),
            pl.BlockSpec((length, GROUP), out_row),
            pl.BlockSpec((length, GROUP), out_row),
            pl.BlockSpec((1, length, LANES), lambda b, p, g: (b, 0, 0)),
            pl.BlockSpec((8, inner), lambda b, p, g: (0, 0)),
        ],
        out_shape=[
            jax.ShapeDtypeStruct((rows, inner), bf16),
            jax.ShapeDtypeStruct((inner, rows), bf16),
            jax.ShapeDtypeStruct((rows, inner), bf16),
            jax.ShapeDtypeStruct((rows, inner), f32),
            jax.ShapeDtypeStruct((seqs, length, LANES), f32),
            jax.ShapeDtypeStruct((8, inner), f32),
        ],
        scratch_shapes=small_scratch(length) + [
            pltpu.VMEM((length, length), f32),
            pltpu.VMEM((length, inner), f32),
            pltpu.VMEM((length, inner), f32),
            pltpu.VMEM((length - BLOCK, inner), f32),
            pltpu.VMEM((2, length, LANES), f32),
            pltpu.VMEM((length, LANES), f32),
        ],
        compiler_params=pltpu.CompilerParams(vmem_limit_bytes=48 << 20),
        cost_estimate=pl.CostEstimate(flops=10**10, bytes_accessed=45 * 10**6, transcendentals=10**7),
        name="mixer_forward",
    )(projected, projected, projected, projected, gm, segr, cw, cw, hp, cp)


def pad_lanes(v, width=LANES):
    return jnp.pad(v, ((0, 0), (0, width - v.shape[1])))


def mixer_tables(segments, kernel_full, shift_full, dt_bias, a_log, d_skip, gate_full):
    taps = kernel_full.shape[0]
    seqs, length = segments.shape
    segr = jnp.broadcast_to(segments.astype(f32)[:, None, :], (seqs, 8, length))
    cw = jnp.concatenate([kernel_full.astype(f32), jnp.broadcast_to(shift_full.astype(f32)[None], (8 - taps, shift_full.shape[0]))])
    hp = pad_lanes(jnp.concatenate([dt_bias[None], jnp.broadcast_to(a_log[None], (7, a_log.shape[0]))]))
    heads = dt_bias.shape[0]
    size = gate_full.shape[0] // heads
    cp = jnp.concatenate([jnp.repeat(d_skip, size)[None], jnp.broadcast_to(gate_full.astype(f32)[None], (7, gate_full.shape[0]))])
    return segr, cw, hp, cp


MESH = pl.DeviceIdType.MESH
PIECES = 3


def ring_place(chip, chips):
    wide = chips // 4
    z, q = chip // wide, chip % wide
    up = 1 + 3 * q + jnp.where(q % 2 == 0, z - 1, 3 - z)
    back = jnp.where(q == 0, 0, 4 * wide - q)
    return jnp.where(z == 0, back, up)


def ring_chip(place, chips):
    wide = chips // 4
    place = place % chips
    q = (place - 1 + chips) % chips // 3
    r = (place - 1 + chips) % chips % 3
    z = jnp.where(q % 2 == 0, 1 + r, 3 - r)
    inner = z * wide + q
    outer = (4 * wide - place) % (4 * wide)
    return jnp.where((place == 0) | (place > 3 * wide), outer, inner)


def gather_kernel(chips, count, *refs):
    ins, outs = refs[:count], refs[count : 2 * count]
    ring_send, ring_recv, far_send, far_recv, pair_send, pair_recv, own_sem = refs[2 * count :]
    me = lax.axis_index("fsdp")
    plane = lax.axis_index("dp")
    chip, core = me // 2, me % 2
    place = ring_place(chip, chips)
    right = 2 * ring_chip(place + 1, chips) + core
    left = 2 * ring_chip(place + chips - 1, chips) + core
    pair = {"fsdp": me + 1 - 2 * core}
    peer = {"dp": 1 - plane}
    ways = ({"fsdp": right}, {"fsdp": left})

    barrier = pltpu.get_barrier_semaphore()
    for other in (ways[0], ways[1], pair, peer):
        pl.semaphore_signal(barrier, inc=1, device_id=other, device_id_type=MESH)
    pl.semaphore_wait(barrier, 4)

    half = chips // 2
    whole = [k == count - 1 for k in range(count)]

    def steps(way, slot):
        return half if way == slot else half - 1

    def owner(way, step):
        move = -step if way == 0 else step
        return 2 * ring_chip(place + move + chips, chips) + core

    def part(refs, k, index, slot):
        if whole[k]:
            return refs[k].at[index]
        piece = 0 if slot == 0 else 1 + plane
        return refs[k].at[index, piece]

    def mine(k, slot):
        if whole[k]:
            return ins[k]
        piece = 0 if slot == 0 else 1 + plane
        return ins[k].at[piece]

    def slots(k):
        return (0,) if whole[k] else (0, 1)

    pending = []

    def send(source, target, send_sem, recv_sem, device):
        copy = pltpu.make_async_remote_copy(
            src_ref=source, dst_ref=target, send_sem=send_sem, recv_sem=recv_sem, device_id=device, device_id_type=MESH)
        copy.start()
        pending.append(copy)

    def arrived(target, send_sem, recv_sem):
        pltpu.make_async_remote_copy(
            src_ref=target, dst_ref=target, send_sem=send_sem, recv_sem=recv_sem, device_id=pair, device_id_type=MESH).wait_recv()

    def ring_sem(sem, way, step, k, slot):
        return sem.at[(way * half + step - 1) * 2 * count + 2 * k + slot]

    def far_sem(sem, way, step, k):
        return sem.at[(way * half + step - 1) * count + k]

    def pair_sem(sem, turn, k, slot):
        return sem.at[(turn * count + k) * 3 + slot]

    def turn(way, step):
        return 1 + (step - 1) * 2 + way

    local = []
    for k in range(count):
        for slot in slots(k):
            for way in range(2):
                send(mine(k, slot), part(outs, k, me, slot), ring_sem(ring_send, way, 1, k, slot), ring_sem(ring_recv, way, 1, k, slot), ways[way])
        send(ins[k], outs[k].at[me], pair_sem(pair_send, 0, k, 0), pair_sem(pair_recv, 0, k, 0), pair)
        copy = pltpu.make_async_copy(ins[k], outs[k].at[me], own_sem.at[k])
        copy.start()
        local.append(copy)

    def from_peer(way, step):
        index = owner(way, step)
        for k in range(count):
            if whole[k] or step > steps(way, 1):
                continue
            target = outs[k].at[index, 2 - plane]
            arrived(target, far_sem(far_send, way, step, k), far_sem(far_recv, way, step, k))
            send(target, target, pair_sem(pair_send, turn(way, step), k, 2), pair_sem(pair_recv, turn(way, step), k, 2), pair)

    for step in range(1, half + 1):
        for way in range(2):
            index = owner(way, step)
            for k in range(count):
                for slot in slots(k):
                    if step > steps(way, slot):
                        continue
                    target = part(outs, k, index, slot)
                    arrived(target, ring_sem(ring_send, way, step, k, slot), ring_sem(ring_recv, way, step, k, slot))
                    if step + 1 <= steps(way, slot):
                        send(target, target, ring_sem(ring_send, way, step + 1, k, slot), ring_sem(ring_recv, way, step + 1, k, slot), ways[way])
                    if slot == 1:
                        send(target, target, far_sem(far_send, way, step, k), far_sem(far_recv, way, step, k), peer)
                    send(target, target, pair_sem(pair_send, turn(way, step), k, slot), pair_sem(pair_recv, turn(way, step), k, slot), pair)
        if step > 1:
            for way in range(2):
                from_peer(way, step - 1)
    for way in range(2):
        from_peer(way, half)
    for k in range(count):
        other = outs[k].at[me + 1 - 2 * core]
        arrived(other, pair_sem(pair_send, 0, k, 0), pair_sem(pair_recv, 0, k, 0))
    for step in range(1, half + 1):
        for way in range(2):
            index = owner(way, step) + 1 - 2 * core
            for k in range(count):
                for slot in slots(k) + (() if whole[k] else (2,)):
                    if step > steps(way, min(slot, 1)):
                        continue
                    if slot == 2:
                        target = outs[k].at[index, 2 - plane]
                    else:
                        target = part(outs, k, index, slot)
                    sems = turn(way, step), k, slot
                    arrived(target, pair_sem(pair_send, *sems), pair_sem(pair_recv, *sems))
    for copy in local:
        copy.wait()
    for copy in pending:
        copy.wait_send()


def gather(arrays, devices):
    count = len(arrays)
    chips = devices // 2
    half = chips // 2
    dma = pltpu.SemaphoreType.DMA
    return pl.pallas_call(
        functools.partial(gather_kernel, chips, count),
        in_specs=[pl.BlockSpec(memory_space=pl.ANY)] * count,
        out_specs=[pl.BlockSpec(memory_space=pl.ANY)] * count,
        out_shape=[jax.ShapeDtypeStruct((devices,) + a.shape, a.dtype) for a in arrays],
        scratch_shapes=[
            dma((4 * half * count,)), dma((4 * half * count,)),
            dma((2 * half * count,)), dma((2 * half * count,)),
            dma(((2 * half + 1) * count * 3,)), dma(((2 * half + 1) * count * 3,)),
            dma((count,)),
        ],
        compiler_params=pltpu.CompilerParams(collective_id=0, has_side_effects=True),
        name="gather_weights",
    )(*arrays)


QUARTERS = 4
TILE = 512
FULL = 62 << 20


def add_up(sources, store, width):
    tile = min(TILE, width)

    def total(cols):
        value = sources[0][:, cols].astype(f32)
        for source in sources[1:]:
            value = value + source[:, cols].astype(f32)
        store[:, cols] = value.astype(store.dtype)

    def one(i, carry):
        total(pl.ds(pl.multiple_of(i * tile, LANES), tile))
        return carry

    lax.fori_loop(0, width // tile, one, 0)
    if width % tile:
        total(slice(width - width % tile, width))


class Links:
    def __init__(self, chips):
        self.chips, self.half = chips, chips // 2
        me = lax.axis_index("fsdp")
        self.plane = lax.axis_index("dp")
        self.chip, self.core = me // 2, me % 2
        self.place = ring_place(self.chip, chips)
        self.ways = tuple(
            {"fsdp": 2 * ring_chip(self.place + move, chips) + self.core} for move in (1, chips - 1))
        self.peer = {"dp": 1 - self.plane}
        self.pair = {"fsdp": me + 1 - 2 * self.core}
        self.turns = [{"fsdp": me + bit - 2 * bit * ((me // bit) % 2)} for bit in (1 << k for k in range(chips.bit_length()))] + [self.peer]
        self.sent = []

    def greet(self, others):
        barrier = pltpu.get_barrier_semaphore()
        for other in others:
            pl.semaphore_signal(barrier, inc=1, device_id=other, device_id_type=MESH)
        pl.semaphore_wait(barrier, len(others))

    def send(self, source, target, send_sem, recv_sem, device):
        make = lambda: pltpu.make_async_remote_copy(
            src_ref=source(), dst_ref=target(), send_sem=send_sem(), recv_sem=recv_sem(), device_id=device, device_id_type=MESH)
        make().start()
        self.sent.append(make)

    def arrived(self, target, send_sem, recv_sem):
        pltpu.make_async_remote_copy(
            src_ref=target, dst_ref=target, send_sem=send_sem, recv_sem=recv_sem, device_id=self.peer, device_id_type=MESH).wait_recv()

    def finish(self):
        for make in self.sent:
            make().wait_send()


class Ring:
    def __init__(self, links, items, shift, parts, held, ring_in, peer_in, held_sem, ring_send, ring_recv, peer_send, peer_recv):
        self.links, self.items, self.shift, self.parts = links, items, shift, parts
        self.held, self.ring_in, self.peer_in = held, ring_in, peer_in
        self.held_sem, self.ring_send, self.ring_recv = held_sem, ring_send, ring_recv
        self.peer_send, self.peer_recv = peer_send, peer_recv

    def hops(self, k, way, slot):
        return self.links.half - (slot + (k + self.shift if slot == 2 else 0) + way) % 2

    def target(self, k, way, slot, step):
        chips = self.links.chips
        ahead = self.hops(k, way, slot) - step + 1
        return ring_chip(self.links.place + (ahead if way == 0 else chips - ahead), chips)

    def quarter(self, slot):
        return slot if slot < 2 else 2 + self.links.plane

    def at(self, way, step, slot):
        return (way * self.links.half + step - 1) * 3 + slot

    def sems(self, k, way, step, slot):
        at = k * 6 * self.links.half + self.at(way, step, slot)
        return self.ring_send.at[at], self.ring_recv.at[at]

    def push(self, k, way, step, slot, source):
        at = self.at(way, step, slot)
        self.links.send(
            source, lambda: self.ring_in[k].at[at],
            lambda: self.sems(k, way, step, slot)[0], lambda: self.sems(k, way, step, slot)[1], self.links.ways[way])

    def start(self):
        links, count = self.links, len(self.items)
        for slot in (0, 1):
            for k in range(count):
                for way in range(2):
                    self.push(k, way, 1, slot, lambda k=k, way=way, slot=slot: self.parts[k].at[self.target(k, way, slot, 1), slot])
        for move in self.order():
            for k in range(count):
                def where(move=move):
                    return (links.place + move) % links.chips
                links.send(
                    lambda k=k, where=where: self.parts[k].at[ring_chip(where(), links.chips), 3 - links.plane],
                    lambda k=k, where=where: self.peer_in[k].at[where()],
                    lambda k=k, where=where: self.peer_send.at[k * links.chips + where()],
                    lambda k=k, where=where: self.peer_recv.at[k * links.chips + where()], links.peer)
        for copy in self.loads():
            copy.start()

    def sequence(self):
        half = self.links.half
        main = [("hop", step, slot) for step in range(2, half + 1) for slot in (0, 1)]
        other = [("hop", step, 2) for step in range(1, half + 1)]
        out = []
        for n, entry in enumerate(main):
            out.append(entry)
            if n >= 3 and n % 2 and len(other) > 2:
                out.append(other.pop(0))
        return out + [("land", 0, 0), ("land", 0, 1)] + other + [("land", 0, 2)]

    def order(self):
        chips, half = self.links.chips, self.links.half
        moves = []
        for ahead in range(half, -1, -1):
            moves.append(ahead)
            if 0 < ahead < half:
                moves.append(chips - ahead)
        return moves

    def loads(self):
        return [
            pltpu.make_async_copy(self.parts[k].at[:, self.quarter(slot)], self.held[k].at[slot], self.held_sem.at[k * 3 + slot])
            for k in range(len(self.items)) for slot in range(3)]

    def from_peer(self, k, chunk):
        where = ring_place(chunk, self.links.chips)
        at = k * self.links.chips + where
        self.links.arrived(self.peer_in[k].at[where], self.peer_send.at[at], self.peer_recv.at[at])
        return self.peer_in[k].at[where]

    def hop(self, step, slot):
        for k in range(len(self.items)):
            for way in range(2):
                if step > self.hops(k, way, slot) or (step == 1 and slot < 2):
                    continue
                chunk = self.target(k, way, slot, step)
                sources = [self.held[k].at[slot, chunk]]
                if slot == 2:
                    sources.append(self.from_peer(k, chunk))
                if step > 1:
                    before = self.at(way, step - 1, slot)
                    self.links.arrived(self.ring_in[k].at[before], *self.sems(k, way, step - 1, slot))
                    sources.append(self.ring_in[k].at[before])
                    store = lambda k=k, before=before: self.ring_in[k].at[before]
                else:
                    store = lambda k=k, way=way, slot=slot, step=step: self.peer_in[k].at[
                        ring_place(self.target(k, way, slot, step), self.links.chips)]
                add_up(sources, store(), self.items[k][1])
                self.push(k, way, step, slot, store)

    def land(self, k, slot, store):
        links = self.links
        sources = [self.held[k].at[slot, links.chip]]
        for way in range(2):
            last = self.hops(k, way, slot)
            at = self.at(way, last, slot)
            links.arrived(self.ring_in[k].at[at], *self.sems(k, way, last, slot))
            sources.append(self.ring_in[k].at[at])
        if slot == 2:
            sources.append(self.from_peer(k, links.chip))
        add_up(sources, store, self.items[k][1])


def ring_scratch(items, chips):
    dma = pltpu.SemaphoreType.DMA
    half, count = chips // 2, len(items)
    vm = lambda *lead: [pltpu.VMEM(lead + item, bf16) for item in items]
    return vm(3, chips) + vm(6 * half) + vm(chips) + [
        dma((3 * count,)), dma((6 * half * count,)), dma((6 * half * count,)), dma((chips * count,)), dma((chips * count,))]


def split_scratch(refs, count):
    return [refs[i * count : (i + 1) * count] for i in range(3)], refs[3 * count : 3 * count + 5]


def middle_kernel(heads, chips, seqs, groups, items, x_ref, bc_ref, dtr_ref, gy_ref, rs_ref, segr_ref, cwx_ref, cwbc_ref, hp_ref, cp_ref,
                  gg_ref, mixed_ref, wout_ref, tok_ref, gz_ref, win_ref, nt_ref, nt2_ref, *refs):
    count = len(items)
    parts, refs = refs[:count], refs[count:]
    px_ref, pr_ref, partx_ref, partr_ref, sg_ref, bo_ref, gn_ref = refs[:7]
    owns, nears, refs = refs[7 : 7 + count], refs[7 + count : 7 + 2 * count], refs[7 + 2 * count :]
    back, (nts, nts2, pxs, prs, px2s, pr2s, nt_sem, px_send, px_recv, pr_send, pr_recv, near_send, near_recv), refs = refs[:13], refs[13:26], refs[26:]
    (held, ring_in, peer_in), sems = split_scratch(refs, count)
    step = pl.program_id(0)
    turns = seqs * groups
    last = turns + 3 * groups
    length = x_ref.shape[0]
    links = Links(chips)
    ring = Ring(links, items, 0, parts, held, ring_in, peer_in, *sems)
    turned = lambda: [
        pltpu.make_async_copy(source.at[:, links.core], target, nt_sem.at[n])
        for n, (source, target) in enumerate(((nt_ref, nts), (nt2_ref, nts2)))]

    @pl.when(step == 0)
    def _():
        links.greet([links.ways[0], links.ways[1], links.peer, links.pair])
        ring.start()
        for copy in turned():
            copy.start()

    plan = {}
    sequence = ring.sequence()
    for n, entry in enumerate(sequence):
        plan.setdefault(max(2, (n + 1) * last // len(sequence)), []).append(entry)

    def px_copy(turn):
        return pltpu.make_async_remote_copy(
            src_ref=pxs.at[turn], dst_ref=px2s.at[turn], send_sem=px_send.at[turn], recv_sem=px_recv.at[turn],
            device_id=links.pair, device_id_type=MESH)

    def pr_copy(seq):
        return pltpu.make_async_remote_copy(
            src_ref=prs.at[seq], dst_ref=pr2s.at[seq], send_sem=pr_send.at[seq], recv_sem=pr_recv.at[seq],
            device_id=links.pair, device_id_type=MESH)

    @pl.when(step < turns)
    def _():
        group = step % groups
        mixer_back(heads, groups, group, step == 0, x_ref, bc_ref, dtr_ref, gy_ref, rs_ref, segr_ref, cwx_ref, cwbc_ref, hp_ref, cp_ref,
                   px_ref, pr_ref, sg_ref, *back)
        pxs[step] = px_ref[...]
        px_copy(step).start()

        @pl.when(group == groups - 1)
        def _():
            seq = step // groups
            prs[seq] = pr_ref[...]
            pr_copy(seq).start()

    @pl.when((step >= turns) & (step < turns + groups))
    def _():
        part = dot(mixed_ref[...], wout_ref[...])

        @pl.when(step == turns)
        def _():
            gn_ref[...] = tok_ref[...].astype(f32) + part

        @pl.when((step > turns) & (step < turns + groups - 1))
        def _():
            gn_ref[...] += part

        @pl.when(step == turns + groups - 1)
        def _():
            bo_ref[...] = (gn_ref[...] + part).astype(bf16)

    @pl.when((step >= turns + groups) & (step < turns + 2 * groups))
    def _():
        part = dot(gz_ref[...], win_ref[...], NT)

        @pl.when(step == turns + groups)
        def _():
            gn_ref[...] = part

        @pl.when(step > turns + groups)
        def _():
            gn_ref[...] += part

    def own_rows(mine, theirs, store):
        many, each, tokens = nts.shape
        pieces = [(n * length, left, right) for left, rights in ((nts, mine), (nts2, theirs)) for n, right in enumerate(rights)]
        if each % 16 == 0:
            total = None
            for at, left, right in pieces:
                part = dot(left[:, :, at : at + length].reshape(many * each, length), right)
                total = part if total is None else total + part
            store[...] = total.astype(bf16)
        else:
            for n in range(many):
                total = sum(dot(left[n, :, at : at + length], right) for at, left, right in pieces)
                store[n * each : (n + 1) * each, :] = total.astype(bf16)

    @pl.when(step == turns + 2 * groups)
    def _():
        for copy in turned():
            copy.wait()
        for turn in range(turns):
            px_copy(turn).wait()
        for seq in range(seqs):
            pr_copy(seq).wait()

    @pl.when((step >= turns + 2 * groups) & (step < turns + 3 * groups))
    def _():
        group = step - turns - 2 * groups
        at = [group + seq * groups for seq in range(seqs)]
        own_rows([pxs[n] for n in at], [px2s[n] for n in at], partx_ref)

    @pl.when(step == last)
    def _():
        own_rows([prs[n] for n in range(seqs)], [pr2s[n] for n in range(seqs)], partr_ref)

    for when in sorted(plan):
        @pl.when(step == when)
        def _(when=when):
            if when == min(plan):
                for copy in ring.loads():
                    copy.wait()
            for kind, hop, slot in plan[when]:
                if kind == "hop":
                    ring.hop(hop, slot)
                    continue
                for k in range(count):
                    ring.land(k, slot, owns[k].at[slot])
                    if slot < 2:
                        links.send(
                            lambda k=k, slot=slot: owns[k].at[slot], lambda k=k, slot=slot: nears[k].at[slot],
                            lambda k=k, slot=slot: near_send.at[2 * k + slot], lambda k=k, slot=slot: near_recv.at[2 * k + slot], links.peer)

    @pl.when(step == last)
    def _():
        sg_ref[6:7, : gg_ref.shape[1]] = gg_ref[0:1, :]
        for slot in range(2):
            for k in range(count):
                links.arrived(nears[k].at[slot], near_send.at[2 * k + slot], near_recv.at[2 * k + slot])
        links.finish()


def middle(projected, gy, rs, segr, cw, hp, cp, gg, mixed, w_out_full, tokens, gz, w_in_full, left, left2, arrays, heads, state, devices):
    seqs, _, length = segr.shape
    inner = gy.shape[1]
    width = tokens.shape[1]
    groups = inner // GROUP
    rows = seqs * length
    turns = seqs * groups
    chips = devices // 2
    items = tuple(a.shape[2:] for a in arrays)
    count = len(items)
    dma = pltpu.SemaphoreType.DMA
    seq = lambda i: jnp.minimum(i // groups, seqs - 1)
    grp = lambda i: jnp.where(i < turns, i % groups, groups - 1)
    out_at = lambda i: jnp.clip(i - turns, 0, groups - 1)
    in_at = lambda i: jnp.clip(i - turns - groups, 0, groups - 1)
    x_at = lambda i: jnp.clip(i - turns - 2 * groups, 0, groups - 1)
    total = chips * left.shape[2]
    const = lambda *shape: pl.BlockSpec(shape, lambda i: (0,) * len(shape), pipeline_mode=pl.Buffered(1))
    any_spec = pl.BlockSpec(memory_space=pl.ANY)
    small_width = inner + 3 * LANES
    return pl.pallas_call(
        functools.partial(middle_kernel, heads, chips, seqs, groups, items),
        grid=(turns + 3 * groups + 1,),
        in_specs=[
            pl.BlockSpec((length, GROUP), lambda i: (seq(i), groups + grp(i))),
            pl.BlockSpec((length, 2 * state), lambda i: (seq(i), 2 * inner // (2 * state))),
            pl.BlockSpec((length, LANES), lambda i: (seq(i), (2 * inner + 2 * state) // LANES)),
            pl.BlockSpec((length, GROUP), lambda i: (seq(i), grp(i))),
            pl.BlockSpec((1, length, LANES), lambda i: (seq(i), 0, 0)),
            pl.BlockSpec((1, 8, length), lambda i: (seq(i), 0, 0)),
            pl.BlockSpec((8, GROUP), lambda i: (0, grp(i))),
            pl.BlockSpec((8, 2 * state), lambda i: (0, inner // (2 * state))),
            pl.BlockSpec((8, LANES), lambda i: (0, 0)),
            pl.BlockSpec((8, GROUP), lambda i: (0, grp(i))),
            const(8, inner),
            pl.BlockSpec((rows, GROUP), lambda i: (0, out_at(i))),
            pl.BlockSpec((GROUP, width), lambda i: (out_at(i), 0)),
            const(rows, width),
            pl.BlockSpec((rows, GROUP), lambda i: (0, in_at(i))),
            pl.BlockSpec((width, GROUP), lambda i: (0, in_at(i))),
        ] + [any_spec] * (2 + count),
        out_specs=[
            pl.BlockSpec((length, GROUP), lambda i: (seq(i), grp(i))),
            pl.BlockSpec((length, 3 * LANES), lambda i: (seq(i), 0)),
            pl.BlockSpec((total, GROUP), lambda i: (0, x_at(i))),
            const(total, 3 * LANES),
            const(8, small_width),
            const(rows, width),
            const(rows, width),
        ] + [const(3, *item) for item in items] + [any_spec] * count,
        out_shape=[
            jax.ShapeDtypeStruct((rows, inner), bf16),
            jax.ShapeDtypeStruct((rows, 3 * LANES), bf16),
            jax.ShapeDtypeStruct((total, inner), bf16),
            jax.ShapeDtypeStruct((total, 3 * LANES), bf16),
            jax.ShapeDtypeStruct((8, small_width), f32),
            jax.ShapeDtypeStruct((rows, width), bf16),
            jax.ShapeDtypeStruct((rows, width), f32),
        ] + [jax.ShapeDtypeStruct((3,) + item, bf16) for item in items] + [jax.ShapeDtypeStruct((2,) + item, bf16) for item in items],
        scratch_shapes=small_scratch(length) + [
            pltpu.VMEM((length, length), f32),
            pltpu.VMEM((length, length), f32),
            pltpu.VMEM((length, LANES), f32),
            pltpu.VMEM((length, LANES), f32),
            pltpu.VMEM((chips,) + left.shape[2:], bf16),
            pltpu.VMEM((chips,) + left.shape[2:], bf16),
            pltpu.VMEM((turns, length, GROUP), bf16),
            pltpu.VMEM((seqs, length, 3 * LANES), bf16),
            pltpu.VMEM((turns, length, GROUP), bf16),
            pltpu.VMEM((seqs, length, 3 * LANES), bf16),
            dma((2,)), dma((turns,)), dma((turns,)), dma((seqs,)), dma((seqs,)), dma((2 * count,)), dma((2 * count,)),
        ] + ring_scratch(items, chips),
        compiler_params=pltpu.CompilerParams(collective_id=1, has_side_effects=True, vmem_limit_bytes=FULL),
        name="middle",
    )(projected, projected, projected, gy, rs, segr, cw, cw, hp, cp, gg, mixed, w_out_full, tokens, gz, w_in_full, left, left2, *arrays)


def tail_kernel(chips, groups, used, items, early, px_ref, pr_ref, win_ref, gacc_ref, tok_ref, cot_ref, gain_ref, sg_ref, *refs):
    count, first = len(items), len(early)
    parts, halves, refs = refs[:count], refs[count : count + first], refs[count + first :]
    gt_ref, small_ref, refs = refs[0], refs[1], refs[2:]
    last_in, last_out, refs = refs[: first + count], refs[first + count : first + 2 * count], refs[first + 2 * count :]
    (small_in, small_sent, small_recv, small_send, small_sem, last_send, last_recv), refs = refs[:7], refs[7:]
    (held, ring_in, peer_in), sems = split_scratch(refs, count)
    step = pl.program_id(0)
    links = Links(chips)
    ring = Ring(links, items, 0, parts, held, ring_in, peer_in, *sems)
    rounds = len(links.turns)

    def swap(k, slot, source):
        at = k * 3 + slot
        links.send(source, lambda: last_in[k].at[slot], lambda: last_send.at[at], lambda: last_recv.at[at], links.peer)

    @pl.when(step == 0)
    def _():
        links.greet(list(links.ways) + links.turns)
        ring.start()
        for k in range(first):
            links.send(lambda k=k: halves[k].at[2], lambda k=k: last_in[k].at[0], lambda k=k: last_send.at[3 * k], lambda k=k: last_recv.at[3 * k], links.peer)
        gt_ref[...] = gacc_ref[...] + dot(px_ref[...], win_ref[...], NT)

    @pl.when((step > 0) & (step < groups))
    def _():
        gt_ref[...] += dot(px_ref[...], win_ref[...], NT)

    every = ring.sequence()
    inside, later = every[:2], every[2:]

    def run(kind, hop, slot):
        if kind == "hop":
            ring.hop(hop, slot)
            return
        for k in range(count):
            ring.land(k, slot, last_out[k].at[slot])
            swap(first + k, slot, lambda k=k, slot=slot: last_out[k].at[slot])

    for n, entry in enumerate(inside):
        @pl.when(step == min(groups - 1, 2 + 2 * n))
        def _(n=n, entry=entry):
            if n == 0:
                for copy in ring.loads():
                    copy.wait()
            run(*entry)

    def small_round(turn):
        links.send(
            lambda: small_in if turn == 0 else small_sent.at[turn - 1], lambda: small_recv.at[turn],
            lambda: small_send.at[turn], lambda: small_sem.at[turn], links.turns[turn])

    def small_finish(turn):
        value = small_in if turn == 0 else small_sent.at[turn - 1]
        links.arrived(small_recv.at[turn], small_send.at[turn], small_sem.at[turn])
        store = small_ref if turn == rounds - 1 else small_sent.at[turn]
        store[...] = value[...] + small_recv[turn]

    @pl.when(step == groups)
    def _():
        size = pr_ref.shape[1]
        col = lax.broadcasted_iota(jnp.int32, (win_ref.shape[0], size), 1)
        rest = jnp.where(col < used, win_ref[:, :size].astype(f32), 0.0).astype(bf16)
        rows, width = gt_ref.shape

        def close(i):
            sl = slice(i * BLOCK, (i + 1) * BLOCK)
            u = tok_ref[sl].astype(f32)
            rstd = lax.rsqrt(jnp.mean(u * u, axis=1, keepdims=True) + epsilon)
            unit = u * rstd
            gn = gt_ref[sl] + dot(pr_ref[sl], rest, NT)
            small_in[7:8, :width] = small_in[7:8, :width] + jnp.sum(gn * unit, axis=0, keepdims=True)
            gu = gn * gain_ref[0:1, :]
            inward = jnp.mean(gu * unit, axis=1, keepdims=True)
            gt_ref[sl] = cot_ref[sl].astype(f32) + rstd * (gu - unit * inward)

        small_in[...] = sg_ref[...]
        chunks, done = 0, -1
        for entry in later:
            if chunks < rows // BLOCK:
                close(chunks)
                chunks += 1
            run(*entry)
            if chunks == rows // BLOCK:
                if done < 0:
                    small_round(0)
                    done = 0
                elif done < rounds - 1:
                    small_finish(done)
                    done += 1
                    small_round(done)
        while done < rounds:
            small_finish(done)
            done += 1
            if done < rounds:
                small_round(done)
        for slot in range(3):
            for k in range(first + count):
                at = k * 3 + slot
                if k >= first or slot == 0:
                    links.arrived(last_in[k].at[slot], last_send.at[at], last_recv.at[at])
        links.finish()


def tail(px, pr, w_in_full, gacc, tokens, cot, gain, sg, arrays, halves, used, devices):
    rows, width = tokens.shape
    groups = px.shape[1] // GROUP
    chips = devices // 2
    items = tuple(a.shape[2:] for a in arrays)
    early = tuple(h.shape[1:] for h in halves)
    count, first = len(items), len(early)
    rounds = chips.bit_length() + 1
    dma = pltpu.SemaphoreType.DMA
    const = lambda *shape: pl.BlockSpec(shape, lambda i: (0,) * len(shape), pipeline_mode=pl.Buffered(1))
    any_spec = pl.BlockSpec(memory_space=pl.ANY)
    every = early + items
    return pl.pallas_call(
        functools.partial(tail_kernel, chips, groups, used, items, early),
        grid=(groups + 1,),
        in_specs=[
            pl.BlockSpec((rows, GROUP), lambda i: (0, jnp.minimum(i, groups - 1))),
            const(rows, pr.shape[1]),
            pl.BlockSpec((width, GROUP), lambda i: (0, groups + i)),
            const(rows, width),
            const(rows, width),
            const(rows, width),
            const(8, width),
            const(*sg.shape),
        ] + [any_spec] * (count + first),
        out_specs=[const(rows, width), const(*sg.shape)] + [any_spec] * len(every) + [const(3, *item) for item in items],
        out_shape=[jax.ShapeDtypeStruct((rows, width), f32), jax.ShapeDtypeStruct(sg.shape, f32)]
        + [jax.ShapeDtypeStruct(((1 if k < first else 3),) + item, bf16) for k, item in enumerate(every + items)],
        scratch_shapes=[
            pltpu.VMEM(sg.shape, f32), pltpu.VMEM((rounds,) + sg.shape, f32), pltpu.VMEM((rounds,) + sg.shape, f32),
            dma((rounds,)), dma((rounds,)), dma((3 * (first + count),)), dma((3 * (first + count),)),
        ] + ring_scratch(items, chips),
        compiler_params=pltpu.CompilerParams(collective_id=2, has_side_effects=True, vmem_limit_bytes=FULL),
        name="tail",
    )(px, pr, w_in_full, gacc, tokens, cot, gain, sg, *arrays, *halves)


def finish_kernel(sizes, count, first, where_ref, *refs):
    taps, share_c, share_g, share_n, heads, columns = sizes
    mine, theirs, nears, refs = refs[:count], refs[count : 2 * count], refs[2 * count : 2 * count + first], refs[2 * count + first :]
    small_ref, w_out_ref, w_in_ref, norm_ref, kernel_ref, shift_ref, dt_ref, rate_ref, skip_ref, gate_ref = refs
    me, plane = where_ref[0], where_ref[1]
    span = small_ref.shape[1]
    begin = 0
    for k in range(count):
        rows, width = mine[k].shape[1:]
        store = w_out_ref if k == 0 else w_in_ref
        left = 0 if k == 0 else begin
        used = min(width, store.shape[1] - left)
        for slot in range(2):
            total = mine[k][slot].astype(f32) + (nears if k < first else theirs)[k][slot].astype(f32)
            store[slot * rows : (slot + 1) * rows, left : left + used] = total[:, :used]
        own, other = mine[k][2].astype(f32), theirs[k][0 if k < first else 2].astype(f32)
        low = jnp.where(plane == 0, own, other)
        high = jnp.where(plane == 0, other, own)
        store[2 * rows : 3 * rows, left : left + used] = low[:, :used]
        store[3 * rows : 4 * rows, left : left + used] = high[:, :used]
        if k:
            begin += width
    small = small_ref[...]
    conv = pltpu.roll(small, lax.rem(span - me * share_c, span), 1)
    kernel_ref[...] = conv[:taps, :share_c]
    shift_ref[...] = conv[taps : taps + 1, :share_c]
    gate_ref[...] = pltpu.roll(small, lax.rem(span - me * share_g, span), 1)[6:7, :share_g]
    norm_ref[...] = pltpu.roll(small, lax.rem(span - me * share_n, span), 1)[7:8, :share_n]
    inner = span - 3 * LANES
    dt_ref[...] = small[0:1, inner + 2 * LANES : inner + 2 * LANES + heads]
    rate_ref[...] = small[1:2, inner + 2 * LANES : inner + 2 * LANES + heads]
    size = inner // heads
    source = lax.broadcasted_iota(jnp.int32, (inner, LANES), 0) // size
    pick = (source == lax.broadcasted_iota(jnp.int32, (inner, LANES), 1)).astype(f32)
    skip_ref[...] = dot(small[:, :inner], pick, precision=highest)[taps + 1 : taps + 2, :heads]


def finish(me, plane, mine, theirs, nears, small, taps, share_c, share_g, share_n, heads, columns):
    count = len(mine)
    out = lambda *shape: jax.ShapeDtypeStruct(shape, f32)
    spec = pl.BlockSpec(memory_space=pltpu.VMEM)
    shapes = [out(4 * mine[0].shape[1], mine[0].shape[2]), out(4 * mine[1].shape[1], columns), out(1, share_n), out(taps, share_c),
              out(1, share_c), out(1, heads), out(1, heads), out(1, heads), out(1, share_g)]
    return pl.pallas_call(
        functools.partial(finish_kernel, (taps, share_c, share_g, share_n, heads, columns), count, len(nears)),
        in_specs=[pl.BlockSpec(memory_space=pltpu.SMEM)] + [spec] * (2 * count + len(nears) + 1),
        out_specs=[spec] * len(shapes),
        out_shape=shapes,
        name="finish",
    )(jnp.stack([me, plane]).astype(jnp.int32), *mine, *theirs, *nears, small)


def parts_kernel(core_ref, a_ref, a2_ref, b_ref, b2_ref, o_ref):
    rows = o_ref.shape[0]
    a = a_ref[...].reshape(rows, a_ref.shape[3])
    a2 = a2_ref[...].reshape(rows, a2_ref.shape[3])
    o_ref[...] = (dot(a, b_ref[...]) + dot(a2, b2_ref[...])).astype(bf16)


def grad_parts(core, left, left2, right, right2, name):
    chips, _, rows, tokens = left.shape
    if rows % 16:
        pick = lambda v: lax.dynamic_index_in_dim(v, core, 1, keepdims=False).reshape(1, 1, chips * rows, tokens)
        left, left2, core, chips, rows = pick(left), pick(left2), 0, 1, chips * rows
    width = right.shape[1]
    tile = min(GROUP, width)
    left_spec = pl.BlockSpec((chips, 1, rows, tokens), lambda i, c: (0, c[0], 0, 0), pipeline_mode=pl.Buffered(1))
    total = chips * rows
    return pl.pallas_call(
        parts_kernel,
        grid_spec=pltpu.PrefetchScalarGridSpec(
            num_scalar_prefetch=1,
            grid=(width // tile,),
            in_specs=[
                left_spec, left_spec,
                pl.BlockSpec((tokens, tile), lambda i, c: (0, i)),
                pl.BlockSpec((tokens, tile), lambda i, c: (0, i)),
            ],
            out_specs=pl.BlockSpec((total, tile), lambda i, c: (0, i)),
        ),
        out_shape=jax.ShapeDtypeStruct((total, width), bf16),
        compiler_params=pltpu.CompilerParams(vmem_limit_bytes=FULL),
        cost_estimate=pl.CostEstimate(flops=4 * total * tokens * width, bytes_accessed=2 * (2 * total * tokens + 2 * tokens * width + total * width), transcendentals=0),
        name=name,
    )(jnp.full((1,), core, jnp.int32), left, left2, right, right2)


def small_rows(size):
    return 16 * (-(-size // (16 * LANES)))


def flat_pack(parts, rows):
    flat = jnp.concatenate([p.reshape(-1) for p in parts])
    return jnp.pad(flat, (0, rows * LANES - flat.shape[0])).reshape(rows, LANES)


def local(devices, tokens, segments, norm_gain, w_in, conv_weight, conv_bias, dt_bias, a_log, d_skip, gate_gain, w_out, cotangent):
    seqs, length, width = tokens.shape
    rows = seqs * length
    proj_width = w_in.shape[1]
    inner = devices * w_out.shape[0]
    taps = conv_weight.shape[0]
    heads = dt_bias.shape[0]
    share_n, share_c, share_g = norm_gain.shape[0], conv_bias.shape[0], gate_gain.shape[0]
    conv_width = devices * share_c
    state = (conv_width - inner) // 2
    chips = devices // 2
    me = lax.axis_index("fsdp")
    core = me % 2
    swap = [(i, i + 1 - 2 * (i % 2)) for i in range(devices)]
    partner = lambda value: lax.ppermute(value, "fsdp", swap)

    size = share_n + share_g + (taps + 1) * share_c
    pack = flat_pack([norm_gain, gate_gain, conv_weight, conv_bias], small_rows(size))
    win_all, wout_all, pack_all = gather(
        [w_in.reshape(PIECES, -1, proj_width), w_out.reshape(PIECES, -1, width), pack], devices)
    w_in_full = win_all.reshape(width, proj_width)
    w_out_full = wout_all.reshape(inner, width)
    pack_all = pack_all.reshape(devices, -1)
    cuts = [share_n, share_n + share_g, share_n + share_g + taps * share_c, size]
    gain_full = pack_all[:, : cuts[0]].reshape(width)
    gate_full = pack_all[:, cuts[0] : cuts[1]].reshape(inner)
    kernel_full = pack_all[:, cuts[1] : cuts[2]].reshape(devices, taps, share_c).transpose(1, 0, 2).reshape(taps, conv_width)
    shift_full = pack_all[:, cuts[2] : cuts[3]].reshape(conv_width)

    flat_tokens = tokens.reshape(rows, width)
    residual = flat_tokens.astype(f32)
    rstd = lax.rsqrt(jnp.mean(residual * residual, axis=-1, keepdims=True) + epsilon)
    gain_f = gain_full.astype(f32)
    normed = (residual * rstd * gain_f).astype(bf16)
    grad_rows = cotangent.reshape(rows, width)
    grad_rows2 = partner(grad_rows)
    normed, normed_t = lax.optimization_barrier((normed, normed.T.reshape(chips, 2, -1, rows)))
    normed_t2 = partner(normed_t)
    projected = dot(normed, w_in_full)
    gm = dot(grad_rows, w_out_full, NT)
    tables = mixer_tables(segments, kernel_full, shift_full, dt_bias, a_log, d_skip, gate_full)
    segr, cw, hp, cp = tables
    hp, normed_t2, grad_rows2 = lax.optimization_barrier((hp, normed_t2, grad_rows2))
    tables = segr, cw, hp, cp
    mixed, mixed_t, gz, gy, rs, gg = mixer_forward(projected, gm, *tables, heads, state)
    mixed_t = mixed_t.reshape(chips, 2, -1, rows)
    gz2, mixed_t2 = partner(gz), partner(mixed_t)
    quarters = lambda part: part.reshape(chips, QUARTERS, -1, part.shape[1])
    part_out = quarters(grad_parts(core, mixed_t, mixed_t2, grad_rows, grad_rows2, "grad_out"))
    part_z = quarters(grad_parts(core, normed_t, normed_t2, gz, gz2, "grad_z"))
    px, pr, part_x, part_r, sg, block_out, gacc, half_out, half_z, *nears = middle(
        projected, gy, rs, *tables, gg, mixed, w_out_full, flat_tokens, gz, w_in_full, normed_t, normed_t2, [part_out, part_z], heads, state, devices)
    gain8 = jnp.broadcast_to(gain_f[None], (8, width))
    grad_tokens, small, *theirs, half_x, half_r = tail(
        px, pr, w_in_full, gacc, flat_tokens, grad_rows, gain8, sg, [quarters(part_x), quarters(part_r)], [half_out, half_z], 2 * state + heads, devices)
    grad_w_out, grad_w_in, norm, kernel, shift, offset, rate, skip, gate = finish(
        me, lax.axis_index("dp"), [half_out, half_z, half_x, half_r], theirs, nears, small, taps, share_c, share_g, share_n, heads, proj_width)
    return (
        block_out.reshape(seqs, length, width),
        grad_tokens.reshape(seqs, length, width),
        norm[0],
        grad_w_in,
        kernel,
        shift[0],
        offset[0],
        rate[0],
        skip[0],
        gate[0],
        grad_w_out,
    )


def solution(mesh):
    rows3, rows2 = P(("fsdp", "dp"), None, None), P(("fsdp", "dp"), None)
    return jax.shard_map(
        functools.partial(local, mesh.shape["fsdp"]),
        mesh=mesh,
        in_specs=(rows3, rows2, P("fsdp"), P("fsdp", None), P(None, "fsdp"), P("fsdp"), P(), P(), P(), P("fsdp"), P("fsdp", None), rows3),
        out_specs=(rows3, rows3, P("fsdp"), P("fsdp", None), P(None, "fsdp"), P("fsdp"), P(), P(), P(), P("fsdp"), P("fsdp", None)),
        check_vma=False,
    )
```

```python
import functools

import jax
import jax.numpy as jnp
from jax import lax
from jax.experimental import pallas as pl
from jax.experimental.pallas import tpu as pltpu
from jax.sharding import PartitionSpec as P

f32, bf16 = jnp.float32, jnp.bfloat16
highest = lax.Precision.HIGHEST
epsilon = 1e-05
LANES = 128
BLOCK = 128
GROUP = 512
PAIRS = GROUP // LANES
NT = (((1,), (1,)), ((), ()))
NN = (((1,), (0,)), ((), ()))


def dot(a, b, dims=NN, precision=None):
    return lax.dot_general(a, b, dims, precision=precision, preferred_element_type=f32)


def sigmoid(v):
    return 0.5 + 0.5 * jnp.tanh(0.5 * v)


def conv_taps(xin, masks):
    taps = []
    for shift in (3, 2, 1):
        taps.append(pltpu.roll(xin, shift, 0) * masks[3 - shift])
    taps.append(xin)
    return taps


def conv_sum(taps, cw):
    total = cw[4:5, :] + cw[3:4, :] * taps[3]
    for k in range(3):
        total = total + cw[k : k + 1, :] * taps[k]
    return total


def conv_back(gsum, xin, cw, masks, length):
    grads = []
    gx = cw[3:4, :] * gsum
    for shift in (3, 2, 1):
        masked = gsum * masks[3 - shift]
        grads.append(jnp.sum(masked * pltpu.roll(xin, shift, 0), axis=0, keepdims=True))
        gx = gx + cw[3 - shift : 4 - shift, :] * pltpu.roll(masked, length - shift, 0)
    grads.append(jnp.sum(gsum * xin, axis=0, keepdims=True))
    grads.append(jnp.sum(gsum, axis=0, keepdims=True))
    return gx, grads


def prologue(heads, bc_ref, dtr_ref, segr_ref, cwbc_ref, hp_ref, mask_s, b_s, c_s, dt_s, cum_s, cumt_s, ef_s, la_s, sp_s):
    length = bc_ref.shape[0]
    segc = segr_ref[0].T
    here = lax.broadcasted_iota(jnp.int32, segc.shape, 0)
    for shift in (1, 2, 3):
        alike = (pltpu.roll(segc, shift, 0) == segc) & (here >= shift)
        mask_s[3 - shift] = jnp.broadcast_to(jnp.where(alike, 1.0, 0.0)[:, 0:1], (length, LANES))
    masks = [mask_s[k] for k in range(3)]
    for half, ref in ((0, b_s), (1, c_s)):
        sl = slice(half * LANES, (half + 1) * LANES)
        taps = conv_taps(bc_ref[:, sl], masks)
        summed = conv_sum(taps, cwbc_ref[:, sl])
        ref[...] = summed * sigmoid(summed)
    lane = lax.broadcasted_iota(jnp.int32, (length, LANES), 1)
    raw = jnp.where(lane < heads, dtr_ref[...] + hp_ref[0:1, :], 0.0)
    soft = jnp.maximum(raw, 0.0) + jnp.log1p(jnp.exp(-jnp.abs(raw)))
    dt = jnp.where(lane < heads, soft, 0.0)
    la = -dt * jnp.exp(hp_ref[1:2, :])
    row = lax.broadcasted_iota(jnp.int32, (length, length), 0)
    col = lax.broadcasted_iota(jnp.int32, (length, length), 1)
    tri = jnp.where(row >= col, 1.0, 0.0).astype(f32)
    cum = dot(tri, la, precision=highest)
    dt_s[...] = dt
    la_s[...] = la
    cum_s[...] = cum
    cumt_s[...] = cum.T
    sp_s[...] = sigmoid(raw)
    mid = cum[BLOCK - 1 : BLOCK, :]
    ef_s[:BLOCK] = jnp.exp(jnp.minimum(mid - cum[:BLOCK], 0.0))
    ef_s[BLOCK:] = jnp.exp(jnp.minimum(cum[BLOCK:] - mid, 0.0))
    same = (segc[:, 0:1] == segr_ref[0, 0:1, :]).astype(f32)
    return row, col, same


def headpick(first, shape):
    source = lax.broadcasted_iota(jnp.int32, shape, 0) // 64
    target = lax.broadcasted_iota(jnp.int32, shape, 1)
    source = source - 2 * (source // 2)
    return jnp.where(target == source + first, 1.0, 0.0).astype(bf16)


def headsum(value, pick):
    hi = value.astype(bf16)
    lo = (value - hi.astype(f32)).astype(bf16)
    return dot(jnp.concatenate([hi, lo], axis=1), pick)


def fwd_kernel(heads, z_ref, x_ref, bc_ref, dtr_ref, gm_ref, segr_ref, cwx_ref, cwbc_ref, hp_ref, cp_ref,
               mixed_ref, mixt_ref, gz_ref, gy_ref, rs_ref, gg_ref,
               mask_s, b_s, c_s, dt_s, cum_s, cumt_s, ef_s, la_s, sp_s, sm_s, ssm_s, yd_s, u_s, st_s, rs_s):
    phase, group = pl.program_id(1), pl.program_id(2)
    length = z_ref.shape[0]
    lane = lax.broadcasted_iota(jnp.int32, (length, LANES), 1)
    first = lane < 64
    half = lax.broadcasted_iota(jnp.int32, (BLOCK, LANES), 1) < 64

    @pl.when((phase == 0) & (group == 0))
    def _():
        row, col, same = prologue(heads, bc_ref, dtr_ref, segr_ref, cwbc_ref, hp_ref, mask_s, b_s, c_s, dt_s, cum_s, cumt_s, ef_s, la_s, sp_s)
        scores = dot(c_s[...], b_s[...], NT, precision=highest)
        sm_s[...] = jnp.where(row >= col, scores * same, 0.0)
        st_s[...] = jnp.zeros_like(st_s)

    width = jnp.int32(8)
    shift = lax.rem(jnp.int32(LANES) - width * group, jnp.int32(LANES))

    @pl.when(phase == 0)
    def _():
        masks = [mask_s[k] for k in range(3)]
        dtg = pltpu.roll(dt_s[...], shift, 1)
        cumg = pltpu.roll(cum_s[...], shift, 1)
        efg = pltpu.roll(ef_s[...], shift, 1)
        cumt = cumt_s[pl.ds(pl.multiple_of(group * 8, 8), 8), :]
        square, across = st_s[0], st_s[1]
        for j in range(PAIRS):
            sl = slice(j * LANES, (j + 1) * LANES)
            place = pl.ds(pl.multiple_of(group * GROUP + j * LANES, LANES), LANES)
            xin = x_ref[:, sl]
            summed = conv_sum(conv_taps(xin, masks), cwx_ref[:, sl])
            xs = summed * sigmoid(summed)
            dtb = jnp.where(first, dtg[:, 2 * j : 2 * j + 1], dtg[:, 2 * j + 1 : 2 * j + 2])
            efb = jnp.where(first, efg[:, 2 * j : 2 * j + 1], efg[:, 2 * j + 1 : 2 * j + 2])
            xd = xs * dtb
            for i in range(2):
                rows = slice(i * BLOCK, (i + 1) * BLOCK)
                part = xd[rows]
                stack = jnp.concatenate([jnp.where(half, part, 0.0), jnp.where(half, 0.0, part)], axis=0).astype(bf16)
                decays = []
                for h in range(2):
                    arg = cumg[rows, 2 * j + h : 2 * j + h + 1] - cumt[2 * j + h : 2 * j + h + 1, rows]
                    decays.append((jnp.exp(jnp.minimum(arg, 0.0)) * sm_s[rows, rows]).astype(bf16))
                yd_s[rows, place] = dot(jnp.concatenate(decays, axis=1), stack)
            far = (xd[:BLOCK] * efb[:BLOCK]).astype(bf16)
            u = dot(sm_s[BLOCK:, :BLOCK].astype(bf16), far)
            u_s[:, place] = u
            base = yd_s[:, place] + cp_ref[0:1, sl] * xs
            ssm = jnp.concatenate([base[:BLOCK], base[BLOCK:] + efb[BLOCK:] * u], axis=0)
            ssm_s[:, place] = ssm
            zin = z_ref[:, sl]
            gated = ssm * (zin * sigmoid(zin))
            square = square + gated * gated
            across = across + gm_ref[:, sl] * cp_ref[1:2, sl] * gated
        st_s[0] = square
        st_s[1] = across

    @pl.when((phase == 1) & (group == 0))
    def _():
        inner = heads * 64
        mean = jnp.sum(st_s[0], axis=1, keepdims=True) / inner
        scale = lax.rsqrt(mean + epsilon)
        inward = jnp.sum(st_s[1], axis=1, keepdims=True) / inner
        st_s[0] = jnp.broadcast_to(scale, (length, LANES))
        st_s[1] = jnp.broadcast_to(scale * scale * scale * inward, (length, LANES))
        rs_s[...] = jnp.zeros_like(rs_s)

    @pl.when(phase == 1)
    def _():
        scale, lean = st_s[0], st_s[1]
        efg = pltpu.roll(ef_s[...], shift, 1)
        total = rs_s[...]
        for j in range(PAIRS):
            sl = slice(j * LANES, (j + 1) * LANES)
            place = pl.ds(pl.multiple_of(group * GROUP + j * LANES, LANES), LANES)
            zin = z_ref[:, sl]
            sg = sigmoid(zin)
            silu = zin * sg
            dsilu = sg + silu * (1.0 - sg)
            ssm = ssm_s[:, place]
            gated = ssm * silu
            unit = gated * scale
            gain = cp_ref[1:2, sl]
            gm = gm_ref[:, sl]
            mixed = unit * gain
            mixed_ref[:, sl] = mixed.astype(bf16)
            mixt_ref[sl, :] = mixed.T.astype(bf16)
            gain_sum = jnp.sum(gm * unit, axis=0, keepdims=True)
            old = gg_ref[0:1, place]
            gg_ref[:, place] = jnp.broadcast_to(jnp.where(pl.program_id(0) == 0, gain_sum, old + gain_sum), (8, LANES))
            ggated = scale * (gm * gain) - gated * lean
            gz_ref[:, sl] = (ggated * ssm * dsilu).astype(bf16)
            gy = ggated * silu
            gy_ref[:, sl] = gy
            efb = jnp.where(first, efg[:, 2 * j : 2 * j + 1], efg[:, 2 * j + 1 : 2 * j + 2])
            near = gy.astype(bf16).astype(f32) * yd_s[:, place]
            fare = (gy[BLOCK:] * efb[BLOCK:]).astype(bf16).astype(f32) * u_s[:, place]
            value = jnp.concatenate([near[:BLOCK], near[BLOCK:] + fare], axis=0)
            total = total + headsum(value, headpick(8 * group + 2 * j, (2 * LANES, LANES)))
        rs_s[...] = total
        rs_ref[0] = total


def mixer_back(heads, groups, group, opening, x_ref, bc_ref, dtr_ref, gy_ref, rs_ref, segr_ref, cwx_ref, cwbc_ref, hp_ref, cp_ref,
               px_ref, pr_ref, sg_ref,
               mask_s, b_s, c_s, dt_s, cum_s, cumt_s, ef_s, la_s, sp_s, smt_s, gst_s, gc_s, gd_s):
    length = x_ref.shape[0]
    inner_width = groups * GROUP

    def keep(row, cols, value):
        sg_ref[row : row + 1, cols] = sg_ref[row : row + 1, cols] + value

    @pl.when(opening)
    def _():
        sg_ref[...] = jnp.zeros_like(sg_ref)

    lane = lax.broadcasted_iota(jnp.int32, (length, LANES), 1)
    first = lane < 64
    half = lax.broadcasted_iota(jnp.int32, (BLOCK, LANES), 1) < 64

    @pl.when(group == 0)
    def _():
        row, col, same = prologue(heads, bc_ref, dtr_ref, segr_ref, cwbc_ref, hp_ref, mask_s, b_s, c_s, dt_s, cum_s, cumt_s, ef_s, la_s, sp_s)
        scores = dot(b_s[...], c_s[...], NT, precision=highest)
        smt_s[...] = jnp.where(row <= col, scores * same, 0.0)
        gst_s[...] = jnp.zeros_like(gst_s)
        gc_s[...] = jnp.zeros_like(gc_s)
        gd_s[...] = jnp.zeros_like(gd_s)

    shift = lax.rem(jnp.int32(LANES) - jnp.int32(8) * group, jnp.int32(LANES))
    masks = [mask_s[k] for k in range(3)]
    dtg = pltpu.roll(dt_s[...], shift, 1)
    cumg = pltpu.roll(cum_s[...], shift, 1)
    efg = pltpu.roll(ef_s[...], shift, 1)
    cumt = cumt_s[pl.ds(pl.multiple_of(group * 8, 8), 8), :]
    gcum, gdir = gc_s[...], gd_s[...]
    for j in range(PAIRS):
        sl = slice(j * LANES, (j + 1) * LANES)
        xin = x_ref[:, sl]
        cw = cwx_ref[:, sl]
        summed = conv_sum(conv_taps(xin, masks), cw)
        sg = sigmoid(summed)
        xs = summed * sg
        dtb = jnp.where(first, dtg[:, 2 * j : 2 * j + 1], dtg[:, 2 * j + 1 : 2 * j + 2])
        efb = jnp.where(first, efg[:, 2 * j : 2 * j + 1], efg[:, 2 * j + 1 : 2 * j + 2])
        xd = xs * dtb
        gy = gy_ref[:, sl]
        gyb = gy.astype(bf16)
        inner = []
        for i in range(2):
            rows = slice(i * BLOCK, (i + 1) * BLOCK)
            part, gpart = xd[rows], gy[rows]
            stack = jnp.concatenate([jnp.where(half, part, 0.0), jnp.where(half, 0.0, part)], axis=0).astype(bf16)
            gstack = jnp.concatenate([jnp.where(half, gpart, 0.0), jnp.where(half, 0.0, gpart)], axis=0).astype(bf16)
            gw = dot(stack, gyb[rows], NT)
            weights = []
            gscore = gst_s[rows, rows]
            for h in range(2):
                arg = cumt[2 * j + h : 2 * j + h + 1, rows] - cumg[rows, 2 * j + h : 2 * j + h + 1]
                decay = jnp.exp(jnp.minimum(arg, 0.0))
                weights.append((decay * smt_s[rows, rows]).astype(bf16))
                gscore = gscore + gw[h * BLOCK : (h + 1) * BLOCK] * decay
            gst_s[rows, rows] = gscore
            inner.append(dot(jnp.concatenate(weights, axis=1), gstack))
        far = (xd[:BLOCK] * efb[:BLOCK]).astype(bf16)
        ge = (gy[BLOCK:] * efb[BLOCK:]).astype(bf16)
        gst_s[:BLOCK, BLOCK:] += dot(far, ge, NT)
        gfar = dot(smt_s[:BLOCK, BLOCK:].astype(bf16), ge)
        xdb = xd.astype(bf16).astype(f32)
        fall0 = xdb[:BLOCK] * inner[0] + far.astype(f32) * gfar
        fall = jnp.concatenate([fall0, xdb[BLOCK:] * inner[1]], axis=0)
        gxd = jnp.concatenate([inner[0] + efb[:BLOCK] * gfar, inner[1]], axis=0)
        sums = headsum(jnp.concatenate([fall, xs * gxd], axis=0), headpick(8 * group + 2 * j, (2 * LANES, LANES)))
        gcum = gcum - sums[:length]
        gdir = gdir + sums[length:]
        gxs = cp_ref[0:1, sl] * gy + dtb * gxd
        gsum = gxs * (sg + xs * (1.0 - sg))
        gx, grads = conv_back(gsum, xin, cw, masks, length)
        px_ref[:, sl] = gx.astype(bf16)
        grads.append(jnp.sum(gy * xs, axis=0, keepdims=True))
        place = pl.ds(pl.multiple_of(group * GROUP + j * LANES, LANES), LANES)
        for k, value in enumerate(grads):
            keep(k, place, value)
    gc_s[...] = gcum
    gd_s[...] = gdir

    @pl.when(group == groups - 1)
    def _():
        row = lax.broadcasted_iota(jnp.int32, (length, length), 0)
        col = lax.broadcasted_iota(jnp.int32, (length, length), 1)
        same = segr_ref[0].T[:, 0:1] == segr_ref[0, 0:1, :]
        gscore = jnp.where((row <= col) & same, gst_s[...], 0.0)
        backs = (dot(gscore, c_s[...], precision=highest), dot(gscore.T, b_s[...], precision=highest))
        for part in range(2):
            sl = slice(part * LANES, (part + 1) * LANES)
            xin = bc_ref[:, sl]
            cw = cwbc_ref[:, sl]
            summed = conv_sum(conv_taps(xin, masks), cw)
            sg = sigmoid(summed)
            gsum = backs[part] * (sg + summed * sg * (1.0 - sg))
            gx, grads = conv_back(gsum, xin, cw, masks, length)
            pr_ref[:, sl] = gx.astype(bf16)
            for k, value in enumerate(grads):
                keep(k, slice(inner_width + part * LANES, inner_width + (part + 1) * LANES), value)
        upper = jnp.where(row <= col, 1.0, 0.0).astype(f32)
        gla = dot(upper, gc_s[...] + rs_ref[0], precision=highest)
        graw = (gd_s[...] - gla * jnp.exp(hp_ref[1:2, :])) * sp_s[...]
        graw = jnp.where(lane < heads, graw, 0.0)
        pr_ref[:, 2 * LANES :] = graw.astype(bf16)
        tail = slice(inner_width + 2 * LANES, inner_width + 3 * LANES)
        keep(0, tail, jnp.sum(graw, axis=0, keepdims=True))
        keep(1, tail, jnp.sum(jnp.where(lane < heads, gla * la_s[...], 0.0), axis=0, keepdims=True))


def small_scratch(length):
    return [
        pltpu.VMEM((3, length, LANES), f32),
        pltpu.VMEM((length, LANES), f32),
        pltpu.VMEM((length, LANES), f32),
        pltpu.VMEM((length, LANES), f32),
        pltpu.VMEM((length, LANES), f32),
        pltpu.VMEM((LANES, length), f32),
        pltpu.VMEM((length, LANES), f32),
        pltpu.VMEM((length, LANES), f32),
        pltpu.VMEM((length, LANES), f32),
    ]


def mixer_forward(projected, gm, segr, cw, hp, cp, heads, state):
    seqs, _, length = segr.shape
    inner = gm.shape[1]
    groups = inner // GROUP
    rows = seqs * length
    kernel = functools.partial(fwd_kernel, heads)
    out_row = lambda b, p, g: (b, g * p)
    return pl.pallas_call(
        kernel,
        grid=(seqs, 2, groups),
        in_specs=[
            pl.BlockSpec((length, GROUP), lambda b, p, g: (b, g)),
            pl.BlockSpec((length, GROUP), lambda b, p, g: (b, groups + g * (1 - p) + (groups - 1) * p)),
            pl.BlockSpec((length, 2 * state), lambda b, p, g: (b, 2 * inner // (2 * state))),
            pl.BlockSpec((length, LANES), lambda b, p, g: (b, (2 * inner + 2 * state) // LANES)),
            pl.BlockSpec((length, GROUP), lambda b, p, g: (b, g)),
            pl.BlockSpec((1, 8, length), lambda b, p, g: (b, 0, 0)),
            pl.BlockSpec((8, GROUP), lambda b, p, g: (0, g)),
            pl.BlockSpec((8, 2 * state), lambda b, p, g: (0, inner // (2 * state))),
            pl.BlockSpec((8, LANES), lambda b, p, g: (0, 0)),
            pl.BlockSpec((8, GROUP), lambda b, p, g: (0, g)),
        ],
        out_specs=[
            pl.BlockSpec((length, GROUP), out_row),
            pl.BlockSpec((GROUP, length), lambda b, p, g: (g * p, b)),
            pl.BlockSpec((length, GROUP), out_row),
            pl.BlockSpec((length, GROUP), out_row),
            pl.BlockSpec((1, length, LANES), lambda b, p, g: (b, 0, 0)),
            pl.BlockSpec((8, inner), lambda b, p, g: (0, 0)),
        ],
        out_shape=[
            jax.ShapeDtypeStruct((rows, inner), bf16),
            jax.ShapeDtypeStruct((inner, rows), bf16),
            jax.ShapeDtypeStruct((rows, inner), bf16),
            jax.ShapeDtypeStruct((rows, inner), f32),
            jax.ShapeDtypeStruct((seqs, length, LANES), f32),
            jax.ShapeDtypeStruct((8, inner), f32),
        ],
        scratch_shapes=small_scratch(length) + [
            pltpu.VMEM((length, length), f32),
            pltpu.VMEM((length, inner), f32),
            pltpu.VMEM((length, inner), f32),
            pltpu.VMEM((length - BLOCK, inner), f32),
            pltpu.VMEM((2, length, LANES), f32),
            pltpu.VMEM((length, LANES), f32),
        ],
        compiler_params=pltpu.CompilerParams(vmem_limit_bytes=62 << 20),
        cost_estimate=pl.CostEstimate(flops=10**10, bytes_accessed=45 * 10**6, transcendentals=10**7),
        name="mixer_forward",
    )(projected, projected, projected, projected, gm, segr, cw, cw, hp, cp)


def pad_lanes(v, width=LANES):
    return jnp.pad(v, ((0, 0), (0, width - v.shape[1])))


def mixer_tables(segments, kernel_full, shift_full, dt_bias, a_log, d_skip, gate_full):
    taps = kernel_full.shape[0]
    seqs, length = segments.shape
    segr = jnp.broadcast_to(segments.astype(f32)[:, None, :], (seqs, 8, length))
    cw = jnp.concatenate([kernel_full.astype(f32), jnp.broadcast_to(shift_full.astype(f32)[None], (8 - taps, shift_full.shape[0]))])
    hp = pad_lanes(jnp.concatenate([dt_bias[None], jnp.broadcast_to(a_log[None], (7, a_log.shape[0]))]))
    heads = dt_bias.shape[0]
    size = gate_full.shape[0] // heads
    cp = jnp.concatenate([jnp.repeat(d_skip, size)[None], jnp.broadcast_to(gate_full.astype(f32)[None], (7, gate_full.shape[0]))])
    return segr, cw, hp, cp


MESH = pl.DeviceIdType.MESH
PIECES = 3


def ring_place(chip, chips):
    wide = chips // 4
    z, q = chip // wide, chip % wide
    up = 1 + 3 * q + jnp.where(q % 2 == 0, z - 1, 3 - z)
    back = jnp.where(q == 0, 0, 4 * wide - q)
    return jnp.where(z == 0, back, up)


def ring_chip(place, chips):
    wide = chips // 4
    place = place % chips
    q = (place - 1 + chips) % chips // 3
    r = (place - 1 + chips) % chips % 3
    z = jnp.where(q % 2 == 0, 1 + r, 3 - r)
    inner = z * wide + q
    outer = (4 * wide - place) % (4 * wide)
    return jnp.where((place == 0) | (place > 3 * wide), outer, inner)


def gather_kernel(chips, count, *refs):
    ins, outs = refs[:count], refs[count : 2 * count]
    ring_send, ring_recv, far_send, far_recv, pair_send, pair_recv, own_sem = refs[2 * count :]
    me = lax.axis_index("fsdp")
    plane = lax.axis_index("dp")
    chip, core = me // 2, me % 2
    place = ring_place(chip, chips)
    right = 2 * ring_chip(place + 1, chips) + core
    left = 2 * ring_chip(place + chips - 1, chips) + core
    pair = {"fsdp": me + 1 - 2 * core}
    peer = {"dp": 1 - plane}
    ways = ({"fsdp": right}, {"fsdp": left})

    barrier = pltpu.get_barrier_semaphore()
    for other in (ways[0], ways[1], pair, peer):
        pl.semaphore_signal(barrier, inc=1, device_id=other, device_id_type=MESH)
    pl.semaphore_wait(barrier, 4)

    half = chips // 2
    whole = [k == count - 1 for k in range(count)]

    def steps(way, slot):
        return half if way == slot else half - 1

    def owner(way, step):
        move = -step if way == 0 else step
        return 2 * ring_chip(place + move + chips, chips) + core

    def part(refs, k, index, slot):
        if whole[k]:
            return refs[k].at[index]
        piece = 0 if slot == 0 else 1 + plane
        return refs[k].at[index, piece]

    def mine(k, slot):
        if whole[k]:
            return ins[k]
        piece = 0 if slot == 0 else 1 + plane
        return ins[k].at[piece]

    def slots(k):
        return (0,) if whole[k] else (1, 0)

    pending = []

    def send(source, target, send_sem, recv_sem, device):
        copy = pltpu.make_async_remote_copy(
            src_ref=source, dst_ref=target, send_sem=send_sem, recv_sem=recv_sem, device_id=device, device_id_type=MESH)
        copy.start()
        pending.append(copy)

    def arrived(target, send_sem, recv_sem):
        pltpu.make_async_remote_copy(
            src_ref=target, dst_ref=target, send_sem=send_sem, recv_sem=recv_sem, device_id=pair, device_id_type=MESH).wait_recv()

    def ring_sem(sem, way, step, k, slot):
        return sem.at[(way * half + step - 1) * 2 * count + 2 * k + slot]

    def far_sem(sem, way, step, k):
        return sem.at[(way * half + step - 1) * count + k]

    def pair_sem(sem, turn, k, slot):
        return sem.at[(turn * count + k) * 3 + slot]

    def turn(way, step):
        return 1 + (step - 1) * 2 + way

    local = []
    for k in range(count):
        for slot in slots(k):
            for way in range(2):
                send(mine(k, slot), part(outs, k, me, slot), ring_sem(ring_send, way, 1, k, slot), ring_sem(ring_recv, way, 1, k, slot), ways[way])
        send(ins[k], outs[k].at[me], pair_sem(pair_send, 0, k, 0), pair_sem(pair_recv, 0, k, 0), pair)
        copy = pltpu.make_async_copy(ins[k], outs[k].at[me], own_sem.at[k])
        copy.start()
        local.append(copy)

    def from_peer(way, step):
        index = owner(way, step)
        for k in range(count):
            if whole[k] or step > steps(way, 1):
                continue
            target = outs[k].at[index, 2 - plane]
            arrived(target, far_sem(far_send, way, step, k), far_sem(far_recv, way, step, k))
            send(target, target, pair_sem(pair_send, turn(way, step), k, 2), pair_sem(pair_recv, turn(way, step), k, 2), pair)

    for step in range(1, half + 1):
        for way in range(2):
            index = owner(way, step)
            for k in range(count):
                for slot in slots(k):
                    if step > steps(way, slot):
                        continue
                    target = part(outs, k, index, slot)
                    arrived(target, ring_sem(ring_send, way, step, k, slot), ring_sem(ring_recv, way, step, k, slot))
                    if step + 1 <= steps(way, slot):
                        send(target, target, ring_sem(ring_send, way, step + 1, k, slot), ring_sem(ring_recv, way, step + 1, k, slot), ways[way])
                    if slot == 1:
                        send(target, target, far_sem(far_send, way, step, k), far_sem(far_recv, way, step, k), peer)
                    send(target, target, pair_sem(pair_send, turn(way, step), k, slot), pair_sem(pair_recv, turn(way, step), k, slot), pair)
        if step > 1:
            for way in range(2):
                from_peer(way, step - 1)
    for way in range(2):
        from_peer(way, half)
    for k in range(count):
        other = outs[k].at[me + 1 - 2 * core]
        arrived(other, pair_sem(pair_send, 0, k, 0), pair_sem(pair_recv, 0, k, 0))
    for step in range(1, half + 1):
        for way in range(2):
            index = owner(way, step) + 1 - 2 * core
            for k in range(count):
                for slot in slots(k) + (() if whole[k] else (2,)):
                    if step > steps(way, min(slot, 1)):
                        continue
                    if slot == 2:
                        target = outs[k].at[index, 2 - plane]
                    else:
                        target = part(outs, k, index, slot)
                    sems = turn(way, step), k, slot
                    arrived(target, pair_sem(pair_send, *sems), pair_sem(pair_recv, *sems))
    for copy in local:
        copy.wait()
    for copy in pending:
        copy.wait_send()


def gather(arrays, devices):
    count = len(arrays)
    chips = devices // 2
    half = chips // 2
    dma = pltpu.SemaphoreType.DMA
    return pl.pallas_call(
        functools.partial(gather_kernel, chips, count),
        in_specs=[pl.BlockSpec(memory_space=pl.ANY)] * count,
        out_specs=[pl.BlockSpec(memory_space=pl.ANY)] * count,
        out_shape=[jax.ShapeDtypeStruct((devices,) + a.shape, a.dtype) for a in arrays],
        scratch_shapes=[
            dma((4 * half * count,)), dma((4 * half * count,)),
            dma((2 * half * count,)), dma((2 * half * count,)),
            dma(((2 * half + 1) * count * 3,)), dma(((2 * half + 1) * count * 3,)),
            dma((count,)),
        ],
        compiler_params=pltpu.CompilerParams(collective_id=0, has_side_effects=True),
        name="gather_weights",
    )(*arrays)


QUARTERS = 4
TILE = 512
FULL = 62 << 20


def add_up(sources, store, width):
    tile = min(TILE, width)

    def total(cols):
        value = sources[0][:, cols].astype(f32)
        for source in sources[1:]:
            value = value + source[:, cols].astype(f32)
        store[:, cols] = value.astype(store.dtype)

    def one(i, carry):
        total(pl.ds(pl.multiple_of(i * tile, LANES), tile))
        return carry

    lax.fori_loop(0, width // tile, one, 0)
    if width % tile:
        total(slice(width - width % tile, width))


class Links:
    def __init__(self, chips):
        self.chips, self.half = chips, chips // 2
        me = lax.axis_index("fsdp")
        self.plane = lax.axis_index("dp")
        self.chip, self.core = me // 2, me % 2
        self.place = ring_place(self.chip, chips)
        self.ways = tuple(
            {"fsdp": 2 * ring_chip(self.place + move, chips) + self.core} for move in (1, chips - 1))
        self.peer = {"dp": 1 - self.plane}
        self.pair = {"fsdp": me + 1 - 2 * self.core}
        self.turns = [{"fsdp": me + bit - 2 * bit * ((me // bit) % 2)} for bit in (1 << k for k in range(chips.bit_length()))] + [self.peer]
        self.sent = []

    def greet(self, others):
        barrier = pltpu.get_barrier_semaphore()
        for other in others:
            pl.semaphore_signal(barrier, inc=1, device_id=other, device_id_type=MESH)
        pl.semaphore_wait(barrier, len(others))

    def send(self, source, target, send_sem, recv_sem, device):
        make = lambda: pltpu.make_async_remote_copy(
            src_ref=source(), dst_ref=target(), send_sem=send_sem(), recv_sem=recv_sem(), device_id=device, device_id_type=MESH)
        make().start()
        self.sent.append(make)

    def arrived(self, target, send_sem, recv_sem):
        pltpu.make_async_remote_copy(
            src_ref=target, dst_ref=target, send_sem=send_sem, recv_sem=recv_sem, device_id=self.peer, device_id_type=MESH).wait_recv()

    def finish(self):
        for make in self.sent:
            make().wait_send()


class Ring:
    def __init__(self, links, items, shift, parts, held, ring_in, peer_in, held_sem, ring_send, ring_recv, peer_send, peer_recv):
        self.links, self.items, self.shift, self.parts = links, items, shift, parts
        self.held, self.ring_in, self.peer_in = held, ring_in, peer_in
        self.held_sem, self.ring_send, self.ring_recv = held_sem, ring_send, ring_recv
        self.peer_send, self.peer_recv = peer_send, peer_recv

    def hops(self, k, way, slot):
        return self.links.half - (slot + (k + self.shift if slot == 2 else 0) + way) % 2

    def target(self, k, way, slot, step):
        chips = self.links.chips
        ahead = self.hops(k, way, slot) - step + 1
        return ring_chip(self.links.place + (ahead if way == 0 else chips - ahead), chips)

    def quarter(self, slot):
        return slot if slot < 2 else 2 + self.links.plane

    def at(self, way, step, slot):
        return (way * self.links.half + step - 1) * 3 + slot

    def sems(self, k, way, step, slot):
        at = k * 6 * self.links.half + self.at(way, step, slot)
        return self.ring_send.at[at], self.ring_recv.at[at]

    def push(self, k, way, step, slot, source):
        at = self.at(way, step, slot)
        self.links.send(
            source, lambda: self.ring_in[k].at[at],
            lambda: self.sems(k, way, step, slot)[0], lambda: self.sems(k, way, step, slot)[1], self.links.ways[way])

    def start(self):
        links, count = self.links, len(self.items)
        for slot in (0, 1):
            for k in range(count):
                for way in range(2):
                    self.push(k, way, 1, slot, lambda k=k, way=way, slot=slot: self.parts[k].at[self.target(k, way, slot, 1), slot])
        for move in self.order():
            for k in range(count):
                def where(move=move):
                    return (links.place + move) % links.chips
                links.send(
                    lambda k=k, where=where: self.parts[k].at[ring_chip(where(), links.chips), 3 - links.plane],
                    lambda k=k, where=where: self.peer_in[k].at[where()],
                    lambda k=k, where=where: self.peer_send.at[k * links.chips + where()],
                    lambda k=k, where=where: self.peer_recv.at[k * links.chips + where()], links.peer)
        for copy in self.loads():
            copy.start()

    def sequence(self):
        half = self.links.half
        main = [("hop", step, slot) for step in range(2, half + 1) for slot in (0, 1)]
        other = [("hop", step, 2) for step in range(1, half + 1)]
        out = []
        for n, entry in enumerate(main):
            out.append(entry)
            if n >= 3 and n % 2 and len(other) > 2:
                out.append(other.pop(0))
        return out + [("land", 0, 0), ("land", 0, 1)] + other + [("land", 0, 2)]

    def order(self):
        chips, half = self.links.chips, self.links.half
        moves = []
        for ahead in range(half, -1, -1):
            moves.append(ahead)
            if 0 < ahead < half:
                moves.append(chips - ahead)
        return moves

    def loads(self):
        return [
            pltpu.make_async_copy(self.parts[k].at[:, self.quarter(slot)], self.held[k].at[slot], self.held_sem.at[k * 3 + slot])
            for k in range(len(self.items)) for slot in range(3)]

    def from_peer(self, k, chunk):
        where = ring_place(chunk, self.links.chips)
        at = k * self.links.chips + where
        self.links.arrived(self.peer_in[k].at[where], self.peer_send.at[at], self.peer_recv.at[at])
        return self.peer_in[k].at[where]

    def hop(self, step, slot):
        for k in range(len(self.items)):
            for way in range(2):
                if step > self.hops(k, way, slot) or (step == 1 and slot < 2):
                    continue
                chunk = self.target(k, way, slot, step)
                sources = [self.held[k].at[slot, chunk]]
                if slot == 2:
                    sources.append(self.from_peer(k, chunk))
                if step > 1:
                    before = self.at(way, step - 1, slot)
                    self.links.arrived(self.ring_in[k].at[before], *self.sems(k, way, step - 1, slot))
                    sources.append(self.ring_in[k].at[before])
                    store = lambda k=k, before=before: self.ring_in[k].at[before]
                else:
                    store = lambda k=k, way=way, slot=slot, step=step: self.peer_in[k].at[
                        ring_place(self.target(k, way, slot, step), self.links.chips)]
                add_up(sources, store(), self.items[k][1])
                self.push(k, way, step, slot, store)

    def land(self, k, slot, store):
        links = self.links
        sources = [self.held[k].at[slot, links.chip]]
        for way in range(2):
            last = self.hops(k, way, slot)
            at = self.at(way, last, slot)
            links.arrived(self.ring_in[k].at[at], *self.sems(k, way, last, slot))
            sources.append(self.ring_in[k].at[at])
        if slot == 2:
            sources.append(self.from_peer(k, links.chip))
        add_up(sources, store, self.items[k][1])


def ring_scratch(items, chips):
    dma = pltpu.SemaphoreType.DMA
    half, count = chips // 2, len(items)
    vm = lambda *lead: [pltpu.VMEM(lead + item, bf16) for item in items]
    return vm(3, chips) + vm(6 * half) + vm(chips) + [
        dma((3 * count,)), dma((6 * half * count,)), dma((6 * half * count,)), dma((chips * count,)), dma((chips * count,))]


def split_scratch(refs, count):
    return [refs[i * count : (i + 1) * count] for i in range(3)], refs[3 * count : 3 * count + 5]


def middle_kernel(heads, chips, seqs, groups, items, x_ref, bc_ref, dtr_ref, gy_ref, rs_ref, segr_ref, cwx_ref, cwbc_ref, hp_ref, cp_ref,
                  gg_ref, mixed_ref, wout_ref, tok_ref, gz_ref, win_ref, nt_ref, nt2_ref, *refs):
    count = len(items)
    parts, refs = refs[:count], refs[count:]
    px_ref, pr_ref, partx_ref, partr_ref, sg_ref, bo_ref, gn_ref = refs[:7]
    owns, nears, refs = refs[7 : 7 + count], refs[7 + count : 7 + 2 * count], refs[7 + 2 * count :]
    back, (nts, nts2, pxs, prs, px2s, pr2s, nt_sem, px_send, px_recv, pr_send, pr_recv, near_send, near_recv), refs = refs[:13], refs[13:26], refs[26:]
    (held, ring_in, peer_in), sems = split_scratch(refs, count)
    step = pl.program_id(0)
    turns = seqs * groups
    last = turns + 3 * groups
    length = x_ref.shape[0]
    links = Links(chips)
    ring = Ring(links, items, 0, parts, held, ring_in, peer_in, *sems)
    turned = lambda: [
        pltpu.make_async_copy(source.at[:, links.core], target, nt_sem.at[n])
        for n, (source, target) in enumerate(((nt_ref, nts), (nt2_ref, nts2)))]

    @pl.when(step == 0)
    def _():
        links.greet([links.ways[0], links.ways[1], links.peer, links.pair])
        ring.start()
        for copy in turned():
            copy.start()

    plan = {}
    sequence = ring.sequence()
    for n, entry in enumerate(sequence):
        plan.setdefault(max(2, (n + 1) * last // len(sequence)), []).append(entry)

    def px_copy(turn):
        return pltpu.make_async_remote_copy(
            src_ref=pxs.at[turn], dst_ref=px2s.at[turn], send_sem=px_send.at[turn], recv_sem=px_recv.at[turn],
            device_id=links.pair, device_id_type=MESH)

    def pr_copy(seq):
        return pltpu.make_async_remote_copy(
            src_ref=prs.at[seq], dst_ref=pr2s.at[seq], send_sem=pr_send.at[seq], recv_sem=pr_recv.at[seq],
            device_id=links.pair, device_id_type=MESH)

    @pl.when(step < turns)
    def _():
        group = step % groups
        mixer_back(heads, groups, group, step == 0, x_ref, bc_ref, dtr_ref, gy_ref, rs_ref, segr_ref, cwx_ref, cwbc_ref, hp_ref, cp_ref,
                   px_ref, pr_ref, sg_ref, *back)
        pxs[step] = px_ref[...]
        px_copy(step).start()

        @pl.when(group == groups - 1)
        def _():
            seq = step // groups
            prs[seq] = pr_ref[...]
            pr_copy(seq).start()

    @pl.when((step >= turns) & (step < turns + groups))
    def _():
        part = dot(mixed_ref[...], wout_ref[...])

        @pl.when(step == turns)
        def _():
            gn_ref[...] = tok_ref[...].astype(f32) + part

        @pl.when((step > turns) & (step < turns + groups - 1))
        def _():
            gn_ref[...] += part

        @pl.when(step == turns + groups - 1)
        def _():
            bo_ref[...] = (gn_ref[...] + part).astype(bf16)

    @pl.when((step >= turns + groups) & (step < turns + 2 * groups))
    def _():
        part = dot(gz_ref[...], win_ref[...], NT)

        @pl.when(step == turns + groups)
        def _():
            gn_ref[...] = part

        @pl.when(step > turns + groups)
        def _():
            gn_ref[...] += part

    def own_rows(mine, theirs, store):
        many, each, tokens = nts.shape
        pieces = [(n * length, left, right) for left, rights in ((nts, mine), (nts2, theirs)) for n, right in enumerate(rights)]
        if each % 16 == 0:
            total = None
            for at, left, right in pieces:
                part = dot(left[:, :, at : at + length].reshape(many * each, length), right)
                total = part if total is None else total + part
            store[...] = total.astype(bf16)
        else:
            for n in range(many):
                total = sum(dot(left[n, :, at : at + length], right) for at, left, right in pieces)
                store[n * each : (n + 1) * each, :] = total.astype(bf16)

    @pl.when(step == turns + 2 * groups)
    def _():
        for copy in turned():
            copy.wait()
        for turn in range(turns):
            px_copy(turn).wait()
        for seq in range(seqs):
            pr_copy(seq).wait()

    @pl.when((step >= turns + 2 * groups) & (step < turns + 3 * groups))
    def _():
        group = step - turns - 2 * groups
        at = [group + seq * groups for seq in range(seqs)]
        own_rows([pxs[n] for n in at], [px2s[n] for n in at], partx_ref)

    @pl.when(step == last)
    def _():
        own_rows([prs[n] for n in range(seqs)], [pr2s[n] for n in range(seqs)], partr_ref)

    for when in sorted(plan):
        @pl.when(step == when)
        def _(when=when):
            if when == min(plan):
                for copy in ring.loads():
                    copy.wait()
            for kind, hop, slot in plan[when]:
                if kind == "hop":
                    ring.hop(hop, slot)
                    continue
                for k in range(count):
                    ring.land(k, slot, owns[k].at[slot])
                    if slot < 2:
                        links.send(
                            lambda k=k, slot=slot: owns[k].at[slot], lambda k=k, slot=slot: nears[k].at[slot],
                            lambda k=k, slot=slot: near_send.at[2 * k + slot], lambda k=k, slot=slot: near_recv.at[2 * k + slot], links.peer)

    @pl.when(step == last)
    def _():
        sg_ref[6:7, : gg_ref.shape[1]] = gg_ref[0:1, :]
        for slot in range(2):
            for k in range(count):
                links.arrived(nears[k].at[slot], near_send.at[2 * k + slot], near_recv.at[2 * k + slot])
        links.finish()


def middle(projected, gy, rs, segr, cw, hp, cp, gg, mixed, w_out_full, tokens, gz, w_in_full, left, left2, arrays, heads, state, devices):
    seqs, _, length = segr.shape
    inner = gy.shape[1]
    width = tokens.shape[1]
    groups = inner // GROUP
    rows = seqs * length
    turns = seqs * groups
    chips = devices // 2
    items = tuple(a.shape[2:] for a in arrays)
    count = len(items)
    dma = pltpu.SemaphoreType.DMA
    seq = lambda i: jnp.minimum(i // groups, seqs - 1)
    grp = lambda i: jnp.where(i < turns, i % groups, groups - 1)
    out_at = lambda i: jnp.clip(i - turns, 0, groups - 1)
    in_at = lambda i: jnp.clip(i - turns - groups, 0, groups - 1)
    x_at = lambda i: jnp.clip(i - turns - 2 * groups, 0, groups - 1)
    total = chips * left.shape[2]
    const = lambda *shape: pl.BlockSpec(shape, lambda i: (0,) * len(shape), pipeline_mode=pl.Buffered(1))
    any_spec = pl.BlockSpec(memory_space=pl.ANY)
    small_width = inner + 3 * LANES
    return pl.pallas_call(
        functools.partial(middle_kernel, heads, chips, seqs, groups, items),
        grid=(turns + 3 * groups + 1,),
        in_specs=[
            pl.BlockSpec((length, GROUP), lambda i: (seq(i), groups + grp(i))),
            pl.BlockSpec((length, 2 * state), lambda i: (seq(i), 2 * inner // (2 * state))),
            pl.BlockSpec((length, LANES), lambda i: (seq(i), (2 * inner + 2 * state) // LANES)),
            pl.BlockSpec((length, GROUP), lambda i: (seq(i), grp(i))),
            pl.BlockSpec((1, length, LANES), lambda i: (seq(i), 0, 0)),
            pl.BlockSpec((1, 8, length), lambda i: (seq(i), 0, 0)),
            pl.BlockSpec((8, GROUP), lambda i: (0, grp(i))),
            pl.BlockSpec((8, 2 * state), lambda i: (0, inner // (2 * state))),
            pl.BlockSpec((8, LANES), lambda i: (0, 0)),
            pl.BlockSpec((8, GROUP), lambda i: (0, grp(i))),
            const(8, inner),
            pl.BlockSpec((rows, GROUP), lambda i: (0, out_at(i))),
            pl.BlockSpec((GROUP, width), lambda i: (out_at(i), 0)),
            const(rows, width),
            pl.BlockSpec((rows, GROUP), lambda i: (0, in_at(i))),
            pl.BlockSpec((width, GROUP), lambda i: (0, in_at(i))),
        ] + [any_spec] * (2 + count),
        out_specs=[
            pl.BlockSpec((length, GROUP), lambda i: (seq(i), grp(i))),
            pl.BlockSpec((length, 3 * LANES), lambda i: (seq(i), 0)),
            pl.BlockSpec((total, GROUP), lambda i: (0, x_at(i))),
            const(total, 3 * LANES),
            const(8, small_width),
            const(rows, width),
            const(rows, width),
        ] + [const(3, *item) for item in items] + [any_spec] * count,
        out_shape=[
            jax.ShapeDtypeStruct((rows, inner), bf16),
            jax.ShapeDtypeStruct((rows, 3 * LANES), bf16),
            jax.ShapeDtypeStruct((total, inner), bf16),
            jax.ShapeDtypeStruct((total, 3 * LANES), bf16),
            jax.ShapeDtypeStruct((8, small_width), f32),
            jax.ShapeDtypeStruct((rows, width), bf16),
            jax.ShapeDtypeStruct((rows, width), f32),
        ] + [jax.ShapeDtypeStruct((3,) + item, bf16) for item in items] + [jax.ShapeDtypeStruct((2,) + item, bf16) for item in items],
        scratch_shapes=small_scratch(length) + [
            pltpu.VMEM((length, length), f32),
            pltpu.VMEM((length, length), f32),
            pltpu.VMEM((length, LANES), f32),
            pltpu.VMEM((length, LANES), f32),
            pltpu.VMEM((chips,) + left.shape[2:], bf16),
            pltpu.VMEM((chips,) + left.shape[2:], bf16),
            pltpu.VMEM((turns, length, GROUP), bf16),
            pltpu.VMEM((seqs, length, 3 * LANES), bf16),
            pltpu.VMEM((turns, length, GROUP), bf16),
            pltpu.VMEM((seqs, length, 3 * LANES), bf16),
            dma((2,)), dma((turns,)), dma((turns,)), dma((seqs,)), dma((seqs,)), dma((2 * count,)), dma((2 * count,)),
        ] + ring_scratch(items, chips),
        compiler_params=pltpu.CompilerParams(collective_id=1, has_side_effects=True, vmem_limit_bytes=FULL),
        name="middle",
    )(projected, projected, projected, gy, rs, segr, cw, cw, hp, cp, gg, mixed, w_out_full, tokens, gz, w_in_full, left, left2, *arrays)


def tail_kernel(chips, groups, used, items, early, px_ref, pr_ref, win_ref, gacc_ref, tok_ref, cot_ref, gain_ref, sg_ref, *refs):
    count, first = len(items), len(early)
    parts, halves, refs = refs[:count], refs[count : count + first], refs[count + first :]
    gt_ref, small_ref, refs = refs[0], refs[1], refs[2:]
    last_in, last_out, refs = refs[: first + count], refs[first + count : first + 2 * count], refs[first + 2 * count :]
    (small_in, small_sent, small_recv, small_send, small_sem, last_send, last_recv), refs = refs[:7], refs[7:]
    (held, ring_in, peer_in), sems = split_scratch(refs, count)
    step = pl.program_id(0)
    links = Links(chips)
    ring = Ring(links, items, 0, parts, held, ring_in, peer_in, *sems)
    rounds = len(links.turns)

    def swap(k, slot, source):
        at = k * 3 + slot
        links.send(source, lambda: last_in[k].at[slot], lambda: last_send.at[at], lambda: last_recv.at[at], links.peer)

    @pl.when(step == 0)
    def _():
        links.greet(list(links.ways) + links.turns)
        ring.start()
        for k in range(first):
            links.send(lambda k=k: halves[k].at[2], lambda k=k: last_in[k].at[0], lambda k=k: last_send.at[3 * k], lambda k=k: last_recv.at[3 * k], links.peer)
        gt_ref[...] = gacc_ref[...] + dot(px_ref[...], win_ref[...], NT)

    @pl.when((step > 0) & (step < groups))
    def _():
        gt_ref[...] += dot(px_ref[...], win_ref[...], NT)

    every = ring.sequence()
    inside, later = every[:3], every[3:]

    def run(kind, hop, slot):
        if kind == "hop":
            ring.hop(hop, slot)
            return
        for k in range(count):
            ring.land(k, slot, last_out[k].at[slot])
            swap(first + k, slot, lambda k=k, slot=slot: last_out[k].at[slot])

    for n, entry in enumerate(inside):
        @pl.when(step == min(groups - 1, 1 + 2 * n))
        def _(n=n, entry=entry):
            if n == 0:
                for copy in ring.loads():
                    copy.wait()
            run(*entry)

    def small_round(turn):
        links.send(
            lambda: small_in if turn == 0 else small_sent.at[turn - 1], lambda: small_recv.at[turn],
            lambda: small_send.at[turn], lambda: small_sem.at[turn], links.turns[turn])

    def small_finish(turn):
        value = small_in if turn == 0 else small_sent.at[turn - 1]
        links.arrived(small_recv.at[turn], small_send.at[turn], small_sem.at[turn])
        store = small_ref if turn == rounds - 1 else small_sent.at[turn]
        store[...] = value[...] + small_recv[turn]

    @pl.when(step == groups)
    def _():
        size = pr_ref.shape[1]
        col = lax.broadcasted_iota(jnp.int32, (win_ref.shape[0], size), 1)
        rest = jnp.where(col < used, win_ref[:, :size].astype(f32), 0.0).astype(bf16)
        rows, width = gt_ref.shape

        def close(i):
            sl = slice(i * BLOCK, (i + 1) * BLOCK)
            u = tok_ref[sl].astype(f32)
            rstd = lax.rsqrt(jnp.mean(u * u, axis=1, keepdims=True) + epsilon)
            unit = u * rstd
            gn = gt_ref[sl] + dot(pr_ref[sl], rest, NT)
            small_in[7:8, :width] = small_in[7:8, :width] + jnp.sum(gn * unit, axis=0, keepdims=True)
            gu = gn * gain_ref[0:1, :]
            inward = jnp.mean(gu * unit, axis=1, keepdims=True)
            gt_ref[sl] = cot_ref[sl].astype(f32) + rstd * (gu - unit * inward)

        small_in[...] = sg_ref[...]
        chunks, done = 0, -1
        sent = []
        for entry in later:
            sent.append(entry)
            if chunks < rows // BLOCK:
                close(chunks)
                chunks += 1
            run(*entry)
            if chunks == rows // BLOCK:
                if done < 0:
                    small_round(0)
                    done = 0
                elif done < rounds - 1 and len(sent) % 2:
                    small_finish(done)
                    done += 1
                    small_round(done)
        while done < rounds:
            small_finish(done)
            done += 1
            if done < rounds:
                small_round(done)
        for slot in range(3):
            for k in range(first + count):
                at = k * 3 + slot
                if k >= first or slot == 0:
                    links.arrived(last_in[k].at[slot], last_send.at[at], last_recv.at[at])
        links.finish()


def tail(px, pr, w_in_full, gacc, tokens, cot, gain, sg, arrays, halves, used, devices):
    rows, width = tokens.shape
    groups = px.shape[1] // GROUP
    chips = devices // 2
    items = tuple(a.shape[2:] for a in arrays)
    early = tuple(h.shape[1:] for h in halves)
    count, first = len(items), len(early)
    rounds = chips.bit_length() + 1
    dma = pltpu.SemaphoreType.DMA
    const = lambda *shape: pl.BlockSpec(shape, lambda i: (0,) * len(shape), pipeline_mode=pl.Buffered(1))
    any_spec = pl.BlockSpec(memory_space=pl.ANY)
    every = early + items
    return pl.pallas_call(
        functools.partial(tail_kernel, chips, groups, used, items, early),
        grid=(groups + 1,),
        in_specs=[
            pl.BlockSpec((rows, GROUP), lambda i: (0, jnp.minimum(i, groups - 1))),
            const(rows, pr.shape[1]),
            pl.BlockSpec((width, GROUP), lambda i: (0, groups + i)),
            const(rows, width),
            const(rows, width),
            const(rows, width),
            const(8, width),
            const(*sg.shape),
        ] + [any_spec] * (count + first),
        out_specs=[const(rows, width), const(*sg.shape)] + [any_spec] * len(every) + [const(3, *item) for item in items],
        out_shape=[jax.ShapeDtypeStruct((rows, width), f32), jax.ShapeDtypeStruct(sg.shape, f32)]
        + [jax.ShapeDtypeStruct(((1 if k < first else 3),) + item, bf16) for k, item in enumerate(every + items)],
        scratch_shapes=[
            pltpu.VMEM(sg.shape, f32), pltpu.VMEM((rounds,) + sg.shape, f32), pltpu.VMEM((rounds,) + sg.shape, f32),
            dma((rounds,)), dma((rounds,)), dma((3 * (first + count),)), dma((3 * (first + count),)),
        ] + ring_scratch(items, chips),
        compiler_params=pltpu.CompilerParams(collective_id=2, has_side_effects=True, vmem_limit_bytes=FULL),
        name="tail",
    )(px, pr, w_in_full, gacc, tokens, cot, gain, sg, *arrays, *halves)


def finish_kernel(sizes, count, first, where_ref, *refs):
    taps, share_c, share_g, share_n, heads, columns = sizes
    mine, theirs, nears, refs = refs[:count], refs[count : 2 * count], refs[2 * count : 2 * count + first], refs[2 * count + first :]
    small_ref, w_out_ref, w_in_ref, norm_ref, kernel_ref, shift_ref, dt_ref, rate_ref, skip_ref, gate_ref = refs
    me, plane = where_ref[0], where_ref[1]
    span = small_ref.shape[1]
    begin = 0
    for k in range(count):
        rows, width = mine[k].shape[1:]
        store = w_out_ref if k == 0 else w_in_ref
        left = 0 if k == 0 else begin
        used = min(width, store.shape[1] - left)
        for slot in range(2):
            total = mine[k][slot].astype(f32) + (nears if k < first else theirs)[k][slot].astype(f32)
            store[slot * rows : (slot + 1) * rows, left : left + used] = total[:, :used]
        own, other = mine[k][2].astype(f32), theirs[k][0 if k < first else 2].astype(f32)
        low = jnp.where(plane == 0, own, other)
        high = jnp.where(plane == 0, other, own)
        store[2 * rows : 3 * rows, left : left + used] = low[:, :used]
        store[3 * rows : 4 * rows, left : left + used] = high[:, :used]
        if k:
            begin += width
    small = small_ref[...]
    conv = pltpu.roll(small, lax.rem(span - me * share_c, span), 1)
    kernel_ref[...] = conv[:taps, :share_c]
    shift_ref[...] = conv[taps : taps + 1, :share_c]
    gate_ref[...] = pltpu.roll(small, lax.rem(span - me * share_g, span), 1)[6:7, :share_g]
    norm_ref[...] = pltpu.roll(small, lax.rem(span - me * share_n, span), 1)[7:8, :share_n]
    inner = span - 3 * LANES
    dt_ref[...] = small[0:1, inner + 2 * LANES : inner + 2 * LANES + heads]
    rate_ref[...] = small[1:2, inner + 2 * LANES : inner + 2 * LANES + heads]
    size = inner // heads
    source = lax.broadcasted_iota(jnp.int32, (inner, LANES), 0) // size
    pick = (source == lax.broadcasted_iota(jnp.int32, (inner, LANES), 1)).astype(f32)
    skip_ref[...] = dot(small[:, :inner], pick, precision=highest)[taps + 1 : taps + 2, :heads]


def finish(me, plane, mine, theirs, nears, small, taps, share_c, share_g, share_n, heads, columns):
    count = len(mine)
    out = lambda *shape: jax.ShapeDtypeStruct(shape, f32)
    spec = pl.BlockSpec(memory_space=pltpu.VMEM)
    shapes = [out(4 * mine[0].shape[1], mine[0].shape[2]), out(4 * mine[1].shape[1], columns), out(1, share_n), out(taps, share_c),
              out(1, share_c), out(1, heads), out(1, heads), out(1, heads), out(1, share_g)]
    return pl.pallas_call(
        functools.partial(finish_kernel, (taps, share_c, share_g, share_n, heads, columns), count, len(nears)),
        in_specs=[pl.BlockSpec(memory_space=pltpu.SMEM)] + [spec] * (2 * count + len(nears) + 1),
        out_specs=[spec] * len(shapes),
        out_shape=shapes,
        name="finish",
    )(jnp.stack([me, plane]).astype(jnp.int32), *mine, *theirs, *nears, small)


def parts_kernel(core_ref, a_ref, a2_ref, b_ref, b2_ref, o_ref):
    rows = o_ref.shape[0]
    a = a_ref[...].reshape(rows, a_ref.shape[3])
    a2 = a2_ref[...].reshape(rows, a2_ref.shape[3])
    o_ref[...] = (dot(a, b_ref[...]) + dot(a2, b2_ref[...])).astype(bf16)


def grad_parts(core, left, left2, right, right2, name):
    chips, _, rows, tokens = left.shape
    if rows % 16:
        pick = lambda v: lax.dynamic_index_in_dim(v, core, 1, keepdims=False).reshape(1, 1, chips * rows, tokens)
        left, left2, core, chips, rows = pick(left), pick(left2), 0, 1, chips * rows
    width = right.shape[1]
    tile = min(GROUP, width)
    left_spec = pl.BlockSpec((chips, 1, rows, tokens), lambda i, c: (0, c[0], 0, 0), pipeline_mode=pl.Buffered(1))
    total = chips * rows
    return pl.pallas_call(
        parts_kernel,
        grid_spec=pltpu.PrefetchScalarGridSpec(
            num_scalar_prefetch=1,
            grid=(width // tile,),
            in_specs=[
                left_spec, left_spec,
                pl.BlockSpec((tokens, tile), lambda i, c: (0, i)),
                pl.BlockSpec((tokens, tile), lambda i, c: (0, i)),
            ],
            out_specs=pl.BlockSpec((total, tile), lambda i, c: (0, i)),
        ),
        out_shape=jax.ShapeDtypeStruct((total, width), bf16),
        compiler_params=pltpu.CompilerParams(vmem_limit_bytes=FULL),
        cost_estimate=pl.CostEstimate(flops=4 * total * tokens * width, bytes_accessed=2 * (2 * total * tokens + 2 * tokens * width + total * width), transcendentals=0),
        name=name,
    )(jnp.full((1,), core, jnp.int32), left, left2, right, right2)


def local(devices, tokens, segments, norm_gain, w_in, conv_weight, conv_bias, dt_bias, a_log, d_skip, gate_gain, w_out, cotangent):
    seqs, length, width = tokens.shape
    rows = seqs * length
    proj_width = w_in.shape[1]
    inner = devices * w_out.shape[0]
    taps = conv_weight.shape[0]
    heads = dt_bias.shape[0]
    share_n, share_c, share_g = norm_gain.shape[0], conv_bias.shape[0], gate_gain.shape[0]
    conv_width = devices * share_c
    state = (conv_width - inner) // 2
    chips = devices // 2
    me = lax.axis_index("fsdp")
    core = me % 2
    swap = [(i, i + 1 - 2 * (i % 2)) for i in range(devices)]
    partner = lambda value: lax.ppermute(value, "fsdp", swap)

    span = LANES * (-(-max(share_n, share_g, share_c) // LANES))
    line = lambda value: pad_lanes(value.reshape(-1, value.shape[-1]), span)
    pack = jnp.concatenate([line(conv_weight), line(conv_bias), line(gate_gain), line(norm_gain)])
    pack = jnp.pad(pack, ((0, -pack.shape[0] % 8), (0, 0)))
    win_all, wout_all, pack_all = gather(
        [w_in.reshape(PIECES, -1, proj_width), w_out.reshape(PIECES, -1, width), pack], devices)
    w_in_full = win_all.reshape(width, proj_width)
    w_out_full = wout_all.reshape(inner, width)
    kernel_full = pack_all[:, :taps, :share_c].transpose(1, 0, 2).reshape(taps, conv_width)
    shift_full = pack_all[:, taps, :share_c].reshape(conv_width)
    gate_full = pack_all[:, taps + 1, :share_g].reshape(inner)
    gain_full = pack_all[:, taps + 2, :share_n].reshape(width)

    flat_tokens = tokens.reshape(rows, width)
    residual = flat_tokens.astype(f32)
    rstd = lax.rsqrt(jnp.mean(residual * residual, axis=-1, keepdims=True) + epsilon)
    gain_f = gain_full.astype(f32)
    normed = (residual * rstd * gain_f).astype(bf16)
    grad_rows = cotangent.reshape(rows, width)
    grad_rows2 = partner(grad_rows)
    normed, normed_t = lax.optimization_barrier((normed, normed.T.reshape(chips, 2, -1, rows)))
    normed_t2 = partner(normed_t)
    projected = dot(normed, w_in_full)
    gm = dot(grad_rows, w_out_full, NT)
    tables = mixer_tables(segments, kernel_full, shift_full, dt_bias, a_log, d_skip, gate_full)
    segr, cw, hp, cp = tables
    hp, normed_t2, grad_rows2 = lax.optimization_barrier((hp, normed_t2, grad_rows2))
    tables = segr, cw, hp, cp
    mixed, mixed_t, gz, gy, rs, gg = mixer_forward(projected, gm, *tables, heads, state)
    mixed_t = mixed_t.reshape(chips, 2, -1, rows)
    gz2, mixed_t2 = partner(gz), partner(mixed_t)
    quarters = lambda part: part.reshape(chips, QUARTERS, -1, part.shape[1])
    part_out = quarters(grad_parts(core, mixed_t, mixed_t2, grad_rows, grad_rows2, "grad_out"))
    part_z = quarters(grad_parts(core, normed_t, normed_t2, gz, gz2, "grad_z"))
    px, pr, part_x, part_r, sg, block_out, gacc, half_out, half_z, *nears = middle(
        projected, gy, rs, *tables, gg, mixed, w_out_full, flat_tokens, gz, w_in_full, normed_t, normed_t2, [part_out, part_z], heads, state, devices)
    gain8 = jnp.broadcast_to(gain_f[None], (8, width))
    grad_tokens, small, *theirs, half_x, half_r = tail(
        px, pr, w_in_full, gacc, flat_tokens, grad_rows, gain8, sg, [quarters(part_x), quarters(part_r)], [half_out, half_z], 2 * state + heads, devices)
    grad_w_out, grad_w_in, norm, kernel, shift, offset, rate, skip, gate = finish(
        me, lax.axis_index("dp"), [half_out, half_z, half_x, half_r], theirs, nears, small, taps, share_c, share_g, share_n, heads, proj_width)
    return (
        block_out.reshape(seqs, length, width),
        grad_tokens.reshape(seqs, length, width),
        norm[0],
        grad_w_in,
        kernel,
        shift[0],
        offset[0],
        rate[0],
        skip[0],
        gate[0],
        grad_w_out,
    )


def solution(mesh):
    rows3, rows2 = P(("fsdp", "dp"), None, None), P(("fsdp", "dp"), None)
    return jax.shard_map(
        functools.partial(local, mesh.shape["fsdp"]),
        mesh=mesh,
        in_specs=(rows3, rows2, P("fsdp"), P("fsdp", None), P(None, "fsdp"), P("fsdp"), P(), P(), P(), P("fsdp"), P("fsdp", None), rows3),
        out_specs=(rows3, rows3, P("fsdp"), P("fsdp", None), P(None, "fsdp"), P("fsdp"), P(), P(), P(), P("fsdp"), P("fsdp", None)),
        check_vma=False,
    )
```
